32 devices in a mesh: seq: 16 (over z, y, x), head: 2 (over core).
Axes of the slice: x: 2, y: 2, z: 4, core: 2. Of those that a mesh axis runs over, the one named last changes fastest.
Arguments:
- queries: bfloat16 [32768, 1024], P('seq', 'head'), may hold values from -10 to 10
- key_vectors: bfloat16 [32768, 1024], P('seq', 'head'), may hold values from -10 to 10
- value_vectors: bfloat16 [32768, 1024], P('seq', 'head'), may hold values from -6 to 6
- grad_output: bfloat16 [32768, 1024], P('seq', 'head'), may hold values from -6 to 6
Outputs:
- attended: bfloat16 [32768, 1024], P('seq', 'head')
- grad_queries: bfloat16 [32768, 1024], P('seq', 'head')
- grad_keys: bfloat16 [32768, 1024], P('seq', 'head')
- grad_values: bfloat16 [32768, 1024], P('seq', 'head')
The draws below stay inside these ranges and needn't reach their ends.
All inputs are finite; a program needn't handle non-finite values.
Results may differ from the reference program's by a relative error of at most 0.019.
Values may be sent and summed in bfloat16 or wider, within the bound.
A program may use at most 128 MiB of HBM per device.

```python
import math
import jax
import jax.numpy as jnp
from jax import lax

ROW_LEN = 512
HEADS = 8
HEAD_DIM = 128
ROWS = 64
TOKENS = 32768


def draw_pair(key):
    base = jax.random.fold_in(key, 11)
    draw_keys = jax.random.split(base, 2)
    width = HEADS * HEAD_DIM
    query_grid = jnp.clip(jax.random.normal(draw_keys[0], (ROWS, ROW_LEN, width), jnp.float32), -6.0, 6.0)
    key_grid = jnp.clip(jax.random.normal(draw_keys[1], (ROWS, ROW_LEN, width), jnp.float32), -6.0, 6.0)
    return (query_grid.reshape(TOKENS, width), key_grid.reshape(TOKENS, width))


def draw_queries(key, part):
    return draw_pair(key)[0].astype(jnp.bfloat16)


def draw_key_vectors(key, part):
    return draw_pair(key)[1].astype(jnp.bfloat16)


def shard_levels(rng, extent, shards, least, top_value):
    loudness, own = 1.0, jax.random.fold_in(rng, 6)
    for dim, parts in shards:
        draws = jnp.exp(jax.random.uniform(jax.random.fold_in(own, dim), (parts,), jnp.float32, least / len(shards), top_value / len(shards)))
        loudness = loudness * jnp.repeat(draws, extent[dim] // parts).reshape([-1 if axis == dim else 1 for axis in range(len(extent))])
    return loudness


def bell_draw(stream_key, dims, scale, bound, cuts=(), dtype=jnp.bfloat16):
    entries = scale * jax.random.normal(stream_key, dims, jnp.float32)
    if cuts:
        entries = entries * shard_levels(stream_key, dims, cuts, -0.22, 0.18)
    return jnp.clip(entries, -bound, bound).astype(dtype)


def setup_inputs(seed: int = 0) -> dict:
    arg_keys = jax.random.split(jax.random.key(seed), 5)
    queries = draw_queries(jax.random.fold_in(arg_keys[4], 71), 0)
    key_vectors = draw_key_vectors(jax.random.fold_in(arg_keys[4], 71), 0)
    value_vectors = bell_draw(arg_keys[2], (TOKENS, HEADS * HEAD_DIM), 1.0, 6.0, ((0, 16), (1, 2)))
    grad_output = bell_draw(arg_keys[3], (TOKENS, HEADS * HEAD_DIM), 1.0, 6.0, ((0, 16), (1, 2)))
    return {"queries": queries, "key_vectors": key_vectors, "value_vectors": value_vectors, "grad_output": grad_output}


NEG_FILL = -1e+30

def rounded(array):
    return lax.optimization_barrier(array.astype(jnp.bfloat16)).astype(jnp.float32)

def pattern_forward(query_block, key_block, value_block, allowed):
    scaling = 1.0 / math.sqrt(HEAD_DIM)
    scores = jnp.einsum('qhd,khd->hqk', query_block.astype(jnp.float32), key_block.astype(jnp.float32)) * scaling
    maxima = lax.optimization_barrier(jnp.max(jnp.where(allowed, scores, NEG_FILL), axis=-1))
    weights = jnp.where(allowed, jnp.exp(scores - maxima[..., None]), 0.0)
    totals = lax.optimization_barrier(jnp.sum(weights, axis=-1))
    accumulated = jnp.einsum('hqk,khd->qhd', rounded(weights), value_block.astype(jnp.float32))
    return (accumulated, maxima.T, totals.T)

def pattern_backward(query_block, key_block, value_block, grad_block, log_totals, correction, allowed):
    scaling = 1.0 / math.sqrt(HEAD_DIM)
    query_f = query_block.astype(jnp.float32)
    key_f = key_block.astype(jnp.float32)
    grad_f = grad_block.astype(jnp.float32)
    scores = jnp.einsum('qhd,khd->hqk', query_f, key_f) * scaling
    probabilities = jnp.where(allowed, jnp.exp(scores - log_totals.T[..., None]), 0.0)
    grad_value = jnp.einsum('hqk,qhd->khd', rounded(probabilities), grad_f)
    grad_probs = jnp.einsum('qhd,khd->hqk', grad_f, value_block.astype(jnp.float32))
    grad_scores = rounded(probabilities * (grad_probs - correction.T[..., None]))
    grad_query = jnp.einsum('hqk,khd->qhd', grad_scores, key_f) * scaling
    grad_key = jnp.einsum('hqk,qhd->khd', grad_scores, query_f) * scaling
    return (grad_query, grad_key, grad_value)

def reference(queries, key_vectors, value_vectors, grad_output):
    layout = (ROWS, ROW_LEN, HEADS, HEAD_DIM)
    query_rows = queries.reshape(layout)
    key_rows = key_vectors.reshape(layout)
    value_rows = value_vectors.reshape(layout)
    grad_rows = grad_output.reshape(layout)
    column_pos = jnp.arange(ROW_LEN)
    row_allowed = column_pos[None, :] <= column_pos[:, None]
    row_pos = jnp.arange(ROWS)
    column_allowed = row_pos[None, :] < row_pos[:, None]

    def swapped(array):
        return jnp.swapaxes(array, 0, 1)
    row_acc, row_max, row_tot = lax.map(lambda blocks: pattern_forward(blocks[0], blocks[1], blocks[2], row_allowed), (query_rows, key_rows, value_rows))
    col_acc, col_max, col_tot = lax.map(lambda blocks: pattern_forward(blocks[0], blocks[1], blocks[2], column_allowed), (swapped(query_rows), swapped(key_rows), swapped(value_rows)))
    col_acc, col_max, col_tot = (swapped(col_acc), swapped(col_max), swapped(col_tot))
    col_floor = jnp.maximum(col_tot, 1.0)
    col_out = rounded(col_acc / col_floor[..., None])
    col_lse = col_max + jnp.log(col_floor)
    maxima = jnp.maximum(row_max, col_lse)
    row_weight = jnp.exp(row_max - maxima)
    col_weight = jnp.exp(col_lse - maxima)
    denominators = row_tot * row_weight + col_weight
    attended = (row_acc * row_weight[..., None] + col_out * col_weight[..., None]) / denominators[..., None]
    log_totals = maxima + jnp.log(denominators)
    attended_low = attended.astype(jnp.bfloat16)
    correction = lax.optimization_barrier(jnp.sum(grad_rows.astype(jnp.float32) * lax.optimization_barrier(attended_low).astype(jnp.float32), axis=-1))
    row_grads = lax.map(lambda blocks: pattern_backward(blocks[0], blocks[1], blocks[2], blocks[3], blocks[4], blocks[5], row_allowed), (query_rows, key_rows, value_rows, grad_rows, log_totals, correction))
    col_grads = lax.map(lambda blocks: pattern_backward(blocks[0], blocks[1], blocks[2], blocks[3], blocks[4], blocks[5], column_allowed), (swapped(query_rows), swapped(key_rows), swapped(value_rows), swapped(grad_rows), swapped(log_totals), swapped(correction)))
    outputs = []
    for row_part, col_part in zip(row_grads, col_grads):
        total = row_part + rounded(swapped(col_part))
        outputs.append(total.astype(jnp.bfloat16).reshape(TOKENS, HEADS * HEAD_DIM))
    return (attended_low.reshape(TOKENS, HEADS * HEAD_DIM), outputs[0], outputs[1], outputs[2])
```

```python
import functools
import math

import jax
import jax.numpy as jnp
from jax import lax
from jax.experimental import pallas as pl
from jax.experimental.pallas import tpu as pltpu
from jax.sharding import PartitionSpec as P

ROW_LEN = 512
HEAD_DIM = 128
GROUP = 8
CHUNK = 256
PIECES = 2
MASKED = -1e30
FLOOR = -1e20
LOG2E = 1.0 / math.log(2.0)
SCALE = 1.0 / math.sqrt(HEAD_DIM)
F32 = jnp.float32
BF16 = jnp.bfloat16


def dot_t(left, right):
    return lax.dot_general(left, right, (((1,), (1,)), ((), ())), preferred_element_type=F32)


def dot_f(left, right):
    return lax.dot_general(left, right, (((0,), (0,)), ((), ())), preferred_element_type=F32)


def dot(left, right):
    return jnp.dot(left, right, preferred_element_type=F32)


def row_bias(first, key_chunk, query_chunk):
    if key_chunk < query_chunk:
        return None
    keys = lax.broadcasted_iota(jnp.int32, (CHUNK, CHUNK), 0)
    queries = lax.broadcasted_iota(jnp.int32, (CHUNK, CHUNK), 1)
    return jnp.where(keys <= queries, 0.0, MASKED)


def col_bias(first, key_chunk, query_chunk):
    keys = lax.broadcasted_iota(jnp.int32, (CHUNK, CHUNK), 0)
    queries = lax.broadcasted_iota(jnp.int32, (CHUNK, CHUNK), 1)
    gap = queries - keys
    same = (gap & (GROUP - 1)) == 0
    if key_chunk == query_chunk:
        same = same & (gap > 0)
    return jnp.where(same, 0.0, MASKED)


def chunk(array, index):
    return array[index * CHUNK : (index + 1) * CHUNK]


def scores_of(query, keys, bias, query_chunk):
    out = []
    for j in range(query_chunk + 1):
        s = dot_t(chunk(keys, j), query) * (SCALE * LOG2E)
        b = bias(None, j, query_chunk)
        out.append(s if b is None else s + b)
    return out


def softmax_of(scores, values):
    top = functools.reduce(
        jnp.maximum, [jnp.max(s, axis=0, keepdims=True) for s in scores]
    )
    top = jnp.maximum(top, FLOOR)
    weights = [jnp.exp2(s - top) for s in scores]
    total = sum(jnp.sum(w, axis=0, keepdims=True) for w in weights)
    acc = sum(dot_f(chunk(values, j), w.astype(BF16)) for j, w in enumerate(weights))
    total = jnp.maximum(total, 1.0)
    return weights, top, total, acc / total


def merge(left, right):
    top = jnp.maximum(left, right)
    w_left, w_right = jnp.exp2(left - top), jnp.exp2(right - top)
    den = w_left + w_right
    return top + jnp.log2(den), w_left / den, w_right / den


def backward_of(i, probs, delta, q, k, v, g, gk, gv):
    query, grad = chunk(q, i), chunk(g, i)
    gq = None
    for j, p in enumerate(probs):
        dv = dot(p.astype(BF16), grad)
        dp = dot_t(chunk(v, j), grad)
        ds = (p * (dp - delta)).astype(BF16)
        dk = dot(ds, query)
        dq = dot_f(chunk(k, j), ds)
        gv[j] = dv if gv[j] is None else gv[j] + dv
        gk[j] = dk if gk[j] is None else gk[j] + dk
        gq = dq if gq is None else gq + dq
    return (gq * SCALE).T


def row_forward_kernel(q_ref, k_ref, v_ref, g_ref, o_ref, lse_ref, dot_ref):
    q, k, v, g = q_ref[0], k_ref[0], v_ref[0], g_ref[0]
    for i in range(q.shape[0] // CHUNK):
        span = slice(i * CHUNK, (i + 1) * CHUNK)
        _, top, total, out = softmax_of(scores_of(chunk(q, i), k, row_bias, i), v)
        o_ref[0, 0, :, span] = out
        lse_ref[0, 0, :, span] = top + jnp.log2(total)
        grad_t = chunk(g, i).astype(F32).T
        dot_ref[0, 0, :, span] = jnp.sum(grad_t * out, axis=0, keepdims=True)


def row_forward(q, k, v, g):
    rows, length, width = q.shape
    heads = width // HEAD_DIM
    block = pl.BlockSpec((1, length, HEAD_DIM), lambda r, h: (r, 0, h))
    stat = pl.BlockSpec((1, 1, 1, length), lambda r, h: (r, h, 0, 0))
    stat_shape = jax.ShapeDtypeStruct((rows, heads, 1, length), F32)
    return pl.pallas_call(
        row_forward_kernel,
        grid=(rows, heads),
        in_specs=[block] * 4,
        out_specs=[
            pl.BlockSpec((1, 1, HEAD_DIM, length), lambda r, h: (r, h, 0, 0)),
            stat,
            stat,
        ],
        out_shape=[
            jax.ShapeDtypeStruct((rows, heads, HEAD_DIM, length), F32),
            stat_shape,
            stat_shape,
        ],
        cost_estimate=pl.CostEstimate(
            flops=rows * heads * length * length * HEAD_DIM * 8,
            bytes_accessed=rows * length * width * 12,
            transcendentals=rows * heads * length * length,
        ),
        name="row_forward",
    )(q, k, v, g)


def col_kernel(x_ref, stat_ref, y_ref, lse_ref):
    devices, _, _, per, width = x_ref.shape
    tokens = devices * per
    chunks = tokens // CHUNK
    q, k, v, g = [x_ref[:, a, 0].reshape(tokens, width) for a in range(4)]
    gk, gv = [None] * chunks, [None] * chunks
    slab = CHUNK // per
    for i in range(chunks):
        span = slice(i * CHUNK, (i + 1) * CHUNK)
        here = slice(i * slab, (i + 1) * slab)
        weights, top, total, out = softmax_of(scores_of(chunk(q, i), k, col_bias, i), v)
        lse_col = top + jnp.log2(total)
        lse_ref[0, 0, :, span] = lse_col
        out_low = out.T.astype(BF16)
        y_ref[here, 0, 0] = out_low.reshape(slab, per, width)
        lse, w_row, w_col = merge(stat_ref[0, 0, 0, :, span], lse_col)
        dot_col = jnp.sum(
            (chunk(g, i).astype(F32) * out_low.astype(F32)).T, axis=0, keepdims=True
        )
        delta = w_row * stat_ref[1, 0, 0, :, span] + w_col * dot_col
        factor = jnp.exp2(top - lse)
        probs = [w * factor for w in weights]
        gq = backward_of(i, probs, delta, q, k, v, g, gk, gv)
        y_ref[here, 1, 0] = gq.astype(BF16).reshape(slab, per, width)
    for j in range(chunks):
        here = slice(j * slab, (j + 1) * slab)
        y_ref[here, 2, 0] = (gk[j] * SCALE).astype(BF16).reshape(slab, per, width)
        y_ref[here, 3, 0] = gv[j].astype(BF16).reshape(slab, per, width)


def col_both(x, stats, first_head):
    devices, kinds, groups, per, width = x.shape
    heads = width // HEAD_DIM
    tokens = devices * per
    block = pl.BlockSpec(
        (devices, kinds, 1, per, HEAD_DIM), lambda c, h: (0, 0, c, 0, h)
    )
    return pl.pallas_call(
        col_kernel,
        grid=(groups, heads),
        in_specs=[
            block,
            pl.BlockSpec((2, 1, 1, 1, tokens), lambda c, h: (0, first_head + h, c, 0, 0)),
        ],
        out_specs=[block, pl.BlockSpec((1, 1, 1, tokens), lambda c, h: (h, c, 0, 0))],
        out_shape=[
            jax.ShapeDtypeStruct(x.shape, BF16),
            jax.ShapeDtypeStruct((heads, groups, 1, tokens), F32),
        ],
        cost_estimate=pl.CostEstimate(
            flops=groups * heads * tokens * tokens * HEAD_DIM * 20,
            bytes_accessed=x.size * 4,
            transcendentals=groups * heads * tokens * tokens,
        ),
        name="col_both",
    )(x, stats)


def row_backward_kernel(
    q_ref, k_ref, v_ref, g_ref, o_ref, lse_ref, back_ref, lse_col_ref, *rest
):
    att_ref, gq_ref, gk_ref, gv_ref = rest[-4:]
    q, k, v, g = q_ref[0], k_ref[0], v_ref[0], g_ref[0]
    length = q.shape[0]
    chunks = length // CHUNK
    devices = back_ref.shape[0]
    slab = devices // chunks

    def came_back(kind, i):
        part = back_ref[i * slab : (i + 1) * slab, kind, :, 0].astype(F32)
        return part.reshape(CHUNK, HEAD_DIM)

    gk, gv = [None] * chunks, [None] * chunks
    for i in range(chunks):
        span = slice(i * CHUNK, (i + 1) * CHUNK)
        lse, w_row, w_col = merge(lse_ref[0, 0, :, span], lse_col_ref[0, 0, :, span])
        col_t = came_back(0, i).T
        att_t = o_ref[0, 0, :, span] * w_row + col_t * w_col
        low = att_t.T.astype(BF16)
        att_ref[0, span, :] = low
        delta = jnp.sum(
            (chunk(g, i).astype(F32) * low.astype(F32)).T, axis=0, keepdims=True
        )
        scores = scores_of(chunk(q, i), k, row_bias, i)
        probs = [jnp.exp2(s - lse) for s in scores]
        gq = backward_of(i, probs, delta, q, k, v, g, gk, gv)
        gq_ref[0, span, :] = (gq + came_back(1, i)).astype(BF16)
    for j in range(chunks):
        span = slice(j * CHUNK, (j + 1) * CHUNK)
        gk_ref[0, span, :] = (gk[j] * SCALE + came_back(2, j)).astype(BF16)
        gv_ref[0, span, :] = (gv[j] + came_back(3, j)).astype(BF16)


def row_backward(q, k, v, g, o, lse, back, lse_col, first_head, earlier):
    rows, length, width = q.shape
    devices, kinds, groups, _, size, piece = back.shape
    heads = piece // HEAD_DIM
    block = pl.BlockSpec((1, length, HEAD_DIM), lambda r, h: (r, 0, first_head + h))
    stat = pl.BlockSpec((1, 1, 1, length), lambda r, h: (r, first_head + h, 0, 0))
    in_specs = [block] * 4 + [
        pl.BlockSpec((1, 1, HEAD_DIM, length), lambda r, h: (r, first_head + h, 0, 0)),
        stat,
        pl.BlockSpec(
            (devices, kinds, groups, 1, size, HEAD_DIM), lambda r, h: (0, 0, 0, r, 0, h)
        ),
        stat,
    ]
    aliases = {}
    if earlier:
        aliases = {len(in_specs) + n: n for n in range(4)}
        in_specs = in_specs + [pl.BlockSpec(memory_space=pl.ANY)] * 4
    return pl.pallas_call(
        row_backward_kernel,
        grid=(rows, heads),
        in_specs=in_specs,
        out_specs=[block] * 4,
        out_shape=[jax.ShapeDtypeStruct(q.shape, BF16)] * 4,
        input_output_aliases=aliases,
        cost_estimate=pl.CostEstimate(
            flops=rows * heads * length * length * HEAD_DIM * 14,
            bytes_accessed=rows * length * piece * 28,
            transcendentals=rows * heads * length * length,
        ),
        name="row_backward",
    )(q, k, v, g, o, lse, back, lse_col, *earlier)


def exchange(array):
    return lax.all_to_all(array, "seq", split_axis=0, concat_axis=0, tiled=True)


def by_all_to_all(queries, key_vectors, value_vectors, grad_output):
    devices = lax.axis_size("seq")
    rows = queries.shape[0] // ROW_LEN
    width = queries.shape[1]
    heads = width // HEAD_DIM
    groups = ROW_LEN // devices // GROUP
    per = rows * GROUP
    tokens = devices * per
    piece = width // PIECES
    piece_heads = piece // HEAD_DIM
    arrays = (queries, key_vectors, value_vectors, grad_output)
    by_row = [a.reshape(rows, ROW_LEN, width) for a in arrays]

    packs = []
    for n in range(PIECES):
        parts = [
            jnp.transpose(
                a[:, n * piece : (n + 1) * piece].reshape(rows, devices, groups, GROUP, piece),
                (1, 2, 0, 3, 4),
            )
            for a in arrays
        ]
        packed = jnp.stack(parts, axis=1).reshape(devices, 4, groups, per, piece)
        packs.append(packed)
    arrived = [exchange(packs[0])]

    o, lse, dots = row_forward(*by_row)
    stats = jnp.stack([lse, dots]).reshape(2, rows, heads, devices, groups, GROUP)
    stats = jnp.transpose(stats, (3, 0, 2, 4, 1, 5)).reshape(devices, -1)
    arrived[0], stats = lax.optimization_barrier((arrived[0], stats))
    stats = exchange(stats)
    for n in range(1, PIECES):
        packs[n], stats = lax.optimization_barrier((packs[n], stats))
        arrived.append(exchange(packs[n]))
    stats = stats.reshape(devices, 2, heads, groups, per)
    stats = jnp.transpose(stats, (1, 2, 3, 0, 4)).reshape(2, heads, groups, 1, tokens)

    columns = [col_both(arrived[n], stats, n * piece_heads) for n in range(PIECES)]
    lse_col = jnp.concatenate([lse_col for _, lse_col in columns], axis=0)
    lse_col = jnp.transpose(
        lse_col.reshape(heads, groups, devices, per), (2, 0, 1, 3)
    ).reshape(devices, -1)
    lse_col = exchange(lse_col)
    sent = [y for y, _ in columns]
    sent[-1], lse_col = lax.optimization_barrier((sent[-1], lse_col))
    lse_col = lse_col.reshape(devices, heads, groups, rows, GROUP)
    lse_col = jnp.transpose(lse_col, (3, 1, 0, 2, 4)).reshape(rows, heads, 1, ROW_LEN)
    backs = [exchange(y).reshape(devices, 4, groups, rows, GROUP, piece) for y in sent]

    outs = ()
    for n in range(PIECES):
        outs = row_backward(*by_row, o, lse, backs[n], lse_col, n * piece_heads, tuple(outs))
    return tuple(a.reshape(queries.shape) for a in outs)


PLANES = 4
SPLITS = 4
LANES = 128


def drain(ref, sem):
    pltpu.make_async_copy(ref, ref, sem).wait()


def fold_lanes(x):
    for shift in (8, 16, 32, 64):
        x = x + pltpu.roll(x, shift, 1)
    return x


def lane_masks():
    group = lax.broadcasted_iota(jnp.int32, (LANES // GROUP, LANES), 1) // GROUP
    row = lax.broadcasted_iota(jnp.int32, (LANES // GROUP, LANES), 0)
    return group, group == row


def to_tile(stat, block):
    group, diagonal = lane_masks()
    spread = fold_lanes(jnp.where(group == block, stat, 0.0))
    return jnp.sum(jnp.where(diagonal, spread, 0.0), axis=0, keepdims=True)


def from_tile(line, block):
    group, diagonal = lane_masks()
    spread = fold_lanes(jnp.where(diagonal, line, 0.0))
    return jnp.where(group == block, spread, 0.0)


def column_unit(q, g, keys, values, query_chunk, lse_row, dot_row):
    count = len(keys)
    scores = []
    for j in range(count):
        bias = col_bias(None, j, count - 1)
        scores.append(dot_t(keys[j], q) * (SCALE * LOG2E) + bias)
    top = functools.reduce(
        jnp.maximum, [jnp.max(s, axis=0, keepdims=True) for s in scores]
    )
    top = jnp.maximum(top, FLOOR)
    weights = [jnp.exp2(s - top) for s in scores]
    total = sum(jnp.sum(w, axis=0, keepdims=True) for w in weights)
    acc = sum(dot_f(v, w.astype(BF16)) for v, w in zip(values, weights))
    total = jnp.maximum(total, 1.0)
    out_low = (acc / total).T.astype(BF16)
    lse_col = top + jnp.log2(total)
    lse, w_row, w_col = merge(lse_row, lse_col)
    dot_col = jnp.sum(
        (g.astype(F32) * out_low.astype(F32)).T, axis=0, keepdims=True
    )
    delta = w_row * dot_row + w_col * dot_col
    factor = jnp.exp2(top - lse)
    gq, gk, gv = None, [], []
    for j in range(count):
        p = weights[j] * factor
        gv.append(dot(p.astype(BF16), g))
        dp = dot_t(values[j], g)
        ds = (p * (dp - delta)).astype(BF16)
        gk.append(dot(ds, q) * SCALE)
        dq = dot_f(keys[j], ds)
        gq = dq if gq is None else gq + dq
    return out_low, (gq * SCALE).T.astype(BF16), gk, gv, lse_col


def fused_kernel(*refs):
    xs, flat, outs = refs[0:4], refs[4:8], refs[8:12]
    (xin, own, far, low, back, orow, st_row, st_own, st_far, lse_own, lse_far,
     lse_back, in_sem, a_loc, a_send, a_recv, b_send, bkv_recv, bqg_recv,
     k1_send, k1_recv, k0_send, k0_recv, d2_send, d2_recv, d1_send, d1_recv,
     e_send, e_recv, s_send, s_recv, sf_send, sf_recv, l1_send, l1_recv,
     le_send, le_recv, out_sem) = refs[12:]
    heads, _, rows = xin.shape[:3]
    chunks = own.shape[0]
    plane_rows, per = own.shape[2], own.shape[3]
    splits = chunks // heads
    devices = lax.axis_size("seq")
    m = devices // PLANES
    blocks = per * splits
    seq, head_index = lax.axis_index("seq"), lax.axis_index("head")
    z, p = seq // m, seq % m
    first = z * m

    def send(src, dst, send_sem, recv_sem, to):
        pltpu.make_async_remote_copy(
            src_ref=src, dst_ref=dst, send_sem=send_sem, recv_sem=recv_sem,
            device_id=(to, head_index), device_id_type=pl.DeviceIdType.MESH,
        ).start()

    outer = (z == 0) | (z == PLANES - 1)
    inner_peer = jnp.where(z == 0, seq + m, seq - m)
    outer_peer = jnp.where(z == 1, seq - m, seq + m)

    barrier = pltpu.get_barrier_semaphore()
    for d in range(1, m):
        pl.semaphore_signal(barrier, inc=1, device_id=(first + (p + d) % m, head_index),
                            device_id_type=pl.DeviceIdType.MESH)
    for d in range(1, PLANES):
        pl.semaphore_signal(barrier, inc=1,
                            device_id=((z + d) % PLANES * m + p, head_index),
                            device_id_type=pl.DeviceIdType.MESH)

    def lanes_of(h):
        return pl.ds(pl.multiple_of(h * HEAD_DIM, HEAD_DIM), HEAD_DIM)

    def load_rows(h, carry):
        for kind in range(4):
            pltpu.make_async_copy(
                flat[kind].at[:, :, lanes_of(h)], xin.at[h, kind], in_sem.at[h]
            ).start()
        return carry

    load_rows(0, 0)
    pl.semaphore_wait(barrier, m - 1 + PLANES - 1)

    def spread_chunk(c, carry):
        h, part = c // splits, c % splits
        for d in range(1, m):
            peer = (p + d) % m
            for kind in range(4):
                send(
                    xs[kind].at[:, pl.ds(peer * blocks + part * per, per), :, lanes_of(h)],
                    own.at[c, kind, pl.ds(p * rows, rows)],
                    a_send, a_recv.at[c], first + peer,
                )
        for kind in range(4):
            pltpu.make_async_copy(
                xs[kind].at[:, pl.ds(p * blocks + part * per, per), :, lanes_of(h)],
                own.at[c, kind, pl.ds(p * rows, rows)],
                a_loc.at[c],
            ).start()
        return carry

    lax.fori_loop(0, chunks, spread_chunk, 0)
    lax.fori_loop(1, heads, load_rows, 0)

    def forward_row(h, r):
        q, k, v, g = [xin[h, kind, r] for kind in range(4)]
        for i in range(q.shape[0] // CHUNK):
            span = slice(i * CHUNK, (i + 1) * CHUNK)
            _, top, total, out = softmax_of(scores_of(chunk(q, i), k, row_bias, i), v)
            orow[h, r, :, span] = out
            lse = top + jnp.log2(total)
            grad_t = chunk(g, i).astype(F32).T
            dots = jnp.sum(grad_t * out, axis=0, keepdims=True)
            for part in range(CHUNK // LANES):
                lanes = slice(part * LANES, (part + 1) * LANES)
                at = i * (CHUNK // LANES) + part
                st_row[2 * h, at, pl.ds(r, 1), :] = lse[:, lanes]
                st_row[2 * h + 1, at, pl.ds(r, 1), :] = dots[:, lanes]

    def forward_head(h):
        drain(xin.at[h], in_sem.at[h])

        def body(r, carry):
            forward_row(h, r)
            return carry

        lax.fori_loop(0, rows, body, 0)

    def send_stats():
        for d in range(1, m):
            peer = (p + d) % m
            send(st_row.at[:, peer], st_own.at[:, p], s_send, s_recv, first + peer)
        st_own[:, p] = st_row[:, p]

        @pl.when(outer)
        def _():
            drain(st_own.at[:, pl.ds(0, m - 1)], s_recv)
            send(st_own, st_far, sf_send, sf_recv, inner_peer)

    def wait_stats():
        drain(st_own.at[:, pl.ds(0, m - 1)], s_recv)
        drain(st_far, sf_recv)

    def tile(ref, *at):
        return ref[at].reshape(plane_rows * GROUP, HEAD_DIM)

    def put(ref, at, value):
        ref[at] = value.astype(BF16).reshape(plane_rows, GROUP, HEAD_DIM)

    def stat_of(ref, which, block):
        return to_tile(ref[which].reshape(plane_rows, LANES), block)

    def add_lse(ref, h, line, block):
        ref[h] = ref[h] + from_tile(line, block).reshape(m, rows, LANES)

    half = plane_rows * GROUP

    def solve(c, lower):
        h, part = c // splits, c % splits
        pair = (far, own) if lower else (own, far)
        lses = (lse_far, lse_own) if lower else (lse_own, lse_far)
        stats = (st_far, st_own) if lower else (st_own, st_far)

        @pl.when(part == 0)
        def _():
            lse_own[h] = jnp.zeros(lse_own.shape[1:], F32)
            lse_far[h] = jnp.zeros(lse_far.shape[1:], F32)

        def body(b, carry):
            block = part * per + b
            every = slice(None)

            def both(kind):
                return jnp.concatenate([tile(ref, c, kind, every, b) for ref in pair], axis=0)

            q, k, v, g = [both(kind) for kind in range(4)]
            keys, values = [k], [v]
            if not lower:
                keys = [jnp.concatenate([tile(low, c, 0, every, b), tile(low, c, 2, every, b)], axis=0), k]
                values = [jnp.concatenate([tile(low, c, 1, every, b), tile(low, c, 3, every, b)], axis=0), v]
            lse_row = jnp.concatenate([stat_of(s, 2 * h, block) for s in stats], axis=1)
            dot_row = jnp.concatenate([stat_of(s, 2 * h + 1, block) for s in stats], axis=1)
            o, gq, gk, gv, lse_col = column_unit(q, g, keys, values, None, lse_row, dot_row)
            gk_own, gv_own = gk[-1], gv[-1]
            if lower:
                gk_own = gk_own + jnp.concatenate(
                    [tile(low, c, 0, every, b), tile(low, c, 2, every, b)], axis=0).astype(F32)
                gv_own = gv_own + jnp.concatenate(
                    [tile(low, c, 1, every, b), tile(low, c, 3, every, b)], axis=0).astype(F32)
            else:
                put(low, (c, 0, every, b), gk[0][:half])
                put(low, (c, 1, every, b), gv[0][:half])
                put(low, (c, 2, every, b), gk[0][half:])
                put(low, (c, 3, every, b), gv[0][half:])
            for n, ref in enumerate(pair):
                span = slice(n * half, (n + 1) * half)
                for kind, value in enumerate((o, gq, gk_own, gv_own)):
                    put(ref, (c, kind, every, b), value[span])
                add_lse(lses[n], h, lse_col[:, span], block)
            return carry

        lax.fori_loop(0, per, body, 0)

    def return_rows(c, ref):
        h, part = c // splits, c % splits
        at = pl.ds(p * blocks + part * per, per)
        for d in range(1, m):
            peer = (p + d) % m
            send(
                ref.at[c, :, pl.ds(peer * rows, rows)], back.at[h, :, :, at],
                e_send, e_recv.at[h], first + peer,
            )
        back[h, :, :, at] = ref[c, :, pl.ds(p * rows, rows)]

        @pl.when(part == splits - 1)
        def _():
            for d in range(1, m):
                peer = (p + d) % m
                send(lse_own.at[h, peer], lse_back.at[h, p], le_send, le_recv.at[h], first + peer)
            lse_back[h, p] = lse_own[h, p]

    def return_far(c):
        h, part = c // splits, c % splits
        send(far.at[c], far.at[c], d1_send, d1_recv.at[c], outer_peer)

        @pl.when(part == splits - 1)
        def _():
            send(lse_far.at[h], lse_own.at[h], l1_send, l1_recv.at[h], outer_peer)

    def pass_on(c):
        drain(own.at[c, :, pl.ds(0, rows * (m - 1))], a_recv.at[c])
        drain(own.at[c, :, pl.ds(0, rows)], a_loc.at[c])

        @pl.when(outer)
        def _():
            send(own.at[c, pl.ds(1, 2)], far.at[c, pl.ds(1, 2)], b_send, bkv_recv.at[c], inner_peer)
            send(own.at[c, 0], far.at[c, 0], b_send, bqg_recv.at[c, 0], inner_peer)
            send(own.at[c, 3], far.at[c, 3], b_send, bqg_recv.at[c, 1], inner_peer)

        @pl.when(z == 1)
        def _():
            send(own.at[c, pl.ds(1, 2)], low.at[c, pl.ds(2, 2)], k1_send.at[c], k1_recv.at[c], seq + m)

    def pass_far(c):
        drain(far.at[c, pl.ds(1, 2)], bkv_recv.at[c])
        send(far.at[c, pl.ds(1, 2)], low.at[c, pl.ds(0, 2)], k0_send.at[c], k0_recv.at[c], seq + m)

    def wait_qg(c):
        drain(far.at[c, 0], bqg_recv.at[c, 0])
        drain(far.at[c, 3], bqg_recv.at[c, 1])

    def upper(c):
        drain(far.at[c, pl.ds(1, 2)], bkv_recv.at[c])
        wait_qg(c)
        drain(low.at[c, pl.ds(2, 2)], k1_recv.at[c])
        drain(low.at[c, pl.ds(0, 2)], k0_recv.at[c])
        solve(c, False)
        send(low.at[c], low.at[c], d2_send, d2_recv.at[c], seq - m)
        return_far(c)
        return_rows(c, own)

    def lower(c):
        wait_qg(c)
        drain(low.at[c], d2_recv.at[c])
        drain(own.at[c, pl.ds(1, 2)], k1_send.at[c])
        drain(far.at[c, pl.ds(1, 2)], k0_send.at[c])
        solve(c, True)
        return_far(c)
        return_rows(c, own)

    def edge(c):
        h, part = c // splits, c % splits
        drain(far.at[c], d1_recv.at[c])

        @pl.when(part == splits - 1)
        def _():
            drain(lse_own.at[h], l1_recv.at[h])

        return_rows(c, far)

    def backward_row(h, r):
        q, k, v, g = [xin[h, kind, r] for kind in range(4)]
        count = q.shape[0] // CHUNK
        slab = CHUNK // GROUP

        def came_back(kind, i):
            return back[h, kind, r, i * slab:(i + 1) * slab].reshape(CHUNK, HEAD_DIM).astype(F32)

        def give(kind, i, value):
            back[h, kind, r, i * slab:(i + 1) * slab] = value.astype(BF16).reshape(slab, GROUP, HEAD_DIM)

        def line(ref, lead, i):
            base = i * (CHUNK // LANES)
            return jnp.concatenate(
                [ref[lead, base + n, pl.ds(r, 1), :] for n in range(CHUNK // LANES)], axis=1)

        gk, gv = [None] * count, [None] * count
        for i in range(count):
            span = slice(i * CHUNK, (i + 1) * CHUNK)
            lse, w_row, w_col = merge(line(st_row, 2 * h, i), line(lse_back, h, i))
            att_t = orow[h, r, :, span] * w_row + came_back(0, i).T * w_col
            att = att_t.T.astype(BF16)
            give(0, i, att)
            delta = jnp.sum(
                (chunk(g, i).astype(F32) * att.astype(F32)).T, axis=0, keepdims=True
            )
            scores = scores_of(chunk(q, i), k, row_bias, i)
            probs = [jnp.exp2(s - lse) for s in scores]
            gq = backward_of(i, probs, delta, q, k, v, g, gk, gv)
            give(1, i, gq + came_back(1, i))
        for j in range(count):
            give(2, j, gk[j] * SCALE + came_back(2, j))
            give(3, j, gv[j] + came_back(3, j))

    def backward_head(h):
        drain(back.at[h, :, :, pl.ds(0, blocks * (m - 1))], e_recv.at[h])
        drain(lse_back.at[h, pl.ds(0, m - 1)], le_recv.at[h])

        def body(r, carry):
            backward_row(h, r)
            return carry

        lax.fori_loop(0, rows, body, 0)
        for kind in range(4):
            pltpu.make_async_copy(
                back.at[h, kind], outs[kind].at[:, :, :, lanes_of(h)], out_sem
            ).start()

    lag_upper, lag_lower, lag_edge, lag_rows = LAGS

    def step(s, carry):
        def at(lag, role=None):
            ready = (s >= lag) & (s < chunks + lag)
            return ready if role is None else ready & role

        @pl.when(s < heads)
        def _():
            forward_head(s)

        @pl.when(s == heads - 1)
        def _():
            send_stats()

        @pl.when(at(0))
        def _():
            pass_on(s)

        @pl.when(at(1, z == 1))
        def _():
            pass_far(s - 1)

        @pl.when((s == lag_upper) & ((z == 1) | (z == 2)))
        def _():
            wait_stats()

        @pl.when(at(lag_upper, z == 2))
        def _():
            upper(s - lag_upper)

        @pl.when(at(lag_lower, z == 1))
        def _():
            lower(s - lag_lower)

        @pl.when(at(lag_edge, outer))
        def _():
            edge(s - lag_edge)

        done = s - lag_rows

        @pl.when((done >= 0) & (done % splits == splits - 1))
        def _():
            backward_head(done // splits)

        return carry

    lax.fori_loop(0, chunks + lag_rows, step, 0)

    drain(own.at[:, :, pl.ds(0, rows * (m - 1))], a_send)
    drain(own.at[:, :, pl.ds(0, rows * (m - 1))], e_send)
    drain(st_own.at[:, pl.ds(0, m - 1)], s_send)
    drain(lse_own.at[:, pl.ds(0, m - 1)], le_send)

    @pl.when(outer)
    def _():
        drain(own, b_send)
        drain(st_far, sf_send)

    @pl.when((z == 1) | (z == 2))
    def _():
        drain(far, d1_send)
        drain(lse_far, l1_send)

    @pl.when(z == 2)
    def _():
        drain(low, d2_send)

    drain(back, out_sem)


LAGS = (3, 6, 8, 11)


def fits(tokens, width, devices):
    rows = tokens // ROW_LEN
    if tokens % ROW_LEN or devices % PLANES or width % HEAD_DIM:
        return False
    m = devices // PLANES
    blocks = ROW_LEN // GROUP
    return (
        m > 1
        and ROW_LEN // m == LANES
        and rows * m * GROUP == LANES
        and (blocks // m) % SPLITS == 0
    )


def by_planes(queries, key_vectors, value_vectors, grad_output):
    devices = lax.axis_size("seq")
    m = devices // PLANES
    tokens, width = queries.shape
    rows, heads, blocks = tokens // ROW_LEN, width // HEAD_DIM, ROW_LEN // GROUP
    per = blocks // m // SPLITS
    chunks = heads * SPLITS
    arrays = (queries, key_vectors, value_vectors, grad_output)
    views = [a.reshape(rows, blocks, GROUP, width) for a in arrays]
    flat = [a.reshape(rows, ROW_LEN, width) for a in arrays]
    buffer = pltpu.VMEM((chunks, 4, rows * m, per, GROUP, HEAD_DIM), BF16)
    dma = pltpu.SemaphoreType.DMA
    stat = pltpu.VMEM((2 * heads, m, rows, LANES), F32)
    lse = pltpu.VMEM((heads, m, rows, LANES), F32)
    each, single = dma((chunks,)), dma(())
    outs = pl.pallas_call(
        fused_kernel,
        in_specs=[pl.BlockSpec(memory_space=pl.ANY)] * 8,
        out_specs=[pl.BlockSpec(memory_space=pl.ANY)] * 4,
        out_shape=[jax.ShapeDtypeStruct(views[0].shape, BF16)] * 4,
        scratch_shapes=[
            pltpu.VMEM((heads, 4, rows, ROW_LEN, HEAD_DIM), BF16),
            buffer, buffer, buffer,
            pltpu.VMEM((heads, 4, rows, blocks, GROUP, HEAD_DIM), BF16),
            pltpu.VMEM((heads, rows, HEAD_DIM, ROW_LEN), F32),
            stat, stat, stat, lse, lse, lse,
            dma((heads,)), each, single, each, single, each, dma((chunks, 2)),
            each, each, each, each, single, each, single, each,
            single, dma((heads,)), single, single, single, single, single, dma((heads,)),
            single, dma((heads,)), single,
        ],
        compiler_params=pltpu.CompilerParams(
            collective_id=0, has_side_effects=True, vmem_limit_bytes=63 * 1024 * 1024
        ),
        cost_estimate=pl.CostEstimate(
            flops=tokens * width * 512 * 24,
            bytes_accessed=tokens * width * 16,
            transcendentals=tokens * width,
        ),
        name="by_planes",
    )(*views, *flat)
    return tuple(a.reshape(queries.shape) for a in outs)


def on_device(queries, key_vectors, value_vectors, grad_output):
    arrays = (queries, key_vectors, value_vectors, grad_output)
    if fits(*queries.shape, lax.axis_size("seq")):
        return by_planes(*arrays)
    return by_all_to_all(*arrays)


def solution(mesh):
    spec = P("seq", "head")
    return jax.shard_map(
        on_device,
        mesh=mesh,
        in_specs=(spec,) * 4,
        out_specs=(spec,) * 4,
        check_vma=False,
    )
```

```python
import functools
import math

import jax
import jax.numpy as jnp
from jax import lax
from jax.experimental import pallas as pl
from jax.experimental.pallas import tpu as pltpu
from jax.sharding import PartitionSpec as P

ROW_LEN = 512
HEAD_DIM = 128
GROUP = 8
CHUNK = 256
PIECES = 2
MASKED = -1e30
FLOOR = -1e20
LOG2E = 1.0 / math.log(2.0)
SCALE = 1.0 / math.sqrt(HEAD_DIM)
F32 = jnp.float32
BF16 = jnp.bfloat16


def dot_t(left, right):
    return lax.dot_general(left, right, (((1,), (1,)), ((), ())), preferred_element_type=F32)


def dot_f(left, right):
    return lax.dot_general(left, right, (((0,), (0,)), ((), ())), preferred_element_type=F32)


def dot(left, right):
    return jnp.dot(left, right, preferred_element_type=F32)


def row_bias(first, key_chunk, query_chunk):
    if key_chunk < query_chunk:
        return None
    keys = lax.broadcasted_iota(jnp.int32, (CHUNK, CHUNK), 0)
    queries = lax.broadcasted_iota(jnp.int32, (CHUNK, CHUNK), 1)
    return jnp.where(keys <= queries, 0.0, MASKED)


def col_bias(first, key_chunk, query_chunk):
    keys = lax.broadcasted_iota(jnp.int32, (CHUNK, CHUNK), 0)
    queries = lax.broadcasted_iota(jnp.int32, (CHUNK, CHUNK), 1)
    gap = queries - keys
    same = (gap & (GROUP - 1)) == 0
    if key_chunk == query_chunk:
        same = same & (gap > 0)
    return jnp.where(same, 0.0, MASKED)


def chunk(array, index):
    return array[index * CHUNK : (index + 1) * CHUNK]


def scores_of(query, keys, bias, query_chunk):
    out = []
    for j in range(query_chunk + 1):
        s = dot_t(chunk(keys, j), query) * (SCALE * LOG2E)
        b = bias(None, j, query_chunk)
        out.append(s if b is None else s + b)
    return out


def softmax_of(scores, values):
    top = functools.reduce(
        jnp.maximum, [jnp.max(s, axis=0, keepdims=True) for s in scores]
    )
    top = jnp.maximum(top, FLOOR)
    weights = [jnp.exp2(s - top) for s in scores]
    total = sum(jnp.sum(w, axis=0, keepdims=True) for w in weights)
    acc = sum(dot_f(chunk(values, j), w.astype(BF16)) for j, w in enumerate(weights))
    total = jnp.maximum(total, 1.0)
    return weights, top, total, acc / total


def merge(left, right):
    top = jnp.maximum(left, right)
    w_left, w_right = jnp.exp2(left - top), jnp.exp2(right - top)
    den = w_left + w_right
    return top + jnp.log2(den), w_left / den, w_right / den


def backward_of(i, probs, delta, q, k, v, g, gk, gv):
    query, grad = chunk(q, i), chunk(g, i)
    gq = None
    for j, p in enumerate(probs):
        dv = dot(p.astype(BF16), grad)
        dp = dot_t(chunk(v, j), grad)
        ds = (p * (dp - delta)).astype(BF16)
        dk = dot(ds, query)
        dq = dot_f(chunk(k, j), ds)
        gv[j] = dv if gv[j] is None else gv[j] + dv
        gk[j] = dk if gk[j] is None else gk[j] + dk
        gq = dq if gq is None else gq + dq
    return (gq * SCALE).T


def row_forward_kernel(q_ref, k_ref, v_ref, g_ref, o_ref, lse_ref, dot_ref):
    q, k, v, g = q_ref[0], k_ref[0], v_ref[0], g_ref[0]
    for i in range(q.shape[0] // CHUNK):
        span = slice(i * CHUNK, (i + 1) * CHUNK)
        _, top, total, out = softmax_of(scores_of(chunk(q, i), k, row_bias, i), v)
        o_ref[0, 0, :, span] = out
        lse_ref[0, 0, :, span] = top + jnp.log2(total)
        grad_t = chunk(g, i).astype(F32).T
        dot_ref[0, 0, :, span] = jnp.sum(grad_t * out, axis=0, keepdims=True)


def row_forward(q, k, v, g):
    rows, length, width = q.shape
    heads = width // HEAD_DIM
    block = pl.BlockSpec((1, length, HEAD_DIM), lambda r, h: (r, 0, h))
    stat = pl.BlockSpec((1, 1, 1, length), lambda r, h: (r, h, 0, 0))
    stat_shape = jax.ShapeDtypeStruct((rows, heads, 1, length), F32)
    return pl.pallas_call(
        row_forward_kernel,
        grid=(rows, heads),
        in_specs=[block] * 4,
        out_specs=[
            pl.BlockSpec((1, 1, HEAD_DIM, length), lambda r, h: (r, h, 0, 0)),
            stat,
            stat,
        ],
        out_shape=[
            jax.ShapeDtypeStruct((rows, heads, HEAD_DIM, length), F32),
            stat_shape,
            stat_shape,
        ],
        cost_estimate=pl.CostEstimate(
            flops=rows * heads * length * length * HEAD_DIM * 8,
            bytes_accessed=rows * length * width * 12,
            transcendentals=rows * heads * length * length,
        ),
        name="row_forward",
    )(q, k, v, g)


def col_kernel(x_ref, stat_ref, y_ref, lse_ref):
    devices, _, _, per, width = x_ref.shape
    tokens = devices * per
    chunks = tokens // CHUNK
    q, k, v, g = [x_ref[:, a, 0].reshape(tokens, width) for a in range(4)]
    gk, gv = [None] * chunks, [None] * chunks
    slab = CHUNK // per
    for i in range(chunks):
        span = slice(i * CHUNK, (i + 1) * CHUNK)
        here = slice(i * slab, (i + 1) * slab)
        weights, top, total, out = softmax_of(scores_of(chunk(q, i), k, col_bias, i), v)
        lse_col = top + jnp.log2(total)
        lse_ref[0, 0, :, span] = lse_col
        out_low = out.T.astype(BF16)
        y_ref[here, 0, 0] = out_low.reshape(slab, per, width)
        lse, w_row, w_col = merge(stat_ref[0, 0, 0, :, span], lse_col)
        dot_col = jnp.sum(
            (chunk(g, i).astype(F32) * out_low.astype(F32)).T, axis=0, keepdims=True
        )
        delta = w_row * stat_ref[1, 0, 0, :, span] + w_col * dot_col
        factor = jnp.exp2(top - lse)
        probs = [w * factor for w in weights]
        gq = backward_of(i, probs, delta, q, k, v, g, gk, gv)
        y_ref[here, 1, 0] = gq.astype(BF16).reshape(slab, per, width)
    for j in range(chunks):
        here = slice(j * slab, (j + 1) * slab)
        y_ref[here, 2, 0] = (gk[j] * SCALE).astype(BF16).reshape(slab, per, width)
        y_ref[here, 3, 0] = gv[j].astype(BF16).reshape(slab, per, width)


def col_both(x, stats, first_head):
    devices, kinds, groups, per, width = x.shape
    heads = width // HEAD_DIM
    tokens = devices * per
    block = pl.BlockSpec(
        (devices, kinds, 1, per, HEAD_DIM), lambda c, h: (0, 0, c, 0, h)
    )
    return pl.pallas_call(
        col_kernel,
        grid=(groups, heads),
        in_specs=[
            block,
            pl.BlockSpec((2, 1, 1, 1, tokens), lambda c, h: (0, first_head + h, c, 0, 0)),
        ],
        out_specs=[block, pl.BlockSpec((1, 1, 1, tokens), lambda c, h: (h, c, 0, 0))],
        out_shape=[
            jax.ShapeDtypeStruct(x.shape, BF16),
            jax.ShapeDtypeStruct((heads, groups, 1, tokens), F32),
        ],
        cost_estimate=pl.CostEstimate(
            flops=groups * heads * tokens * tokens * HEAD_DIM * 20,
            bytes_accessed=x.size * 4,
            transcendentals=groups * heads * tokens * tokens,
        ),
        name="col_both",
    )(x, stats)


def row_backward_kernel(
    q_ref, k_ref, v_ref, g_ref, o_ref, lse_ref, back_ref, lse_col_ref, *rest
):
    att_ref, gq_ref, gk_ref, gv_ref = rest[-4:]
    q, k, v, g = q_ref[0], k_ref[0], v_ref[0], g_ref[0]
    length = q.shape[0]
    chunks = length // CHUNK
    devices = back_ref.shape[0]
    slab = devices // chunks

    def came_back(kind, i):
        part = back_ref[i * slab : (i + 1) * slab, kind, :, 0].astype(F32)
        return part.reshape(CHUNK, HEAD_DIM)

    gk, gv = [None] * chunks, [None] * chunks
    for i in range(chunks):
        span = slice(i * CHUNK, (i + 1) * CHUNK)
        lse, w_row, w_col = merge(lse_ref[0, 0, :, span], lse_col_ref[0, 0, :, span])
        col_t = came_back(0, i).T
        att_t = o_ref[0, 0, :, span] * w_row + col_t * w_col
        low = att_t.T.astype(BF16)
        att_ref[0, span, :] = low
        delta = jnp.sum(
            (chunk(g, i).astype(F32) * low.astype(F32)).T, axis=0, keepdims=True
        )
        scores = scores_of(chunk(q, i), k, row_bias, i)
        probs = [jnp.exp2(s - lse) for s in scores]
        gq = backward_of(i, probs, delta, q, k, v, g, gk, gv)
        gq_ref[0, span, :] = (gq + came_back(1, i)).astype(BF16)
    for j in range(chunks):
        span = slice(j * CHUNK, (j + 1) * CHUNK)
        gk_ref[0, span, :] = (gk[j] * SCALE + came_back(2, j)).astype(BF16)
        gv_ref[0, span, :] = (gv[j] + came_back(3, j)).astype(BF16)


def row_backward(q, k, v, g, o, lse, back, lse_col, first_head, earlier):
    rows, length, width = q.shape
    devices, kinds, groups, _, size, piece = back.shape
    heads = piece // HEAD_DIM
    block = pl.BlockSpec((1, length, HEAD_DIM), lambda r, h: (r, 0, first_head + h))
    stat = pl.BlockSpec((1, 1, 1, length), lambda r, h: (r, first_head + h, 0, 0))
    in_specs = [block] * 4 + [
        pl.BlockSpec((1, 1, HEAD_DIM, length), lambda r, h: (r, first_head + h, 0, 0)),
        stat,
        pl.BlockSpec(
            (devices, kinds, groups, 1, size, HEAD_DIM), lambda r, h: (0, 0, 0, r, 0, h)
        ),
        stat,
    ]
    aliases = {}
    if earlier:
        aliases = {len(in_specs) + n: n for n in range(4)}
        in_specs = in_specs + [pl.BlockSpec(memory_space=pl.ANY)] * 4
    return pl.pallas_call(
        row_backward_kernel,
        grid=(rows, heads),
        in_specs=in_specs,
        out_specs=[block] * 4,
        out_shape=[jax.ShapeDtypeStruct(q.shape, BF16)] * 4,
        input_output_aliases=aliases,
        cost_estimate=pl.CostEstimate(
            flops=rows * heads * length * length * HEAD_DIM * 14,
            bytes_accessed=rows * length * piece * 28,
            transcendentals=rows * heads * length * length,
        ),
        name="row_backward",
    )(q, k, v, g, o, lse, back, lse_col, *earlier)


def exchange(array):
    return lax.all_to_all(array, "seq", split_axis=0, concat_axis=0, tiled=True)


def by_all_to_all(queries, key_vectors, value_vectors, grad_output):
    devices = lax.axis_size("seq")
    rows = queries.shape[0] // ROW_LEN
    width = queries.shape[1]
    heads = width // HEAD_DIM
    groups = ROW_LEN // devices // GROUP
    per = rows * GROUP
    tokens = devices * per
    piece = width // PIECES
    piece_heads = piece // HEAD_DIM
    arrays = (queries, key_vectors, value_vectors, grad_output)
    by_row = [a.reshape(rows, ROW_LEN, width) for a in arrays]

    packs = []
    for n in range(PIECES):
        parts = [
            jnp.transpose(
                a[:, n * piece : (n + 1) * piece].reshape(rows, devices, groups, GROUP, piece),
                (1, 2, 0, 3, 4),
            )
            for a in arrays
        ]
        packed = jnp.stack(parts, axis=1).reshape(devices, 4, groups, per, piece)
        packs.append(packed)
    arrived = [exchange(packs[0])]

    o, lse, dots = row_forward(*by_row)
    stats = jnp.stack([lse, dots]).reshape(2, rows, heads, devices, groups, GROUP)
    stats = jnp.transpose(stats, (3, 0, 2, 4, 1, 5)).reshape(devices, -1)
    arrived[0], stats = lax.optimization_barrier((arrived[0], stats))
    stats = exchange(stats)
    for n in range(1, PIECES):
        packs[n], stats = lax.optimization_barrier((packs[n], stats))
        arrived.append(exchange(packs[n]))
    stats = stats.reshape(devices, 2, heads, groups, per)
    stats = jnp.transpose(stats, (1, 2, 3, 0, 4)).reshape(2, heads, groups, 1, tokens)

    columns = [col_both(arrived[n], stats, n * piece_heads) for n in range(PIECES)]
    lse_col = jnp.concatenate([lse_col for _, lse_col in columns], axis=0)
    lse_col = jnp.transpose(
        lse_col.reshape(heads, groups, devices, per), (2, 0, 1, 3)
    ).reshape(devices, -1)
    lse_col = exchange(lse_col)
    sent = [y for y, _ in columns]
    sent[-1], lse_col = lax.optimization_barrier((sent[-1], lse_col))
    lse_col = lse_col.reshape(devices, heads, groups, rows, GROUP)
    lse_col = jnp.transpose(lse_col, (3, 1, 0, 2, 4)).reshape(rows, heads, 1, ROW_LEN)
    backs = [exchange(y).reshape(devices, 4, groups, rows, GROUP, piece) for y in sent]

    outs = ()
    for n in range(PIECES):
        outs = row_backward(*by_row, o, lse, backs[n], lse_col, n * piece_heads, tuple(outs))
    return tuple(a.reshape(queries.shape) for a in outs)


PLANES = 4
SPLITS = 16
LANES = 128


def drain(ref, sem):
    pltpu.make_async_copy(ref, ref, sem).wait()


def fold_lanes(x):
    for shift in (8, 16, 32, 64):
        x = x + pltpu.roll(x, shift, 1)
    return x


def lane_masks():
    group = lax.broadcasted_iota(jnp.int32, (LANES // GROUP, LANES), 1) // GROUP
    row = lax.broadcasted_iota(jnp.int32, (LANES // GROUP, LANES), 0)
    return group, group == row


def to_tile(stat, block):
    group, diagonal = lane_masks()
    spread = fold_lanes(jnp.where(group == block, stat, 0.0))
    return jnp.sum(jnp.where(diagonal, spread, 0.0), axis=0, keepdims=True)


def from_tile(line, block):
    group, diagonal = lane_masks()
    spread = fold_lanes(jnp.where(diagonal, line, 0.0))
    return jnp.where(group == block, spread, 0.0)


def column_unit(q, g, keys, values, query_chunk, lse_row, dot_row):
    count = len(keys)
    scores = []
    for j in range(count):
        bias = col_bias(None, j, count - 1)
        scores.append(dot_t(keys[j], q) * (SCALE * LOG2E) + bias)
    top = functools.reduce(
        jnp.maximum, [jnp.max(s, axis=0, keepdims=True) for s in scores]
    )
    top = jnp.maximum(top, FLOOR)
    weights = [jnp.exp2(s - top) for s in scores]
    total = sum(jnp.sum(w, axis=0, keepdims=True) for w in weights)
    acc = sum(dot_f(v, w.astype(BF16)) for v, w in zip(values, weights))
    total = jnp.maximum(total, 1.0)
    out_low = (acc / total).T.astype(BF16)
    lse_col = top + jnp.log2(total)
    lse, w_row, w_col = merge(lse_row, lse_col)
    dot_col = jnp.sum(
        (g.astype(F32) * out_low.astype(F32)).T, axis=0, keepdims=True
    )
    delta = w_row * dot_row + w_col * dot_col
    factor = jnp.exp2(top - lse)
    gq, gk, gv = None, [], []
    for j in range(count):
        p = weights[j] * factor
        gv.append(dot(p.astype(BF16), g))
        dp = dot_t(values[j], g)
        ds = (p * (dp - delta)).astype(BF16)
        gk.append(dot(ds, q) * SCALE)
        dq = dot_f(keys[j], ds)
        gq = dq if gq is None else gq + dq
    return out_low, (gq * SCALE).T.astype(BF16), gk, gv, lse_col


def fused_kernel(*refs):
    xs, flat, outs = refs[0:4], refs[4:8], refs[8:12]
    (xin, own, far, low, back, orow, st_row, st_own, st_far, lse_own, lse_far,
     lse_back, in_sem, a_loc, a_send, a_recv, b_send, bkv_recv, bqg_recv,
     k1_send, k1_recv, k0_send, k0_recv, d2_send, d2_recv, d1_send, d1_recv,
     e_send, e_recv, s_send, s_recv, sf_send, sf_recv, l1_send, l1_recv,
     le_send, le_recv, out_sem) = refs[12:]
    heads, _, rows = xin.shape[:3]
    chunks = own.shape[0]
    plane_rows, per = own.shape[2], own.shape[3]
    splits = chunks // heads
    devices = lax.axis_size("seq")
    m = devices // PLANES
    blocks = per * splits
    seq, head_index = lax.axis_index("seq"), lax.axis_index("head")
    z, p = seq // m, seq % m
    first = z * m

    def send(src, dst, send_sem, recv_sem, to):
        pltpu.make_async_remote_copy(
            src_ref=src, dst_ref=dst, send_sem=send_sem, recv_sem=recv_sem,
            device_id=(to, head_index), device_id_type=pl.DeviceIdType.MESH,
        ).start()

    outer = (z == 0) | (z == PLANES - 1)
    inner_peer = jnp.where(z == 0, seq + m, seq - m)
    outer_peer = jnp.where(z == 1, seq - m, seq + m)

    barrier = pltpu.get_barrier_semaphore()
    for d in range(1, m):
        pl.semaphore_signal(barrier, inc=1, device_id=(first + (p + d) % m, head_index),
                            device_id_type=pl.DeviceIdType.MESH)
    for d in range(1, PLANES):
        pl.semaphore_signal(barrier, inc=1,
                            device_id=((z + d) % PLANES * m + p, head_index),
                            device_id_type=pl.DeviceIdType.MESH)

    def lanes_of(h):
        return pl.ds(pl.multiple_of(h * HEAD_DIM, HEAD_DIM), HEAD_DIM)

    def load_rows(h, carry):
        for kind in range(4):
            pltpu.make_async_copy(
                flat[kind].at[:, :, lanes_of(h)], xin.at[h, kind], in_sem.at[h]
            ).start()
        return carry

    load_rows(0, 0)
    pl.semaphore_wait(barrier, m - 1 + PLANES - 1)

    def spread_chunk(c, carry):
        h, part = c // splits, c % splits
        for d in range(1, m):
            peer = (p + d) % m
            for kind in range(4):
                send(
                    xs[kind].at[:, pl.ds(peer * blocks + part * per, per), :, lanes_of(h)],
                    own.at[c, kind, pl.ds(p * rows, rows)],
                    a_send, a_recv.at[c], first + peer,
                )
        for kind in range(4):
            pltpu.make_async_copy(
                xs[kind].at[:, pl.ds(p * blocks + part * per, per), :, lanes_of(h)],
                own.at[c, kind, pl.ds(p * rows, rows)],
                a_loc.at[c],
            ).start()
        return carry

    lax.fori_loop(0, AHEAD, spread_chunk, 0)
    lax.fori_loop(1, heads, load_rows, 0)

    def forward_row(h, r):
        q, k, v, g = [xin[h, kind, r] for kind in range(4)]
        for i in range(q.shape[0] // CHUNK):
            span = slice(i * CHUNK, (i + 1) * CHUNK)
            _, top, total, out = softmax_of(scores_of(chunk(q, i), k, row_bias, i), v)
            orow[h, r, :, span] = out
            lse = top + jnp.log2(total)
            grad_t = chunk(g, i).astype(F32).T
            dots = jnp.sum(grad_t * out, axis=0, keepdims=True)
            for part in range(CHUNK // LANES):
                lanes = slice(part * LANES, (part + 1) * LANES)
                at = i * (CHUNK // LANES) + part
                st_row[2 * h, at, pl.ds(r, 1), :] = lse[:, lanes]
                st_row[2 * h + 1, at, pl.ds(r, 1), :] = dots[:, lanes]

    def forward_head(h):
        drain(xin.at[h], in_sem.at[h])

        def body(r, carry):
            forward_row(h, r)
            return carry

        lax.fori_loop(0, rows, body, 0)

    def send_stats():
        for d in range(1, m):
            peer = (p + d) % m
            send(st_row.at[:, peer], st_own.at[:, p], s_send, s_recv, first + peer)
        st_own[:, p] = st_row[:, p]

        @pl.when(outer)
        def _():
            drain(st_own.at[:, pl.ds(0, m - 1)], s_recv)
            send(st_own, st_far, sf_send, sf_recv, inner_peer)

    def wait_stats():
        drain(st_own.at[:, pl.ds(0, m - 1)], s_recv)
        drain(st_far, sf_recv)

    def tile(ref, *at):
        return ref[at].reshape(plane_rows * GROUP, HEAD_DIM)

    def put(ref, at, value):
        ref[at] = value.astype(BF16).reshape(plane_rows, GROUP, HEAD_DIM)

    def stat_of(ref, which, block):
        return to_tile(ref[which].reshape(plane_rows, LANES), block)

    def add_lse(ref, h, line, block):
        ref[h] = ref[h] + from_tile(line, block).reshape(m, rows, LANES)

    half = plane_rows * GROUP

    def solve(c, lower):
        h, part = c // splits, c % splits
        pair = (far, own) if lower else (own, far)
        lses = (lse_far, lse_own) if lower else (lse_own, lse_far)
        stats = (st_far, st_own) if lower else (st_own, st_far)

        @pl.when(part == 0)
        def _():
            lse_own[h] = jnp.zeros(lse_own.shape[1:], F32)
            lse_far[h] = jnp.zeros(lse_far.shape[1:], F32)

        def body(b, carry):
            block = part * per + b
            every = slice(None)

            def both(kind):
                return jnp.concatenate([tile(ref, c, kind, every, b) for ref in pair], axis=0)

            q, k, v, g = [both(kind) for kind in range(4)]
            keys, values = [k], [v]
            if not lower:
                keys = [jnp.concatenate([tile(low, c, 0, every, b), tile(low, c, 2, every, b)], axis=0), k]
                values = [jnp.concatenate([tile(low, c, 1, every, b), tile(low, c, 3, every, b)], axis=0), v]
            lse_row = jnp.concatenate([stat_of(s, 2 * h, block) for s in stats], axis=1)
            dot_row = jnp.concatenate([stat_of(s, 2 * h + 1, block) for s in stats], axis=1)
            o, gq, gk, gv, lse_col = column_unit(q, g, keys, values, None, lse_row, dot_row)
            gk_own, gv_own = gk[-1], gv[-1]
            if lower:
                gk_own = gk_own + jnp.concatenate(
                    [tile(low, c, 0, every, b), tile(low, c, 2, every, b)], axis=0).astype(F32)
                gv_own = gv_own + jnp.concatenate(
                    [tile(low, c, 1, every, b), tile(low, c, 3, every, b)], axis=0).astype(F32)
            else:
                put(low, (c, 0, every, b), gk[0][:half])
                put(low, (c, 1, every, b), gv[0][:half])
                put(low, (c, 2, every, b), gk[0][half:])
                put(low, (c, 3, every, b), gv[0][half:])
            for n, ref in enumerate(pair):
                span = slice(n * half, (n + 1) * half)
                for kind, value in enumerate((o, gq, gk_own, gv_own)):
                    put(ref, (c, kind, every, b), value[span])
                add_lse(lses[n], h, lse_col[:, span], block)
            return carry

        lax.fori_loop(0, per, body, 0)

    def return_rows(c, ref):
        h, part = c // splits, c % splits
        at = pl.ds(p * blocks + part * per, per)
        for d in range(1, m):
            peer = (p + d) % m
            send(
                ref.at[c, :, pl.ds(peer * rows, rows)], back.at[h, :, :, at],
                e_send, e_recv.at[h], first + peer,
            )
        back[h, :, :, at] = ref[c, :, pl.ds(p * rows, rows)]

        @pl.when(part == splits - 1)
        def _():
            for d in range(1, m):
                peer = (p + d) % m
                send(lse_own.at[h, peer], lse_back.at[h, p], le_send, le_recv.at[h], first + peer)
            lse_back[h, p] = lse_own[h, p]

    def return_far(c):
        h, part = c // splits, c % splits
        send(far.at[c], far.at[c], d1_send, d1_recv.at[c], outer_peer)

        @pl.when(part == splits - 1)
        def _():
            send(lse_far.at[h], lse_own.at[h], l1_send, l1_recv.at[h], outer_peer)

    def pass_on(c):
        drain(own.at[c, :, pl.ds(0, rows * (m - 1))], a_recv.at[c])
        drain(own.at[c, :, pl.ds(0, rows)], a_loc.at[c])

        @pl.when(outer)
        def _():
            send(own.at[c, pl.ds(1, 2)], far.at[c, pl.ds(1, 2)], b_send, bkv_recv.at[c], inner_peer)
            send(own.at[c, 0], far.at[c, 0], b_send, bqg_recv.at[c, 0], inner_peer)
            send(own.at[c, 3], far.at[c, 3], b_send, bqg_recv.at[c, 1], inner_peer)

        @pl.when(z == 1)
        def _():
            send(own.at[c, pl.ds(1, 2)], low.at[c, pl.ds(2, 2)], k1_send.at[c], k1_recv.at[c], seq + m)

    def pass_far(c):
        drain(far.at[c, pl.ds(1, 2)], bkv_recv.at[c])
        send(far.at[c, pl.ds(1, 2)], low.at[c, pl.ds(0, 2)], k0_send.at[c], k0_recv.at[c], seq + m)

    def wait_qg(c):
        drain(far.at[c, 0], bqg_recv.at[c, 0])
        drain(far.at[c, 3], bqg_recv.at[c, 1])

    def upper(c):
        drain(far.at[c, pl.ds(1, 2)], bkv_recv.at[c])
        wait_qg(c)
        drain(low.at[c, pl.ds(2, 2)], k1_recv.at[c])
        drain(low.at[c, pl.ds(0, 2)], k0_recv.at[c])
        solve(c, False)
        send(low.at[c], low.at[c], d2_send, d2_recv.at[c], seq - m)
        return_far(c)
        return_rows(c, own)

    def lower(c):
        wait_qg(c)
        drain(low.at[c], d2_recv.at[c])
        drain(own.at[c, pl.ds(1, 2)], k1_send.at[c])
        drain(far.at[c, pl.ds(1, 2)], k0_send.at[c])
        solve(c, True)
        return_far(c)
        return_rows(c, own)

    def edge(c):
        h, part = c // splits, c % splits
        drain(far.at[c], d1_recv.at[c])

        @pl.when(part == splits - 1)
        def _():
            drain(lse_own.at[h], l1_recv.at[h])

        return_rows(c, far)

    def backward_row(h, r):
        q, k, v, g = [xin[h, kind, r] for kind in range(4)]
        count = q.shape[0] // CHUNK
        slab = CHUNK // GROUP

        def came_back(kind, i):
            return back[h, kind, r, i * slab:(i + 1) * slab].reshape(CHUNK, HEAD_DIM).astype(F32)

        def give(kind, i, value):
            back[h, kind, r, i * slab:(i + 1) * slab] = value.astype(BF16).reshape(slab, GROUP, HEAD_DIM)

        def line(ref, lead, i):
            base = i * (CHUNK // LANES)
            return jnp.concatenate(
                [ref[lead, base + n, pl.ds(r, 1), :] for n in range(CHUNK // LANES)], axis=1)

        gk, gv = [None] * count, [None] * count
        for i in range(count):
            span = slice(i * CHUNK, (i + 1) * CHUNK)
            lse, w_row, w_col = merge(line(st_row, 2 * h, i), line(lse_back, h, i))
            att_t = orow[h, r, :, span] * w_row + came_back(0, i).T * w_col
            att = att_t.T.astype(BF16)
            give(0, i, att)
            delta = jnp.sum(
                (chunk(g, i).astype(F32) * att.astype(F32)).T, axis=0, keepdims=True
            )
            scores = scores_of(chunk(q, i), k, row_bias, i)
            probs = [jnp.exp2(s - lse) for s in scores]
            gq = backward_of(i, probs, delta, q, k, v, g, gk, gv)
            give(1, i, gq + came_back(1, i))
        for j in range(count):
            give(2, j, gk[j] * SCALE + came_back(2, j))
            give(3, j, gv[j] + came_back(3, j))

    def backward_head(h):
        drain(back.at[h, :, :, pl.ds(0, blocks * (m - 1))], e_recv.at[h])
        drain(lse_back.at[h, pl.ds(0, m - 1)], le_recv.at[h])

        def body(r, carry):
            backward_row(h, r)
            return carry

        lax.fori_loop(0, rows, body, 0)
        for kind in range(4):
            pltpu.make_async_copy(
                back.at[h, kind], outs[kind].at[:, :, :, lanes_of(h)], out_sem
            ).start()

    lag_upper, lag_lower, lag_edge, lag_rows = LAGS

    def step(s, carry):
        def at(lag, role=None):
            ready = (s >= lag) & (s < chunks + lag)
            return ready if role is None else ready & role

        @pl.when(s < heads)
        def _():
            forward_head(s)

        @pl.when(s == heads - 1)
        def _():
            send_stats()

        @pl.when(at(0))
        def _():
            pass_on(s)

        @pl.when(s + AHEAD < chunks)
        def _():
            spread_chunk(s + AHEAD, 0)

        @pl.when(at(1, z == 1))
        def _():
            pass_far(s - 1)

        @pl.when((s == lag_upper) & ((z == 1) | (z == 2)))
        def _():
            wait_stats()

        @pl.when(at(lag_upper, z == 2))
        def _():
            upper(s - lag_upper)

        @pl.when(at(lag_lower, z == 1))
        def _():
            lower(s - lag_lower)

        @pl.when(at(lag_edge, outer))
        def _():
            edge(s - lag_edge)

        done = s - lag_rows

        @pl.when((done >= 0) & (done % splits == splits - 1))
        def _():
            backward_head(done // splits)

        return carry

    lax.fori_loop(0, chunks + lag_rows, step, 0)

    drain(own.at[:, :, pl.ds(0, rows * (m - 1))], a_send)
    drain(own.at[:, :, pl.ds(0, rows * (m - 1))], e_send)
    drain(st_own.at[:, pl.ds(0, m - 1)], s_send)
    drain(lse_own.at[:, pl.ds(0, m - 1)], le_send)

    @pl.when(outer)
    def _():
        drain(own, b_send)
        drain(st_far, sf_send)

    @pl.when((z == 1) | (z == 2))
    def _():
        drain(far, d1_send)
        drain(lse_far, l1_send)

    @pl.when(z == 2)
    def _():
        drain(low, d2_send)

    drain(back, out_sem)


AHEAD = 2
LAGS = (3, 6, 8, 11)


def fits(tokens, width, devices):
    rows = tokens // ROW_LEN
    if tokens % ROW_LEN or devices % PLANES or width % HEAD_DIM:
        return False
    m = devices // PLANES
    blocks = ROW_LEN // GROUP
    return (
        m > 1
        and ROW_LEN // m == LANES
        and rows * m * GROUP == LANES
        and (blocks // m) % SPLITS == 0
    )


def by_planes(queries, key_vectors, value_vectors, grad_output):
    devices = lax.axis_size("seq")
    m = devices // PLANES
    tokens, width = queries.shape
    rows, heads, blocks = tokens // ROW_LEN, width // HEAD_DIM, ROW_LEN // GROUP
    per = blocks // m // SPLITS
    chunks = heads * SPLITS
    arrays = (queries, key_vectors, value_vectors, grad_output)
    views = [a.reshape(rows, blocks, GROUP, width) for a in arrays]
    flat = [a.reshape(rows, ROW_LEN, width) for a in arrays]
    buffer = pltpu.VMEM((chunks, 4, rows * m, per, GROUP, HEAD_DIM), BF16)
    dma = pltpu.SemaphoreType.DMA
    stat = pltpu.VMEM((2 * heads, m, rows, LANES), F32)
    lse = pltpu.VMEM((heads, m, rows, LANES), F32)
    each, single = dma((chunks,)), dma(())
    outs = pl.pallas_call(
        fused_kernel,
        in_specs=[pl.BlockSpec(memory_space=pl.ANY)] * 8,
        out_specs=[pl.BlockSpec(memory_space=pl.ANY)] * 4,
        out_shape=[jax.ShapeDtypeStruct(views[0].shape, BF16)] * 4,
        scratch_shapes=[
            pltpu.VMEM((heads, 4, rows, ROW_LEN, HEAD_DIM), BF16),
            buffer, buffer, buffer,
            pltpu.VMEM((heads, 4, rows, blocks, GROUP, HEAD_DIM), BF16),
            pltpu.VMEM((heads, rows, HEAD_DIM, ROW_LEN), F32),
            stat, stat, stat, lse, lse, lse,
            dma((heads,)), each, single, each, single, each, dma((chunks, 2)),
            each, each, each, each, single, each, single, each,
            single, dma((heads,)), single, single, single, single, single, dma((heads,)),
            single, dma((heads,)), single,
        ],
        compiler_params=pltpu.CompilerParams(
            collective_id=0, has_side_effects=True, vmem_limit_bytes=63 * 1024 * 1024
        ),
        cost_estimate=pl.CostEstimate(
            flops=tokens * width * 512 * 24,
            bytes_accessed=tokens * width * 16,
            transcendentals=tokens * width,
        ),
        name="by_planes",
    )(*views, *flat)
    return tuple(a.reshape(queries.shape) for a in outs)


def on_device(queries, key_vectors, value_vectors, grad_output):
    arrays = (queries, key_vectors, value_vectors, grad_output)
    if fits(*queries.shape, lax.axis_size("seq")):
        return by_planes(*arrays)
    return by_all_to_all(*arrays)


def solution(mesh):
    spec = P("seq", "head")
    return jax.shard_map(
        on_device,
        mesh=mesh,
        in_specs=(spec,) * 4,
        out_specs=(spec,) * 4,
        check_vma=False,
    )
```

```python
import functools
import math

import jax
import jax.numpy as jnp
from jax import lax
from jax.experimental import pallas as pl
from jax.experimental.pallas import tpu as pltpu
from jax.sharding import PartitionSpec as P

ROW_LEN = 512
HEAD_DIM = 128
GROUP = 8
CHUNK = 256
PIECES = 2
MASKED = -1e30
FLOOR = -1e20
LOG2E = 1.0 / math.log(2.0)
SCALE = 1.0 / math.sqrt(HEAD_DIM)
F32 = jnp.float32
BF16 = jnp.bfloat16


def dot_t(left, right):
    return lax.dot_general(left, right, (((1,), (1,)), ((), ())), preferred_element_type=F32)


def dot_f(left, right):
    return lax.dot_general(left, right, (((0,), (0,)), ((), ())), preferred_element_type=F32)


def dot(left, right):
    return jnp.dot(left, right, preferred_element_type=F32)


def row_bias(first, key_chunk, query_chunk):
    if key_chunk < query_chunk:
        return None
    keys = lax.broadcasted_iota(jnp.int32, (CHUNK, CHUNK), 0)
    queries = lax.broadcasted_iota(jnp.int32, (CHUNK, CHUNK), 1)
    return jnp.where(keys <= queries, 0.0, MASKED)


def col_bias(first, key_chunk, query_chunk):
    keys = lax.broadcasted_iota(jnp.int32, (CHUNK, CHUNK), 0)
    queries = lax.broadcasted_iota(jnp.int32, (CHUNK, CHUNK), 1)
    gap = queries - keys
    same = (gap & (GROUP - 1)) == 0
    if key_chunk == query_chunk:
        same = same & (gap > 0)
    return jnp.where(same, 0.0, MASKED)


def chunk(array, index):
    return array[index * CHUNK : (index + 1) * CHUNK]


def scores_of(query, keys, bias, query_chunk):
    out = []
    for j in range(query_chunk + 1):
        s = dot_t(chunk(keys, j), query) * (SCALE * LOG2E)
        b = bias(None, j, query_chunk)
        out.append(s if b is None else s + b)
    return out


def softmax_of(scores, values):
    top = functools.reduce(
        jnp.maximum, [jnp.max(s, axis=0, keepdims=True) for s in scores]
    )
    top = jnp.maximum(top, FLOOR)
    weights = [jnp.exp2(s - top) for s in scores]
    total = sum(jnp.sum(w, axis=0, keepdims=True) for w in weights)
    acc = sum(dot_f(chunk(values, j), w.astype(BF16)) for j, w in enumerate(weights))
    total = jnp.maximum(total, 1.0)
    return weights, top, total, acc / total


def merge(left, right):
    top = jnp.maximum(left, right)
    w_left, w_right = jnp.exp2(left - top), jnp.exp2(right - top)
    den = w_left + w_right
    return top + jnp.log2(den), w_left / den, w_right / den


def backward_of(i, probs, delta, q, k, v, g, gk, gv):
    query, grad = chunk(q, i), chunk(g, i)
    gq = None
    for j, p in enumerate(probs):
        dv = dot(p.astype(BF16), grad)
        dp = dot_t(chunk(v, j), grad)
        ds = (p * (dp - delta)).astype(BF16)
        dk = dot(ds, query)
        dq = dot_f(chunk(k, j), ds)
        gv[j] = dv if gv[j] is None else gv[j] + dv
        gk[j] = dk if gk[j] is None else gk[j] + dk
        gq = dq if gq is None else gq + dq
    return (gq * SCALE).T


def row_forward_kernel(q_ref, k_ref, v_ref, g_ref, o_ref, lse_ref, dot_ref):
    q, k, v, g = q_ref[0], k_ref[0], v_ref[0], g_ref[0]
    for i in range(q.shape[0] // CHUNK):
        span = slice(i * CHUNK, (i + 1) * CHUNK)
        _, top, total, out = softmax_of(scores_of(chunk(q, i), k, row_bias, i), v)
        o_ref[0, 0, :, span] = out
        lse_ref[0, 0, :, span] = top + jnp.log2(total)
        grad_t = chunk(g, i).astype(F32).T
        dot_ref[0, 0, :, span] = jnp.sum(grad_t * out, axis=0, keepdims=True)


def row_forward(q, k, v, g):
    rows, length, width = q.shape
    heads = width // HEAD_DIM
    block = pl.BlockSpec((1, length, HEAD_DIM), lambda r, h: (r, 0, h))
    stat = pl.BlockSpec((1, 1, 1, length), lambda r, h: (r, h, 0, 0))
    stat_shape = jax.ShapeDtypeStruct((rows, heads, 1, length), F32)
    return pl.pallas_call(
        row_forward_kernel,
        grid=(rows, heads),
        in_specs=[block] * 4,
        out_specs=[
            pl.BlockSpec((1, 1, HEAD_DIM, length), lambda r, h: (r, h, 0, 0)),
            stat,
            stat,
        ],
        out_shape=[
            jax.ShapeDtypeStruct((rows, heads, HEAD_DIM, length), F32),
            stat_shape,
            stat_shape,
        ],
        cost_estimate=pl.CostEstimate(
            flops=rows * heads * length * length * HEAD_DIM * 8,
            bytes_accessed=rows * length * width * 12,
            transcendentals=rows * heads * length * length,
        ),
        name="row_forward",
    )(q, k, v, g)


def col_kernel(x_ref, stat_ref, y_ref, lse_ref):
    devices, _, _, per, width = x_ref.shape
    tokens = devices * per
    chunks = tokens // CHUNK
    q, k, v, g = [x_ref[:, a, 0].reshape(tokens, width) for a in range(4)]
    gk, gv = [None] * chunks, [None] * chunks
    slab = CHUNK // per
    for i in range(chunks):
        span = slice(i * CHUNK, (i + 1) * CHUNK)
        here = slice(i * slab, (i + 1) * slab)
        weights, top, total, out = softmax_of(scores_of(chunk(q, i), k, col_bias, i), v)
        lse_col = top + jnp.log2(total)
        lse_ref[0, 0, :, span] = lse_col
        out_low = out.T.astype(BF16)
        y_ref[here, 0, 0] = out_low.reshape(slab, per, width)
        lse, w_row, w_col = merge(stat_ref[0, 0, 0, :, span], lse_col)
        dot_col = jnp.sum(
            (chunk(g, i).astype(F32) * out_low.astype(F32)).T, axis=0, keepdims=True
        )
        delta = w_row * stat_ref[1, 0, 0, :, span] + w_col * dot_col
        factor = jnp.exp2(top - lse)
        probs = [w * factor for w in weights]
        gq = backward_of(i, probs, delta, q, k, v, g, gk, gv)
        y_ref[here, 1, 0] = gq.astype(BF16).reshape(slab, per, width)
    for j in range(chunks):
        here = slice(j * slab, (j + 1) * slab)
        y_ref[here, 2, 0] = (gk[j] * SCALE).astype(BF16).reshape(slab, per, width)
        y_ref[here, 3, 0] = gv[j].astype(BF16).reshape(slab, per, width)


def col_both(x, stats, first_head):
    devices, kinds, groups, per, width = x.shape
    heads = width // HEAD_DIM
    tokens = devices * per
    block = pl.BlockSpec(
        (devices, kinds, 1, per, HEAD_DIM), lambda c, h: (0, 0, c, 0, h)
    )
    return pl.pallas_call(
        col_kernel,
        grid=(groups, heads),
        in_specs=[
            block,
            pl.BlockSpec((2, 1, 1, 1, tokens), lambda c, h: (0, first_head + h, c, 0, 0)),
        ],
        out_specs=[block, pl.BlockSpec((1, 1, 1, tokens), lambda c, h: (h, c, 0, 0))],
        out_shape=[
            jax.ShapeDtypeStruct(x.shape, BF16),
            jax.ShapeDtypeStruct((heads, groups, 1, tokens), F32),
        ],
        cost_estimate=pl.CostEstimate(
            flops=groups * heads * tokens * tokens * HEAD_DIM * 20,
            bytes_accessed=x.size * 4,
            transcendentals=groups * heads * tokens * tokens,
        ),
        name="col_both",
    )(x, stats)


def row_backward_kernel(
    q_ref, k_ref, v_ref, g_ref, o_ref, lse_ref, back_ref, lse_col_ref, *rest
):
    att_ref, gq_ref, gk_ref, gv_ref = rest[-4:]
    q, k, v, g = q_ref[0], k_ref[0], v_ref[0], g_ref[0]
    length = q.shape[0]
    chunks = length // CHUNK
    devices = back_ref.shape[0]
    slab = devices // chunks

    def came_back(kind, i):
        part = back_ref[i * slab : (i + 1) * slab, kind, :, 0].astype(F32)
        return part.reshape(CHUNK, HEAD_DIM)

    gk, gv = [None] * chunks, [None] * chunks
    for i in range(chunks):
        span = slice(i * CHUNK, (i + 1) * CHUNK)
        lse, w_row, w_col = merge(lse_ref[0, 0, :, span], lse_col_ref[0, 0, :, span])
        col_t = came_back(0, i).T
        att_t = o_ref[0, 0, :, span] * w_row + col_t * w_col
        low = att_t.T.astype(BF16)
        att_ref[0, span, :] = low
        delta = jnp.sum(
            (chunk(g, i).astype(F32) * low.astype(F32)).T, axis=0, keepdims=True
        )
        scores = scores_of(chunk(q, i), k, row_bias, i)
        probs = [jnp.exp2(s - lse) for s in scores]
        gq = backward_of(i, probs, delta, q, k, v, g, gk, gv)
        gq_ref[0, span, :] = (gq + came_back(1, i)).astype(BF16)
    for j in range(chunks):
        span = slice(j * CHUNK, (j + 1) * CHUNK)
        gk_ref[0, span, :] = (gk[j] * SCALE + came_back(2, j)).astype(BF16)
        gv_ref[0, span, :] = (gv[j] + came_back(3, j)).astype(BF16)


def row_backward(q, k, v, g, o, lse, back, lse_col, first_head, earlier):
    rows, length, width = q.shape
    devices, kinds, groups, _, size, piece = back.shape
    heads = piece // HEAD_DIM
    block = pl.BlockSpec((1, length, HEAD_DIM), lambda r, h: (r, 0, first_head + h))
    stat = pl.BlockSpec((1, 1, 1, length), lambda r, h: (r, first_head + h, 0, 0))
    in_specs = [block] * 4 + [
        pl.BlockSpec((1, 1, HEAD_DIM, length), lambda r, h: (r, first_head + h, 0, 0)),
        stat,
        pl.BlockSpec(
            (devices, kinds, groups, 1, size, HEAD_DIM), lambda r, h: (0, 0, 0, r, 0, h)
        ),
        stat,
    ]
    aliases = {}
    if earlier:
        aliases = {len(in_specs) + n: n for n in range(4)}
        in_specs = in_specs + [pl.BlockSpec(memory_space=pl.ANY)] * 4
    return pl.pallas_call(
        row_backward_kernel,
        grid=(rows, heads),
        in_specs=in_specs,
        out_specs=[block] * 4,
        out_shape=[jax.ShapeDtypeStruct(q.shape, BF16)] * 4,
        input_output_aliases=aliases,
        cost_estimate=pl.CostEstimate(
            flops=rows * heads * length * length * HEAD_DIM * 14,
            bytes_accessed=rows * length * piece * 28,
            transcendentals=rows * heads * length * length,
        ),
        name="row_backward",
    )(q, k, v, g, o, lse, back, lse_col, *earlier)


def exchange(array):
    return lax.all_to_all(array, "seq", split_axis=0, concat_axis=0, tiled=True)


def by_all_to_all(queries, key_vectors, value_vectors, grad_output):
    devices = lax.axis_size("seq")
    rows = queries.shape[0] // ROW_LEN
    width = queries.shape[1]
    heads = width // HEAD_DIM
    groups = ROW_LEN // devices // GROUP
    per = rows * GROUP
    tokens = devices * per
    piece = width // PIECES
    piece_heads = piece // HEAD_DIM
    arrays = (queries, key_vectors, value_vectors, grad_output)
    by_row = [a.reshape(rows, ROW_LEN, width) for a in arrays]

    packs = []
    for n in range(PIECES):
        parts = [
            jnp.transpose(
                a[:, n * piece : (n + 1) * piece].reshape(rows, devices, groups, GROUP, piece),
                (1, 2, 0, 3, 4),
            )
            for a in arrays
        ]
        packed = jnp.stack(parts, axis=1).reshape(devices, 4, groups, per, piece)
        packs.append(packed)
    arrived = [exchange(packs[0])]

    o, lse, dots = row_forward(*by_row)
    stats = jnp.stack([lse, dots]).reshape(2, rows, heads, devices, groups, GROUP)
    stats = jnp.transpose(stats, (3, 0, 2, 4, 1, 5)).reshape(devices, -1)
    arrived[0], stats = lax.optimization_barrier((arrived[0], stats))
    stats = exchange(stats)
    for n in range(1, PIECES):
        packs[n], stats = lax.optimization_barrier((packs[n], stats))
        arrived.append(exchange(packs[n]))
    stats = stats.reshape(devices, 2, heads, groups, per)
    stats = jnp.transpose(stats, (1, 2, 3, 0, 4)).reshape(2, heads, groups, 1, tokens)

    columns = [col_both(arrived[n], stats, n * piece_heads) for n in range(PIECES)]
    lse_col = jnp.concatenate([lse_col for _, lse_col in columns], axis=0)
    lse_col = jnp.transpose(
        lse_col.reshape(heads, groups, devices, per), (2, 0, 1, 3)
    ).reshape(devices, -1)
    lse_col = exchange(lse_col)
    sent = [y for y, _ in columns]
    sent[-1], lse_col = lax.optimization_barrier((sent[-1], lse_col))
    lse_col = lse_col.reshape(devices, heads, groups, rows, GROUP)
    lse_col = jnp.transpose(lse_col, (3, 1, 0, 2, 4)).reshape(rows, heads, 1, ROW_LEN)
    backs = [exchange(y).reshape(devices, 4, groups, rows, GROUP, piece) for y in sent]

    outs = ()
    for n in range(PIECES):
        outs = row_backward(*by_row, o, lse, backs[n], lse_col, n * piece_heads, tuple(outs))
    return tuple(a.reshape(queries.shape) for a in outs)


PLANES = 4
SPLITS = 16
LANES = 128


def drain(ref, sem):
    pltpu.make_async_copy(ref, ref, sem).wait()


def fold_lanes(x):
    for shift in (8, 16, 32, 64):
        x = x + pltpu.roll(x, shift, 1)
    return x


def lane_masks():
    group = lax.broadcasted_iota(jnp.int32, (LANES // GROUP, LANES), 1) // GROUP
    row = lax.broadcasted_iota(jnp.int32, (LANES // GROUP, LANES), 0)
    return group, group == row


def to_tile(stat, block):
    group, diagonal = lane_masks()
    spread = fold_lanes(jnp.where(group == block, stat, 0.0))
    return jnp.sum(jnp.where(diagonal, spread, 0.0), axis=0, keepdims=True)


def from_tile(line, block):
    group, diagonal = lane_masks()
    spread = fold_lanes(jnp.where(diagonal, line, 0.0))
    return jnp.where(group == block, spread, 0.0)


def column_unit(q, g, keys, values, query_chunk, lse_row, dot_row):
    count = len(keys)
    scores = []
    for j in range(count):
        bias = col_bias(None, j, count - 1)
        scores.append(dot_t(keys[j], q) * (SCALE * LOG2E) + bias)
    top = functools.reduce(
        jnp.maximum, [jnp.max(s, axis=0, keepdims=True) for s in scores]
    )
    top = jnp.maximum(top, FLOOR)
    weights = [jnp.exp2(s - top) for s in scores]
    total = sum(jnp.sum(w, axis=0, keepdims=True) for w in weights)
    acc = sum(dot_f(v, w.astype(BF16)) for v, w in zip(values, weights))
    total = jnp.maximum(total, 1.0)
    out_low = (acc / total).T.astype(BF16)
    lse_col = top + jnp.log2(total)
    lse, w_row, w_col = merge(lse_row, lse_col)
    dot_col = jnp.sum(
        (g.astype(F32) * out_low.astype(F32)).T, axis=0, keepdims=True
    )
    delta = w_row * dot_row + w_col * dot_col
    factor = jnp.exp2(top - lse)
    gq, gk, gv = None, [], []
    for j in range(count):
        p = weights[j] * factor
        gv.append(dot(p.astype(BF16), g))
        dp = dot_t(values[j], g)
        ds = (p * (dp - delta)).astype(BF16)
        gk.append(dot(ds, q) * SCALE)
        dq = dot_f(keys[j], ds)
        gq = dq if gq is None else gq + dq
    return out_low, (gq * SCALE).T.astype(BF16), gk, gv, lse_col


def fused_kernel(*refs):
    xs, flat, outs = refs[0:4], refs[4:8], refs[8:12]
    (xin, own, far, low, back, orow, st_row, st_own, st_far, lse_own, lse_far,
     lse_back, in_sem, a_loc, a_send, a_recv, b_send, bkv_recv, bqg_recv,
     k1_send, k1_recv, k0_send, k0_recv, d2_send, d2_recv, d1_send, d1_recv,
     e_send, e_recv, s_send, s_recv, sf_send, sf_recv, l1_send, l1_recv,
     le_send, le_recv, out_sem) = refs[12:]
    heads, _, rows = xin.shape[:3]
    chunks = own.shape[0]
    plane_rows, per = own.shape[2], own.shape[3]
    splits = chunks // heads
    devices = lax.axis_size("seq")
    m = devices // PLANES
    blocks = per * splits
    seq, head_index = lax.axis_index("seq"), lax.axis_index("head")
    z, p = seq // m, seq % m
    first = z * m

    def send(src, dst, send_sem, recv_sem, to):
        pltpu.make_async_remote_copy(
            src_ref=src, dst_ref=dst, send_sem=send_sem, recv_sem=recv_sem,
            device_id=(to, head_index), device_id_type=pl.DeviceIdType.MESH,
        ).start()

    outer = (z == 0) | (z == PLANES - 1)
    inner_peer = jnp.where(z == 0, seq + m, seq - m)
    outer_peer = jnp.where(z == 1, seq - m, seq + m)

    barrier = pltpu.get_barrier_semaphore()
    for d in range(1, m):
        pl.semaphore_signal(barrier, inc=1, device_id=(first + (p + d) % m, head_index),
                            device_id_type=pl.DeviceIdType.MESH)
    for d in range(1, PLANES):
        pl.semaphore_signal(barrier, inc=1,
                            device_id=((z + d) % PLANES * m + p, head_index),
                            device_id_type=pl.DeviceIdType.MESH)

    def lanes_of(h):
        return pl.ds(pl.multiple_of(h * HEAD_DIM, HEAD_DIM), HEAD_DIM)

    def load_rows(h, carry):
        for kind in range(4):
            pltpu.make_async_copy(
                flat[kind].at[:, :, lanes_of(h)], xin.at[h, kind], in_sem.at[h]
            ).start()
        return carry

    load_rows(0, 0)
    pl.semaphore_wait(barrier, m - 1 + PLANES - 1)

    def spread_chunk(c, carry):
        h, part = c // splits, c % splits
        for d in range(1, m):
            peer = (p + d) % m
            for kind in range(4):
                send(
                    xs[kind].at[:, pl.ds(peer * blocks + part * per, per), :, lanes_of(h)],
                    own.at[c, kind, pl.ds(p * rows, rows)],
                    a_send, a_recv.at[c], first + peer,
                )
        for kind in range(4):
            pltpu.make_async_copy(
                xs[kind].at[:, pl.ds(p * blocks + part * per, per), :, lanes_of(h)],
                own.at[c, kind, pl.ds(p * rows, rows)],
                a_loc.at[c],
            ).start()
        return carry

    lax.fori_loop(0, AHEAD, spread_chunk, 0)
    lax.fori_loop(1, heads, load_rows, 0)

    def forward_row(h, r):
        q, k, v, g = [xin[h, kind, r] for kind in range(4)]
        for i in range(q.shape[0] // CHUNK):
            span = slice(i * CHUNK, (i + 1) * CHUNK)
            _, top, total, out = softmax_of(scores_of(chunk(q, i), k, row_bias, i), v)
            orow[h, r, :, span] = out
            lse = top + jnp.log2(total)
            grad_t = chunk(g, i).astype(F32).T
            dots = jnp.sum(grad_t * out, axis=0, keepdims=True)
            for part in range(CHUNK // LANES):
                lanes = slice(part * LANES, (part + 1) * LANES)
                at = i * (CHUNK // LANES) + part
                st_row[2 * h, at, pl.ds(r, 1), :] = lse[:, lanes]
                st_row[2 * h + 1, at, pl.ds(r, 1), :] = dots[:, lanes]

    def send_stats(h):
        pair = pl.ds(2 * h, 2)
        for d in range(1, m):
            peer = (p + d) % m
            send(st_row.at[pair, peer], st_own.at[pair, p], s_send, s_recv.at[h], first + peer)
        st_own[pair, p] = st_row[pair, p]

    def wait_stats(h):
        drain(st_own.at[pl.ds(2 * h, 2), pl.ds(0, m - 1)], s_recv.at[h])

    def pass_stats(h):
        wait_stats(h)
        pair = pl.ds(2 * h, 2)
        send(st_own.at[pair], st_far.at[pair], sf_send, sf_recv.at[h], inner_peer)

    def tile(ref, *at):
        return ref[at].reshape(plane_rows * GROUP, HEAD_DIM)

    def put(ref, at, value):
        ref[at] = value.astype(BF16).reshape(plane_rows, GROUP, HEAD_DIM)

    def stat_of(ref, which, block):
        return to_tile(ref[which].reshape(plane_rows, LANES), block)

    def add_lse(ref, h, line, block):
        ref[h] = ref[h] + from_tile(line, block).reshape(m, rows, LANES)

    half = plane_rows * GROUP

    def solve(c, lower):
        h, part = c // splits, c % splits
        pair = (far, own) if lower else (own, far)
        lses = (lse_far, lse_own) if lower else (lse_own, lse_far)
        stats = (st_far, st_own) if lower else (st_own, st_far)

        @pl.when(part == 0)
        def _():
            wait_stats(h)
            drain(st_far.at[pl.ds(2 * h, 2)], sf_recv.at[h])
            lse_own[h] = jnp.zeros(lse_own.shape[1:], F32)
            lse_far[h] = jnp.zeros(lse_far.shape[1:], F32)

        def body(b, carry):
            block = part * per + b
            every = slice(None)

            def both(kind):
                return jnp.concatenate([tile(ref, c, kind, every, b) for ref in pair], axis=0)

            q, k, v, g = [both(kind) for kind in range(4)]
            keys, values = [k], [v]
            if not lower:
                keys = [jnp.concatenate([tile(low, c, 0, every, b), tile(low, c, 2, every, b)], axis=0), k]
                values = [jnp.concatenate([tile(low, c, 1, every, b), tile(low, c, 3, every, b)], axis=0), v]
            lse_row = jnp.concatenate([stat_of(s, 2 * h, block) for s in stats], axis=1)
            dot_row = jnp.concatenate([stat_of(s, 2 * h + 1, block) for s in stats], axis=1)
            o, gq, gk, gv, lse_col = column_unit(q, g, keys, values, None, lse_row, dot_row)
            gk_own, gv_own = gk[-1], gv[-1]
            if lower:
                gk_own = gk_own + jnp.concatenate(
                    [tile(low, c, 0, every, b), tile(low, c, 2, every, b)], axis=0).astype(F32)
                gv_own = gv_own + jnp.concatenate(
                    [tile(low, c, 1, every, b), tile(low, c, 3, every, b)], axis=0).astype(F32)
            else:
                put(low, (c, 0, every, b), gk[0][:half])
                put(low, (c, 1, every, b), gv[0][:half])
                put(low, (c, 2, every, b), gk[0][half:])
                put(low, (c, 3, every, b), gv[0][half:])
            for n, ref in enumerate(pair):
                span = slice(n * half, (n + 1) * half)
                for kind, value in enumerate((o, gq, gk_own, gv_own)):
                    put(ref, (c, kind, every, b), value[span])
                add_lse(lses[n], h, lse_col[:, span], block)
            return carry

        lax.fori_loop(0, per, body, 0)

    def return_rows(c, ref):
        h, part = c // splits, c % splits
        at = pl.ds(p * blocks + part * per, per)
        for d in range(1, m):
            peer = (p + d) % m
            send(
                ref.at[c, :, pl.ds(peer * rows, rows)], back.at[h, :, :, at],
                e_send, e_recv.at[h], first + peer,
            )
        back[h, :, :, at] = ref[c, :, pl.ds(p * rows, rows)]

        @pl.when(part == splits - 1)
        def _():
            for d in range(1, m):
                peer = (p + d) % m
                send(lse_own.at[h, peer], lse_back.at[h, p], le_send, le_recv.at[h], first + peer)
            lse_back[h, p] = lse_own[h, p]

    def return_far(c):
        h, part = c // splits, c % splits
        send(far.at[c], far.at[c], d1_send, d1_recv.at[c], outer_peer)

        @pl.when(part == splits - 1)
        def _():
            send(lse_far.at[h], lse_own.at[h], l1_send, l1_recv.at[h], outer_peer)

    def pass_on(c):
        drain(own.at[c, :, pl.ds(0, rows * (m - 1))], a_recv.at[c])
        drain(own.at[c, :, pl.ds(0, rows)], a_loc.at[c])

        @pl.when(outer)
        def _():
            send(own.at[c, pl.ds(1, 2)], far.at[c, pl.ds(1, 2)], b_send, bkv_recv.at[c], inner_peer)
            send(own.at[c, 0], far.at[c, 0], b_send, bqg_recv.at[c, 0], inner_peer)
            send(own.at[c, 3], far.at[c, 3], b_send, bqg_recv.at[c, 1], inner_peer)

        @pl.when(z == 1)
        def _():
            send(own.at[c, pl.ds(1, 2)], low.at[c, pl.ds(2, 2)], k1_send.at[c], k1_recv.at[c], seq + m)

    def pass_far(c):
        drain(far.at[c, pl.ds(1, 2)], bkv_recv.at[c])
        send(far.at[c, pl.ds(1, 2)], low.at[c, pl.ds(0, 2)], k0_send.at[c], k0_recv.at[c], seq + m)

    def wait_qg(c):
        drain(far.at[c, 0], bqg_recv.at[c, 0])
        drain(far.at[c, 3], bqg_recv.at[c, 1])

    def upper(c):
        drain(far.at[c, pl.ds(1, 2)], bkv_recv.at[c])
        wait_qg(c)
        drain(low.at[c, pl.ds(2, 2)], k1_recv.at[c])
        drain(low.at[c, pl.ds(0, 2)], k0_recv.at[c])
        solve(c, False)
        send(low.at[c], low.at[c], d2_send, d2_recv.at[c], seq - m)
        return_far(c)
        return_rows(c, own)

    def lower(c):
        wait_qg(c)
        drain(low.at[c], d2_recv.at[c])
        drain(own.at[c, pl.ds(1, 2)], k1_send.at[c])
        drain(far.at[c, pl.ds(1, 2)], k0_send.at[c])
        solve(c, True)
        return_far(c)
        return_rows(c, own)

    def edge(c):
        h, part = c // splits, c % splits
        drain(far.at[c], d1_recv.at[c])

        @pl.when(part == splits - 1)
        def _():
            drain(lse_own.at[h], l1_recv.at[h])

        return_rows(c, far)

    def backward_row(h, r):
        q, k, v, g = [xin[h, kind, r] for kind in range(4)]
        count = q.shape[0] // CHUNK
        slab = CHUNK // GROUP

        def came_back(kind, i):
            return back[h, kind, r, i * slab:(i + 1) * slab].reshape(CHUNK, HEAD_DIM).astype(F32)

        def give(kind, i, value):
            back[h, kind, r, i * slab:(i + 1) * slab] = value.astype(BF16).reshape(slab, GROUP, HEAD_DIM)

        def line(ref, lead, i):
            base = i * (CHUNK // LANES)
            return jnp.concatenate(
                [ref[lead, base + n, pl.ds(r, 1), :] for n in range(CHUNK // LANES)], axis=1)

        gk, gv = [None] * count, [None] * count
        for i in range(count):
            span = slice(i * CHUNK, (i + 1) * CHUNK)
            lse, w_row, w_col = merge(line(st_row, 2 * h, i), line(lse_back, h, i))
            att_t = orow[h, r, :, span] * w_row + came_back(0, i).T * w_col
            att = att_t.T.astype(BF16)
            give(0, i, att)
            delta = jnp.sum(
                (chunk(g, i).astype(F32) * att.astype(F32)).T, axis=0, keepdims=True
            )
            scores = scores_of(chunk(q, i), k, row_bias, i)
            probs = [jnp.exp2(s - lse) for s in scores]
            gq = backward_of(i, probs, delta, q, k, v, g, gk, gv)
            give(1, i, gq + came_back(1, i))
        for j in range(count):
            give(2, j, gk[j] * SCALE + came_back(2, j))
            give(3, j, gv[j] + came_back(3, j))

    def backward_ready(h):
        drain(back.at[h, :, :, pl.ds(0, blocks * (m - 1))], e_recv.at[h])
        drain(lse_back.at[h, pl.ds(0, m - 1)], le_recv.at[h])

    def give_out(h):
        for kind in range(4):
            pltpu.make_async_copy(
                back.at[h, kind], outs[kind].at[:, :, :, lanes_of(h)], out_sem
            ).start()

    lag_upper, lag_lower, lag_edge, lag_rows = LAGS
    pace = splits // rows

    def rows_forward(s):
        h = s // splits + 1

        @pl.when((h < heads) & (s % splits == 0))
        def _():
            drain(xin.at[h], in_sem.at[h])

        @pl.when((h < heads) & (s % pace == 0))
        def _():
            forward_row(h, s % splits // pace)

        @pl.when((h < heads) & (s % splits == (rows - 1) * pace))
        def _():
            send_stats(h)

        @pl.when((h < heads) & (s % splits == splits - 1) & outer)
        def _():
            pass_stats(h)

    def rows_backward(t):
        h = t // splits
        last = h == heads - 1

        @pl.when((t >= 0) & (t % splits == 0))
        def _():
            backward_ready(h)

        @pl.when((t >= 0) & (t % pace == 0))
        def _():
            def body(r, carry):
                backward_row(h, r)
                return carry

            start = jnp.where(last, 0, t % splits // pace)
            lax.fori_loop(start, jnp.where(last, rows, start + 1), body, 0)

        @pl.when((t >= 0) & (last | (t % splits == (rows - 1) * pace)))
        def _():
            give_out(h)

    def step(s, carry):
        def at(lag, role=None):
            ready = (s >= lag) & (s < chunks + lag)
            return ready if role is None else ready & role

        @pl.when(at(0))
        def _():
            pass_on(s)

        @pl.when(s + AHEAD < chunks)
        def _():
            spread_chunk(s + AHEAD, 0)

        @pl.when(at(1, z == 1))
        def _():
            pass_far(s - 1)

        @pl.when((s == 0) & outer)
        def _():
            pass_stats(0)

        @pl.when(at(lag_upper, z == 2))
        def _():
            upper(s - lag_upper)

        @pl.when(at(lag_lower, z == 1))
        def _():
            lower(s - lag_lower)

        @pl.when(at(lag_edge, outer))
        def _():
            edge(s - lag_edge)

        rows_forward(s)
        rows_backward(s - lag_rows - (splits - 1))
        return carry

    drain(xin.at[0], in_sem.at[0])

    def first_head(r, carry):
        forward_row(0, r)
        return carry

    lax.fori_loop(0, rows, first_head, 0)
    send_stats(0)
    lax.fori_loop(0, chunks + lag_rows, step, 0)

    drain(own.at[:, :, pl.ds(0, rows * (m - 1))], a_send)
    drain(own.at[:, :, pl.ds(0, rows * (m - 1))], e_send)
    drain(st_own.at[:, pl.ds(0, m - 1)], s_send)
    drain(lse_own.at[:, pl.ds(0, m - 1)], le_send)

    @pl.when(outer)
    def _():
        drain(own, b_send)
        drain(st_far, sf_send)

    @pl.when((z == 1) | (z == 2))
    def _():
        drain(far, d1_send)
        drain(lse_far, l1_send)

    @pl.when(z == 2)
    def _():
        drain(low, d2_send)

    drain(back, out_sem)


AHEAD = 2
LAGS = (2, 5, 7, 9)


def fits(tokens, width, devices):
    rows = tokens // ROW_LEN
    if tokens % ROW_LEN or devices % PLANES or width % HEAD_DIM:
        return False
    m = devices // PLANES
    blocks = ROW_LEN // GROUP
    return (
        m > 1
        and ROW_LEN // m == LANES
        and rows * m * GROUP == LANES
        and (blocks // m) % SPLITS == 0
        and SPLITS % rows == 0
    )


def by_planes(queries, key_vectors, value_vectors, grad_output):
    devices = lax.axis_size("seq")
    m = devices // PLANES
    tokens, width = queries.shape
    rows, heads, blocks = tokens // ROW_LEN, width // HEAD_DIM, ROW_LEN // GROUP
    per = blocks // m // SPLITS
    chunks = heads * SPLITS
    arrays = (queries, key_vectors, value_vectors, grad_output)
    views = [a.reshape(rows, blocks, GROUP, width) for a in arrays]
    flat = [a.reshape(rows, ROW_LEN, width) for a in arrays]
    buffer = pltpu.VMEM((chunks, 4, rows * m, per, GROUP, HEAD_DIM), BF16)
    dma = pltpu.SemaphoreType.DMA
    stat = pltpu.VMEM((2 * heads, m, rows, LANES), F32)
    lse = pltpu.VMEM((heads, m, rows, LANES), F32)
    each, single = dma((chunks,)), dma(())
    outs = pl.pallas_call(
        fused_kernel,
        in_specs=[pl.BlockSpec(memory_space=pl.ANY)] * 8,
        out_specs=[pl.BlockSpec(memory_space=pl.ANY)] * 4,
        out_shape=[jax.ShapeDtypeStruct(views[0].shape, BF16)] * 4,
        scratch_shapes=[
            pltpu.VMEM((heads, 4, rows, ROW_LEN, HEAD_DIM), BF16),
            buffer, buffer, buffer,
            pltpu.VMEM((heads, 4, rows, blocks, GROUP, HEAD_DIM), BF16),
            pltpu.VMEM((heads, rows, HEAD_DIM, ROW_LEN), F32),
            stat, stat, stat, lse, lse, lse,
            dma((heads,)), each, single, each, single, each, dma((chunks, 2)),
            each, each, each, each, single, each, single, each,
            single, dma((heads,)), single, dma((heads,)), single, dma((heads,)),
            single, dma((heads,)), single, dma((heads,)), single,
        ],
        compiler_params=pltpu.CompilerParams(
            collective_id=0, has_side_effects=True, vmem_limit_bytes=63 * 1024 * 1024
        ),
        cost_estimate=pl.CostEstimate(
            flops=tokens * width * 512 * 24,
            bytes_accessed=tokens * width * 16,
            transcendentals=tokens * width,
        ),
        name="by_planes",
    )(*views, *flat)
    return tuple(a.reshape(queries.shape) for a in outs)


def on_device(queries, key_vectors, value_vectors, grad_output):
    arrays = (queries, key_vectors, value_vectors, grad_output)
    if fits(*queries.shape, lax.axis_size("seq")):
        return by_planes(*arrays)
    return by_all_to_all(*arrays)


def solution(mesh):
    spec = P("seq", "head")
    return jax.shard_map(
        on_device,
        mesh=mesh,
        in_specs=(spec,) * 4,
        out_specs=(spec,) * 4,
        check_vma=False,
    )
```

```python
import functools
import math

import jax
import jax.numpy as jnp
from jax import lax
from jax.experimental import pallas as pl
from jax.experimental.pallas import tpu as pltpu
from jax.sharding import PartitionSpec as P

ROW_LEN = 512
HEAD_DIM = 128
GROUP = 8
CHUNK = 256
PIECES = 2
MASKED = -1e30
FLOOR = -1e20
LOG2E = 1.0 / math.log(2.0)
SCALE = 1.0 / math.sqrt(HEAD_DIM)
F32 = jnp.float32
BF16 = jnp.bfloat16


def dot_t(left, right):
    return lax.dot_general(left, right, (((1,), (1,)), ((), ())), preferred_element_type=F32)


def dot_f(left, right):
    return lax.dot_general(left, right, (((0,), (0,)), ((), ())), preferred_element_type=F32)


def dot(left, right):
    return jnp.dot(left, right, preferred_element_type=F32)


def row_bias(first, key_chunk, query_chunk):
    if key_chunk < query_chunk:
        return None
    keys = lax.broadcasted_iota(jnp.int32, (CHUNK, CHUNK), 0)
    queries = lax.broadcasted_iota(jnp.int32, (CHUNK, CHUNK), 1)
    return jnp.where(keys <= queries, 0.0, MASKED)


def col_bias(first, key_chunk, query_chunk):
    keys = lax.broadcasted_iota(jnp.int32, (CHUNK, CHUNK), 0)
    queries = lax.broadcasted_iota(jnp.int32, (CHUNK, CHUNK), 1)
    gap = queries - keys
    same = (gap & (GROUP - 1)) == 0
    if key_chunk == query_chunk:
        same = same & (gap > 0)
    return jnp.where(same, 0.0, MASKED)


def chunk(array, index):
    return array[index * CHUNK : (index + 1) * CHUNK]


def scores_of(query, keys, bias, query_chunk):
    out = []
    for j in range(query_chunk + 1):
        s = dot_t(chunk(keys, j), query) * (SCALE * LOG2E)
        b = bias(None, j, query_chunk)
        out.append(s if b is None else s + b)
    return out


def softmax_of(scores, values):
    top = functools.reduce(
        jnp.maximum, [jnp.max(s, axis=0, keepdims=True) for s in scores]
    )
    top = jnp.maximum(top, FLOOR)
    weights = [jnp.exp2(s - top) for s in scores]
    total = sum(jnp.sum(w, axis=0, keepdims=True) for w in weights)
    acc = sum(dot_f(chunk(values, j), w.astype(BF16)) for j, w in enumerate(weights))
    total = jnp.maximum(total, 1.0)
    return weights, top, total, acc / total


def merge(left, right):
    top = jnp.maximum(left, right)
    w_left, w_right = jnp.exp2(left - top), jnp.exp2(right - top)
    den = w_left + w_right
    return top + jnp.log2(den), w_left / den, w_right / den


def backward_of(i, probs, delta, q, k, v, g, gk, gv):
    query, grad = chunk(q, i), chunk(g, i)
    gq = None
    for j, p in enumerate(probs):
        dv = dot(p.astype(BF16), grad)
        dp = dot_t(chunk(v, j), grad)
        ds = (p * (dp - delta)).astype(BF16)
        dk = dot(ds, query)
        dq = dot_f(chunk(k, j), ds)
        gv[j] = dv if gv[j] is None else gv[j] + dv
        gk[j] = dk if gk[j] is None else gk[j] + dk
        gq = dq if gq is None else gq + dq
    return (gq * SCALE).T


def row_forward_kernel(q_ref, k_ref, v_ref, g_ref, o_ref, lse_ref, dot_ref):
    q, k, v, g = q_ref[0], k_ref[0], v_ref[0], g_ref[0]
    for i in range(q.shape[0] // CHUNK):
        span = slice(i * CHUNK, (i + 1) * CHUNK)
        _, top, total, out = softmax_of(scores_of(chunk(q, i), k, row_bias, i), v)
        o_ref[0, 0, :, span] = out
        lse_ref[0, 0, :, span] = top + jnp.log2(total)
        grad_t = chunk(g, i).astype(F32).T
        dot_ref[0, 0, :, span] = jnp.sum(grad_t * out, axis=0, keepdims=True)


def row_forward(q, k, v, g):
    rows, length, width = q.shape
    heads = width // HEAD_DIM
    block = pl.BlockSpec((1, length, HEAD_DIM), lambda r, h: (r, 0, h))
    stat = pl.BlockSpec((1, 1, 1, length), lambda r, h: (r, h, 0, 0))
    stat_shape = jax.ShapeDtypeStruct((rows, heads, 1, length), F32)
    return pl.pallas_call(
        row_forward_kernel,
        grid=(rows, heads),
        in_specs=[block] * 4,
        out_specs=[
            pl.BlockSpec((1, 1, HEAD_DIM, length), lambda r, h: (r, h, 0, 0)),
            stat,
            stat,
        ],
        out_shape=[
            jax.ShapeDtypeStruct((rows, heads, HEAD_DIM, length), F32),
            stat_shape,
            stat_shape,
        ],
        cost_estimate=pl.CostEstimate(
            flops=rows * heads * length * length * HEAD_DIM * 8,
            bytes_accessed=rows * length * width * 12,
            transcendentals=rows * heads * length * length,
        ),
        name="row_forward",
    )(q, k, v, g)


def col_kernel(x_ref, stat_ref, y_ref, lse_ref):
    devices, _, _, per, width = x_ref.shape
    tokens = devices * per
    chunks = tokens // CHUNK
    q, k, v, g = [x_ref[:, a, 0].reshape(tokens, width) for a in range(4)]
    gk, gv = [None] * chunks, [None] * chunks
    slab = CHUNK // per
    for i in range(chunks):
        span = slice(i * CHUNK, (i + 1) * CHUNK)
        here = slice(i * slab, (i + 1) * slab)
        weights, top, total, out = softmax_of(scores_of(chunk(q, i), k, col_bias, i), v)
        lse_col = top + jnp.log2(total)
        lse_ref[0, 0, :, span] = lse_col
        out_low = out.T.astype(BF16)
        y_ref[here, 0, 0] = out_low.reshape(slab, per, width)
        lse, w_row, w_col = merge(stat_ref[0, 0, 0, :, span], lse_col)
        dot_col = jnp.sum(
            (chunk(g, i).astype(F32) * out_low.astype(F32)).T, axis=0, keepdims=True
        )
        delta = w_row * stat_ref[1, 0, 0, :, span] + w_col * dot_col
        factor = jnp.exp2(top - lse)
        probs = [w * factor for w in weights]
        gq = backward_of(i, probs, delta, q, k, v, g, gk, gv)
        y_ref[here, 1, 0] = gq.astype(BF16).reshape(slab, per, width)
    for j in range(chunks):
        here = slice(j * slab, (j + 1) * slab)
        y_ref[here, 2, 0] = (gk[j] * SCALE).astype(BF16).reshape(slab, per, width)
        y_ref[here, 3, 0] = gv[j].astype(BF16).reshape(slab, per, width)


def col_both(x, stats, first_head):
    devices, kinds, groups, per, width = x.shape
    heads = width // HEAD_DIM
    tokens = devices * per
    block = pl.BlockSpec(
        (devices, kinds, 1, per, HEAD_DIM), lambda c, h: (0, 0, c, 0, h)
    )
    return pl.pallas_call(
        col_kernel,
        grid=(groups, heads),
        in_specs=[
            block,
            pl.BlockSpec((2, 1, 1, 1, tokens), lambda c, h: (0, first_head + h, c, 0, 0)),
        ],
        out_specs=[block, pl.BlockSpec((1, 1, 1, tokens), lambda c, h: (h, c, 0, 0))],
        out_shape=[
            jax.ShapeDtypeStruct(x.shape, BF16),
            jax.ShapeDtypeStruct((heads, groups, 1, tokens), F32),
        ],
        cost_estimate=pl.CostEstimate(
            flops=groups * heads * tokens * tokens * HEAD_DIM * 20,
            bytes_accessed=x.size * 4,
            transcendentals=groups * heads * tokens * tokens,
        ),
        name="col_both",
    )(x, stats)


def row_backward_kernel(
    q_ref, k_ref, v_ref, g_ref, o_ref, lse_ref, back_ref, lse_col_ref, *rest
):
    att_ref, gq_ref, gk_ref, gv_ref = rest[-4:]
    q, k, v, g = q_ref[0], k_ref[0], v_ref[0], g_ref[0]
    length = q.shape[0]
    chunks = length // CHUNK
    devices = back_ref.shape[0]
    slab = devices // chunks

    def came_back(kind, i):
        part = back_ref[i * slab : (i + 1) * slab, kind, :, 0].astype(F32)
        return part.reshape(CHUNK, HEAD_DIM)

    gk, gv = [None] * chunks, [None] * chunks
    for i in range(chunks):
        span = slice(i * CHUNK, (i + 1) * CHUNK)
        lse, w_row, w_col = merge(lse_ref[0, 0, :, span], lse_col_ref[0, 0, :, span])
        col_t = came_back(0, i).T
        att_t = o_ref[0, 0, :, span] * w_row + col_t * w_col
        low = att_t.T.astype(BF16)
        att_ref[0, span, :] = low
        delta = jnp.sum(
            (chunk(g, i).astype(F32) * low.astype(F32)).T, axis=0, keepdims=True
        )
        scores = scores_of(chunk(q, i), k, row_bias, i)
        probs = [jnp.exp2(s - lse) for s in scores]
        gq = backward_of(i, probs, delta, q, k, v, g, gk, gv)
        gq_ref[0, span, :] = (gq + came_back(1, i)).astype(BF16)
    for j in range(chunks):
        span = slice(j * CHUNK, (j + 1) * CHUNK)
        gk_ref[0, span, :] = (gk[j] * SCALE + came_back(2, j)).astype(BF16)
        gv_ref[0, span, :] = (gv[j] + came_back(3, j)).astype(BF16)


def row_backward(q, k, v, g, o, lse, back, lse_col, first_head, earlier):
    rows, length, width = q.shape
    devices, kinds, groups, _, size, piece = back.shape
    heads = piece // HEAD_DIM
    block = pl.BlockSpec((1, length, HEAD_DIM), lambda r, h: (r, 0, first_head + h))
    stat = pl.BlockSpec((1, 1, 1, length), lambda r, h: (r, first_head + h, 0, 0))
    in_specs = [block] * 4 + [
        pl.BlockSpec((1, 1, HEAD_DIM, length), lambda r, h: (r, first_head + h, 0, 0)),
        stat,
        pl.BlockSpec(
            (devices, kinds, groups, 1, size, HEAD_DIM), lambda r, h: (0, 0, 0, r, 0, h)
        ),
        stat,
    ]
    aliases = {}
    if earlier:
        aliases = {len(in_specs) + n: n for n in range(4)}
        in_specs = in_specs + [pl.BlockSpec(memory_space=pl.ANY)] * 4
    return pl.pallas_call(
        row_backward_kernel,
        grid=(rows, heads),
        in_specs=in_specs,
        out_specs=[block] * 4,
        out_shape=[jax.ShapeDtypeStruct(q.shape, BF16)] * 4,
        input_output_aliases=aliases,
        cost_estimate=pl.CostEstimate(
            flops=rows * heads * length * length * HEAD_DIM * 14,
            bytes_accessed=rows * length * piece * 28,
            transcendentals=rows * heads * length * length,
        ),
        name="row_backward",
    )(q, k, v, g, o, lse, back, lse_col, *earlier)


def exchange(array):
    return lax.all_to_all(array, "seq", split_axis=0, concat_axis=0, tiled=True)


def by_all_to_all(queries, key_vectors, value_vectors, grad_output):
    devices = lax.axis_size("seq")
    rows = queries.shape[0] // ROW_LEN
    width = queries.shape[1]
    heads = width // HEAD_DIM
    groups = ROW_LEN // devices // GROUP
    per = rows * GROUP
    tokens = devices * per
    piece = width // PIECES
    piece_heads = piece // HEAD_DIM
    arrays = (queries, key_vectors, value_vectors, grad_output)
    by_row = [a.reshape(rows, ROW_LEN, width) for a in arrays]

    packs = []
    for n in range(PIECES):
        parts = [
            jnp.transpose(
                a[:, n * piece : (n + 1) * piece].reshape(rows, devices, groups, GROUP, piece),
                (1, 2, 0, 3, 4),
            )
            for a in arrays
        ]
        packed = jnp.stack(parts, axis=1).reshape(devices, 4, groups, per, piece)
        packs.append(packed)
    arrived = [exchange(packs[0])]

    o, lse, dots = row_forward(*by_row)
    stats = jnp.stack([lse, dots]).reshape(2, rows, heads, devices, groups, GROUP)
    stats = jnp.transpose(stats, (3, 0, 2, 4, 1, 5)).reshape(devices, -1)
    arrived[0], stats = lax.optimization_barrier((arrived[0], stats))
    stats = exchange(stats)
    for n in range(1, PIECES):
        packs[n], stats = lax.optimization_barrier((packs[n], stats))
        arrived.append(exchange(packs[n]))
    stats = stats.reshape(devices, 2, heads, groups, per)
    stats = jnp.transpose(stats, (1, 2, 3, 0, 4)).reshape(2, heads, groups, 1, tokens)

    columns = [col_both(arrived[n], stats, n * piece_heads) for n in range(PIECES)]
    lse_col = jnp.concatenate([lse_col for _, lse_col in columns], axis=0)
    lse_col = jnp.transpose(
        lse_col.reshape(heads, groups, devices, per), (2, 0, 1, 3)
    ).reshape(devices, -1)
    lse_col = exchange(lse_col)
    sent = [y for y, _ in columns]
    sent[-1], lse_col = lax.optimization_barrier((sent[-1], lse_col))
    lse_col = lse_col.reshape(devices, heads, groups, rows, GROUP)
    lse_col = jnp.transpose(lse_col, (3, 1, 0, 2, 4)).reshape(rows, heads, 1, ROW_LEN)
    backs = [exchange(y).reshape(devices, 4, groups, rows, GROUP, piece) for y in sent]

    outs = ()
    for n in range(PIECES):
        outs = row_backward(*by_row, o, lse, backs[n], lse_col, n * piece_heads, tuple(outs))
    return tuple(a.reshape(queries.shape) for a in outs)


PLANES = 4
SPLITS = 16
LANES = 128


def drain(ref, sem):
    pltpu.make_async_copy(ref, ref, sem).wait()


def fold_lanes(x):
    for shift in (8, 16, 32, 64):
        x = x + pltpu.roll(x, shift, 1)
    return x


def lane_masks():
    group = lax.broadcasted_iota(jnp.int32, (LANES // GROUP, LANES), 1) // GROUP
    row = lax.broadcasted_iota(jnp.int32, (LANES // GROUP, LANES), 0)
    return group, group == row


def to_tile(stat, block):
    group, diagonal = lane_masks()
    spread = fold_lanes(jnp.where(group == block, stat, 0.0))
    return jnp.sum(jnp.where(diagonal, spread, 0.0), axis=0, keepdims=True)


def from_tile(line, block):
    group, diagonal = lane_masks()
    spread = fold_lanes(jnp.where(diagonal, line, 0.0))
    return jnp.where(group == block, spread, 0.0)


def column_unit(q, g, keys, values, query_chunk, lse_row, dot_row):
    count = len(keys)
    scores = []
    for j in range(count):
        bias = col_bias(None, j, count - 1)
        scores.append(dot_t(keys[j], q) * (SCALE * LOG2E) + bias)
    top = functools.reduce(
        jnp.maximum, [jnp.max(s, axis=0, keepdims=True) for s in scores]
    )
    top = jnp.maximum(top, FLOOR)
    weights = [jnp.exp2(s - top) for s in scores]
    total = sum(jnp.sum(w, axis=0, keepdims=True) for w in weights)
    acc = sum(dot_f(v, w.astype(BF16)) for v, w in zip(values, weights))
    total = jnp.maximum(total, 1.0)
    out_low = (acc / total).T.astype(BF16)
    lse_col = top + jnp.log2(total)
    lse, w_row, w_col = merge(lse_row, lse_col)
    dot_col = jnp.sum(
        (g.astype(F32) * out_low.astype(F32)).T, axis=0, keepdims=True
    )
    delta = w_row * dot_row + w_col * dot_col
    factor = jnp.exp2(top - lse)
    gq, gk, gv = None, [], []
    for j in range(count):
        p = weights[j] * factor
        gv.append(dot(p.astype(BF16), g))
        dp = dot_t(values[j], g)
        ds = (p * (dp - delta)).astype(BF16)
        gk.append(dot(ds, q) * SCALE)
        dq = dot_f(keys[j], ds)
        gq = dq if gq is None else gq + dq
    return out_low, (gq * SCALE).T.astype(BF16), gk, gv, lse_col


def stat_line(ref, r, i):
    base = i * (CHUNK // LANES)
    return jnp.concatenate(
        [ref[base + n, pl.ds(r, 1), :] for n in range(CHUNK // LANES)], axis=1
    )


def row_gradients(q, k, v, g, o_row, lse_row, lse_col, came_back, give):
    count = q.shape[0] // CHUNK
    gk, gv = [None] * count, [None] * count
    for i in range(count):
        span = slice(i * CHUNK, (i + 1) * CHUNK)
        lse, w_row, w_col = merge(lse_row(i), lse_col(i))
        att_t = o_row(span) * w_row + came_back(0, i).T * w_col
        att = att_t.T.astype(BF16)
        give(0, i, att)
        delta = jnp.sum(
            (chunk(g, i).astype(F32) * att.astype(F32)).T, axis=0, keepdims=True
        )
        scores = scores_of(chunk(q, i), k, row_bias, i)
        probs = [jnp.exp2(s - lse) for s in scores]
        gq = backward_of(i, probs, delta, q, k, v, g, gk, gv)
        give(1, i, gq + came_back(1, i))
    for j in range(count):
        give(2, j, gk[j] * SCALE + came_back(2, j))
        give(3, j, gv[j] + came_back(3, j))


def tail_kernel(*refs):
    done, (q, k, v, g) = refs[0:4], [ref[0] for ref in refs[4:8]]
    back, o_row, st_row, lse_back = refs[8:12]
    outs = refs[12:]
    r = pl.program_id(0)
    width = done[0].shape[2]

    def came_back(kind, i):
        return back[kind, 0, i * CHUNK:(i + 1) * CHUNK].astype(F32)

    def give(kind, i, value):
        outs[kind][0, i * CHUNK:(i + 1) * CHUNK, width:] = value.astype(BF16)

    for n in range(4):
        outs[n][0, :, :width] = done[n][0]
    row_gradients(
        q, k, v, g,
        lambda span: o_row[0, :, span],
        lambda i: stat_line(st_row, r, i),
        lambda i: stat_line(lse_back, r, i),
        came_back, give,
    )


def finish(done, flat, back, o_row, st_row, lse_back):
    rows, length, width = flat[0].shape
    last = width // HEAD_DIM - 1
    lines = pl.BlockSpec(st_row.shape, lambda r: (0, 0, 0))
    return pl.pallas_call(
        tail_kernel,
        grid=(rows,),
        in_specs=[pl.BlockSpec((1, length, done[0].shape[2]), lambda r: (r, 0, 0))] * 4
        + [pl.BlockSpec((1, length, HEAD_DIM), lambda r: (r, 0, last))] * 4
        + [
            pl.BlockSpec((4, 1, length, HEAD_DIM), lambda r: (0, r, 0, 0)),
            pl.BlockSpec((1, HEAD_DIM, length), lambda r: (r, 0, 0)),
            lines, lines,
        ],
        out_specs=[pl.BlockSpec((1, length, width), lambda r: (r, 0, 0))] * 4,
        out_shape=[jax.ShapeDtypeStruct((rows, length, width), BF16)] * 4,
        name="finish",
    )(*done, *flat, back, o_row, st_row, lse_back)


def fused_kernel(*refs):
    xs, flat, outs = refs[0:4], refs[4:8], refs[8:12]
    tail_back, tail_o, tail_row, tail_col = refs[12:16]
    (xin, own, far, low, back, orow, st_row, st_own, st_far, lse_own, lse_far,
     lse_back, in_sem, a_loc, a_send, a_recv, b_send, bkv_recv, bqg_recv,
     k1_send, k1_recv, k0_send, k0_recv, d2_send, d2_recv, d1_send, d1_recv,
     e_send, e_recv, s_send, s_recv, sf_send, sf_recv, l1_send, l1_recv,
     le_send, le_recv, out_sem, tail_sem) = refs[16:]
    heads, _, rows = xin.shape[:3]
    chunks = own.shape[0]
    plane_rows, per = own.shape[2], own.shape[3]
    splits = chunks // heads
    devices = lax.axis_size("seq")
    m = devices // PLANES
    blocks = per * splits
    seq, head_index = lax.axis_index("seq"), lax.axis_index("head")
    z, p = seq // m, seq % m
    first = z * m

    def send(src, dst, send_sem, recv_sem, to):
        pltpu.make_async_remote_copy(
            src_ref=src, dst_ref=dst, send_sem=send_sem, recv_sem=recv_sem,
            device_id=(to, head_index), device_id_type=pl.DeviceIdType.MESH,
        ).start()

    outer = (z == 0) | (z == PLANES - 1)
    inner_peer = jnp.where(z == 0, seq + m, seq - m)
    outer_peer = jnp.where(z == 1, seq - m, seq + m)

    barrier = pltpu.get_barrier_semaphore()
    for d in range(1, m):
        pl.semaphore_signal(barrier, inc=1, device_id=(first + (p + d) % m, head_index),
                            device_id_type=pl.DeviceIdType.MESH)
    for d in range(1, PLANES):
        pl.semaphore_signal(barrier, inc=1,
                            device_id=((z + d) % PLANES * m + p, head_index),
                            device_id_type=pl.DeviceIdType.MESH)

    def lanes_of(h):
        return pl.ds(pl.multiple_of(h * HEAD_DIM, HEAD_DIM), HEAD_DIM)

    def load_rows(h, carry):
        for kind in range(4):
            pltpu.make_async_copy(
                flat[kind].at[:, :, lanes_of(h)], xin.at[h, kind], in_sem.at[h]
            ).start()
        return carry

    load_rows(0, 0)
    pl.semaphore_wait(barrier, m - 1 + PLANES - 1)

    def spread_chunk(c, carry):
        h, part = c // splits, c % splits
        for d in range(1, m):
            peer = (p + d) % m
            for kind in range(4):
                send(
                    xs[kind].at[:, pl.ds(peer * blocks + part * per, per), :, lanes_of(h)],
                    own.at[c, kind, pl.ds(p * rows, rows)],
                    a_send, a_recv.at[c], first + peer,
                )
        for kind in range(4):
            pltpu.make_async_copy(
                xs[kind].at[:, pl.ds(p * blocks + part * per, per), :, lanes_of(h)],
                own.at[c, kind, pl.ds(p * rows, rows)],
                a_loc.at[c],
            ).start()
        return carry

    lax.fori_loop(0, AHEAD, spread_chunk, 0)
    lax.fori_loop(1, heads, load_rows, 0)

    def forward_row(h, r):
        q, k, v, g = [xin[h, kind, r] for kind in range(4)]
        for i in range(q.shape[0] // CHUNK):
            span = slice(i * CHUNK, (i + 1) * CHUNK)
            _, top, total, out = softmax_of(scores_of(chunk(q, i), k, row_bias, i), v)
            orow[h, r, :, span] = out
            lse = top + jnp.log2(total)
            grad_t = chunk(g, i).astype(F32).T
            dots = jnp.sum(grad_t * out, axis=0, keepdims=True)
            for part in range(CHUNK // LANES):
                lanes = slice(part * LANES, (part + 1) * LANES)
                at = i * (CHUNK // LANES) + part
                st_row[2 * h, at, pl.ds(r, 1), :] = lse[:, lanes]
                st_row[2 * h + 1, at, pl.ds(r, 1), :] = dots[:, lanes]

    def send_stats(h):
        pair = pl.ds(2 * h, 2)
        for d in range(1, m):
            peer = (p + d) % m
            send(st_row.at[pair, peer], st_own.at[pair, p], s_send, s_recv.at[h], first + peer)
        st_own[pair, p] = st_row[pair, p]

    def wait_stats(h):
        drain(st_own.at[pl.ds(2 * h, 2), pl.ds(0, m - 1)], s_recv.at[h])

    def pass_stats(h):
        wait_stats(h)
        pair = pl.ds(2 * h, 2)
        send(st_own.at[pair], st_far.at[pair], sf_send, sf_recv.at[h], inner_peer)

    def tile(ref, *at):
        return ref[at].reshape(plane_rows * GROUP, HEAD_DIM)

    def put(ref, at, value):
        ref[at] = value.astype(BF16).reshape(plane_rows, GROUP, HEAD_DIM)

    def stat_of(ref, which, block):
        return to_tile(ref[which].reshape(plane_rows, LANES), block)

    def add_lse(ref, h, line, block):
        ref[h] = ref[h] + from_tile(line, block).reshape(m, rows, LANES)

    half = plane_rows * GROUP

    def solve(c, lower):
        h, part = c // splits, c % splits
        pair = (far, own) if lower else (own, far)
        lses = (lse_far, lse_own) if lower else (lse_own, lse_far)
        stats = (st_far, st_own) if lower else (st_own, st_far)

        @pl.when(part == 0)
        def _():
            wait_stats(h)
            drain(st_far.at[pl.ds(2 * h, 2)], sf_recv.at[h])
            lse_own[h] = jnp.zeros(lse_own.shape[1:], F32)
            lse_far[h] = jnp.zeros(lse_far.shape[1:], F32)

        def body(b, carry):
            block = part * per + b
            every = slice(None)

            def both(kind):
                return jnp.concatenate([tile(ref, c, kind, every, b) for ref in pair], axis=0)

            q, k, v, g = [both(kind) for kind in range(4)]
            keys, values = [k], [v]
            if not lower:
                keys = [jnp.concatenate([tile(low, c, 0, every, b), tile(low, c, 2, every, b)], axis=0), k]
                values = [jnp.concatenate([tile(low, c, 1, every, b), tile(low, c, 3, every, b)], axis=0), v]
            lse_row = jnp.concatenate([stat_of(s, 2 * h, block) for s in stats], axis=1)
            dot_row = jnp.concatenate([stat_of(s, 2 * h + 1, block) for s in stats], axis=1)
            o, gq, gk, gv, lse_col = column_unit(q, g, keys, values, None, lse_row, dot_row)
            gk_own, gv_own = gk[-1], gv[-1]
            if lower:
                gk_own = gk_own + jnp.concatenate(
                    [tile(low, c, 0, every, b), tile(low, c, 2, every, b)], axis=0).astype(F32)
                gv_own = gv_own + jnp.concatenate(
                    [tile(low, c, 1, every, b), tile(low, c, 3, every, b)], axis=0).astype(F32)
            else:
                put(low, (c, 0, every, b), gk[0][:half])
                put(low, (c, 1, every, b), gv[0][:half])
                put(low, (c, 2, every, b), gk[0][half:])
                put(low, (c, 3, every, b), gv[0][half:])
            for n, ref in enumerate(pair):
                span = slice(n * half, (n + 1) * half)
                for kind, value in enumerate((o, gq, gk_own, gv_own)):
                    put(ref, (c, kind, every, b), value[span])
                add_lse(lses[n], h, lse_col[:, span], block)
            return carry

        lax.fori_loop(0, per, body, 0)

    def return_rows(c, ref):
        h, part = c // splits, c % splits
        at = pl.ds(p * blocks + part * per, per)
        for d in range(1, m):
            peer = (p + d) % m
            send(
                ref.at[c, :, pl.ds(peer * rows, rows)], back.at[h, :, :, at],
                e_send, e_recv.at[h], first + peer,
            )
        back[h, :, :, at] = ref[c, :, pl.ds(p * rows, rows)]

        @pl.when(part == splits - 1)
        def _():
            for d in range(1, m):
                peer = (p + d) % m
                send(lse_own.at[h, peer], lse_back.at[h, p], le_send, le_recv.at[h], first + peer)
            lse_back[h, p] = lse_own[h, p]

    def return_far(c):
        h, part = c // splits, c % splits
        send(far.at[c], far.at[c], d1_send, d1_recv.at[c], outer_peer)

        @pl.when(part == splits - 1)
        def _():
            send(lse_far.at[h], lse_own.at[h], l1_send, l1_recv.at[h], outer_peer)

    def pass_on(c):
        drain(own.at[c, :, pl.ds(0, rows * (m - 1))], a_recv.at[c])
        drain(own.at[c, :, pl.ds(0, rows)], a_loc.at[c])

        @pl.when(outer)
        def _():
            send(own.at[c, pl.ds(1, 2)], far.at[c, pl.ds(1, 2)], b_send, bkv_recv.at[c], inner_peer)
            send(own.at[c, 0], far.at[c, 0], b_send, bqg_recv.at[c, 0], inner_peer)
            send(own.at[c, 3], far.at[c, 3], b_send, bqg_recv.at[c, 1], inner_peer)

        @pl.when(z == 1)
        def _():
            send(own.at[c, pl.ds(1, 2)], low.at[c, pl.ds(2, 2)], k1_send.at[c], k1_recv.at[c], seq + m)

    def pass_far(c):
        drain(far.at[c, pl.ds(1, 2)], bkv_recv.at[c])
        send(far.at[c, pl.ds(1, 2)], low.at[c, pl.ds(0, 2)], k0_send.at[c], k0_recv.at[c], seq + m)

    def wait_qg(c):
        drain(far.at[c, 0], bqg_recv.at[c, 0])
        drain(far.at[c, 3], bqg_recv.at[c, 1])

    def upper(c):
        drain(far.at[c, pl.ds(1, 2)], bkv_recv.at[c])
        wait_qg(c)
        drain(low.at[c, pl.ds(2, 2)], k1_recv.at[c])
        drain(low.at[c, pl.ds(0, 2)], k0_recv.at[c])
        solve(c, False)
        send(low.at[c], low.at[c], d2_send, d2_recv.at[c], seq - m)
        return_far(c)
        return_rows(c, own)

    def lower(c):
        wait_qg(c)
        drain(low.at[c], d2_recv.at[c])
        drain(own.at[c, pl.ds(1, 2)], k1_send.at[c])
        drain(far.at[c, pl.ds(1, 2)], k0_send.at[c])
        solve(c, True)
        return_far(c)
        return_rows(c, own)

    def edge(c):
        h, part = c // splits, c % splits
        drain(far.at[c], d1_recv.at[c])

        @pl.when(part == splits - 1)
        def _():
            drain(lse_own.at[h], l1_recv.at[h])

        return_rows(c, far)

    def backward_row(h, r):
        slab = CHUNK // GROUP

        def came_back(kind, i):
            return back[h, kind, r, i * slab:(i + 1) * slab].reshape(CHUNK, HEAD_DIM).astype(F32)

        def give(kind, i, value):
            back[h, kind, r, i * slab:(i + 1) * slab] = value.astype(BF16).reshape(slab, GROUP, HEAD_DIM)

        row_gradients(
            *[xin[h, kind, r] for kind in range(4)],
            lambda span: orow[h, r, :, span],
            lambda i: stat_line(st_row.at[2 * h], r, i),
            lambda i: stat_line(lse_back.at[h], r, i),
            came_back, give,
        )

    def backward_ready(h):
        drain(back.at[h, :, :, pl.ds(0, blocks * (m - 1))], e_recv.at[h])
        drain(lse_back.at[h, pl.ds(0, m - 1)], le_recv.at[h])

    def give_out(h):
        for kind in range(4):
            pltpu.make_async_copy(
                back.at[h, kind], outs[kind].at[:, :, :, lanes_of(h)], out_sem
            ).start()

    lag_upper, lag_lower, lag_edge, lag_rows = LAGS
    pace = splits // rows

    def rows_forward(s):
        h = s // splits + 1

        @pl.when((h < heads) & (s % splits == 0))
        def _():
            drain(xin.at[h], in_sem.at[h])

        @pl.when((h < heads) & (s % pace == 0))
        def _():
            forward_row(h, s % splits // pace)

        @pl.when((h < heads) & (s % splits == (rows - 1) * pace))
        def _():
            send_stats(h)

        @pl.when((h < heads) & (s % splits == splits - 1) & outer)
        def _():
            pass_stats(h)

        @pl.when((h == heads - 1) & (s % splits == splits - 1))
        def _():
            pltpu.make_async_copy(orow.at[h], tail_o, tail_sem.at[2]).start()
            pltpu.make_async_copy(st_row.at[2 * h], tail_row, tail_sem.at[3]).start()

    def rows_backward(t):
        h = t // splits

        @pl.when((t >= 0) & (t % splits == 0))
        def _():
            backward_ready(h)

        @pl.when((t >= 0) & (h < heads - 1) & (t % pace == 0))
        def _():
            backward_row(h, t % splits // pace)

        @pl.when((t >= 0) & (h < heads - 1) & (t % splits == (rows - 1) * pace))
        def _():
            give_out(h)

    def step(s, carry):
        def at(lag, role=None):
            ready = (s >= lag) & (s < chunks + lag)
            return ready if role is None else ready & role

        @pl.when(at(0))
        def _():
            pass_on(s)

        @pl.when(s + AHEAD < chunks)
        def _():
            spread_chunk(s + AHEAD, 0)

        @pl.when(at(1, z == 1))
        def _():
            pass_far(s - 1)

        @pl.when((s == 0) & outer)
        def _():
            pass_stats(0)

        @pl.when(at(lag_upper, z == 2))
        def _():
            upper(s - lag_upper)

        @pl.when(at(lag_lower, z == 1))
        def _():
            lower(s - lag_lower)

        @pl.when(at(lag_edge, outer))
        def _():
            edge(s - lag_edge)

        rows_forward(s)
        rows_backward(s - lag_rows - (splits - 1))
        return carry

    drain(xin.at[0], in_sem.at[0])

    def first_head(r, carry):
        forward_row(0, r)
        return carry

    lax.fori_loop(0, rows, first_head, 0)
    send_stats(0)
    lax.fori_loop(0, chunks + lag_rows, step, 0)

    drain(own.at[:, :, pl.ds(0, rows * (m - 1))], a_send)
    drain(own.at[:, :, pl.ds(0, rows * (m - 1))], e_send)
    drain(st_own.at[:, pl.ds(0, m - 1)], s_send)
    drain(lse_own.at[:, pl.ds(0, m - 1)], le_send)

    @pl.when(outer)
    def _():
        drain(own, b_send)
        drain(st_far, sf_send)

    @pl.when((z == 1) | (z == 2))
    def _():
        drain(far, d1_send)
        drain(lse_far, l1_send)

    @pl.when(z == 2)
    def _():
        drain(low, d2_send)

    last = heads - 1
    copies = [
        pltpu.make_async_copy(back.at[last], tail_back, tail_sem.at[0]),
        pltpu.make_async_copy(lse_back.at[last], tail_col, tail_sem.at[1]),
    ]
    for copy in copies:
        copy.start()
    for copy in copies:
        copy.wait()
    pltpu.make_async_copy(orow.at[last], tail_o, tail_sem.at[2]).wait()
    pltpu.make_async_copy(st_row.at[2 * last], tail_row, tail_sem.at[3]).wait()
    drain(back.at[pl.ds(0, last)], out_sem)


AHEAD = 2
LAGS = (2, 5, 7, 9)


def fits(tokens, width, devices):
    rows = tokens // ROW_LEN
    if tokens % ROW_LEN or devices % PLANES or width % HEAD_DIM:
        return False
    m = devices // PLANES
    blocks = ROW_LEN // GROUP
    return (
        m > 1
        and width > HEAD_DIM
        and ROW_LEN // m == LANES
        and rows * m * GROUP == LANES
        and (blocks // m) % SPLITS == 0
        and SPLITS % rows == 0
    )


def by_planes(queries, key_vectors, value_vectors, grad_output):
    devices = lax.axis_size("seq")
    m = devices // PLANES
    tokens, width = queries.shape
    rows, heads, blocks = tokens // ROW_LEN, width // HEAD_DIM, ROW_LEN // GROUP
    per = blocks // m // SPLITS
    chunks = heads * SPLITS
    arrays = (queries, key_vectors, value_vectors, grad_output)
    views = [a.reshape(rows, blocks, GROUP, width) for a in arrays]
    flat = [a.reshape(rows, ROW_LEN, width) for a in arrays]
    buffer = pltpu.VMEM((chunks, 4, rows * m, per, GROUP, HEAD_DIM), BF16)
    dma = pltpu.SemaphoreType.DMA
    stat = pltpu.VMEM((2 * heads, m, rows, LANES), F32)
    lse = pltpu.VMEM((heads, m, rows, LANES), F32)
    each, single = dma((chunks,)), dma(())
    outs = pl.pallas_call(
        fused_kernel,
        in_specs=[pl.BlockSpec(memory_space=pl.ANY)] * 8,
        out_specs=[pl.BlockSpec(memory_space=pl.ANY)] * 8,
        out_shape=[jax.ShapeDtypeStruct((rows, blocks, GROUP, width - HEAD_DIM), BF16)] * 4
        + [
            jax.ShapeDtypeStruct((4, rows, blocks, GROUP, HEAD_DIM), BF16),
            jax.ShapeDtypeStruct((rows, HEAD_DIM, ROW_LEN), F32),
            jax.ShapeDtypeStruct((m, rows, LANES), F32),
            jax.ShapeDtypeStruct((m, rows, LANES), F32),
        ],
        scratch_shapes=[
            pltpu.VMEM((heads, 4, rows, ROW_LEN, HEAD_DIM), BF16),
            buffer, buffer, buffer,
            pltpu.VMEM((heads, 4, rows, blocks, GROUP, HEAD_DIM), BF16),
            pltpu.VMEM((heads, rows, HEAD_DIM, ROW_LEN), F32),
            stat, stat, stat, lse, lse, lse,
            dma((heads,)), each, single, each, single, each, dma((chunks, 2)),
            each, each, each, each, single, each, single, each,
            single, dma((heads,)), single, dma((heads,)), single, dma((heads,)),
            single, dma((heads,)), single, dma((heads,)), single, dma((4,)),
        ],
        compiler_params=pltpu.CompilerParams(
            collective_id=0, has_side_effects=True, vmem_limit_bytes=63 * 1024 * 1024
        ),
        cost_estimate=pl.CostEstimate(
            flops=tokens * width * 512 * 24,
            bytes_accessed=tokens * width * 16,
            transcendentals=tokens * width,
        ),
        name="by_planes",
    )(*views, *flat)
    done = [a.reshape(rows, ROW_LEN, width - HEAD_DIM) for a in outs[:4]]
    back = outs[4].reshape(4, rows, ROW_LEN, HEAD_DIM)
    outs = finish(done, flat, back, *outs[5:])
    return tuple(a.reshape(queries.shape) for a in outs)


def on_device(queries, key_vectors, value_vectors, grad_output):
    arrays = (queries, key_vectors, value_vectors, grad_output)
    if fits(*queries.shape, lax.axis_size("seq")):
        return by_planes(*arrays)
    return by_all_to_all(*arrays)


def solution(mesh):
    spec = P("seq", "head")
    return jax.shard_map(
        on_device,
        mesh=mesh,
        in_specs=(spec,) * 4,
        out_specs=(spec,) * 4,
        check_vma=False,
    )
```

```python
import functools
import math

import jax
import jax.numpy as jnp
from jax import lax
from jax.experimental import pallas as pl
from jax.experimental.pallas import tpu as pltpu
from jax.sharding import PartitionSpec as P

ROW_LEN = 512
HEAD_DIM = 128
GROUP = 8
CHUNK = 256
PIECES = 2
MASKED = -1e30
FLOOR = -1e20
LOG2E = 1.0 / math.log(2.0)
SCALE = 1.0 / math.sqrt(HEAD_DIM)
F32 = jnp.float32
BF16 = jnp.bfloat16


def dot_t(left, right):
    return lax.dot_general(left, right, (((1,), (1,)), ((), ())), preferred_element_type=F32)


def dot_f(left, right):
    return lax.dot_general(left, right, (((0,), (0,)), ((), ())), preferred_element_type=F32)


def dot(left, right):
    return jnp.dot(left, right, preferred_element_type=F32)


def row_bias(first, key_chunk, query_chunk):
    if key_chunk < query_chunk:
        return None
    keys = lax.broadcasted_iota(jnp.int32, (CHUNK, CHUNK), 0)
    queries = lax.broadcasted_iota(jnp.int32, (CHUNK, CHUNK), 1)
    return jnp.where(keys <= queries, 0.0, MASKED)


def col_bias(first, key_chunk, query_chunk):
    keys = lax.broadcasted_iota(jnp.int32, (CHUNK, CHUNK), 0)
    queries = lax.broadcasted_iota(jnp.int32, (CHUNK, CHUNK), 1)
    gap = queries - keys
    same = (gap & (GROUP - 1)) == 0
    if key_chunk == query_chunk:
        same = same & (gap > 0)
    return jnp.where(same, 0.0, MASKED)


def chunk(array, index):
    return array[index * CHUNK : (index + 1) * CHUNK]


def scores_of(query, keys, bias, query_chunk):
    out = []
    for j in range(query_chunk + 1):
        s = dot_t(chunk(keys, j), query) * (SCALE * LOG2E)
        b = bias(None, j, query_chunk)
        out.append(s if b is None else s + b)
    return out


def softmax_of(scores, values):
    top = functools.reduce(
        jnp.maximum, [jnp.max(s, axis=0, keepdims=True) for s in scores]
    )
    top = jnp.maximum(top, FLOOR)
    weights = [jnp.exp2(s - top) for s in scores]
    total = sum(jnp.sum(w, axis=0, keepdims=True) for w in weights)
    acc = sum(dot_f(chunk(values, j), w.astype(BF16)) for j, w in enumerate(weights))
    total = jnp.maximum(total, 1.0)
    return weights, top, total, acc / total


def merge(left, right):
    top = jnp.maximum(left, right)
    w_left, w_right = jnp.exp2(left - top), jnp.exp2(right - top)
    den = w_left + w_right
    return top + jnp.log2(den), w_left / den, w_right / den


def backward_of(i, probs, delta, q, k, v, g, gk, gv):
    query, grad = chunk(q, i), chunk(g, i)
    gq = None
    for j, p in enumerate(probs):
        dv = dot(p.astype(BF16), grad)
        dp = dot_t(chunk(v, j), grad)
        ds = (p * (dp - delta)).astype(BF16)
        dk = dot(ds, query)
        dq = dot_f(chunk(k, j), ds)
        gv[j] = dv if gv[j] is None else gv[j] + dv
        gk[j] = dk if gk[j] is None else gk[j] + dk
        gq = dq if gq is None else gq + dq
    return (gq * SCALE).T


def row_forward_kernel(q_ref, k_ref, v_ref, g_ref, o_ref, lse_ref, dot_ref):
    q, k, v, g = q_ref[0], k_ref[0], v_ref[0], g_ref[0]
    for i in range(q.shape[0] // CHUNK):
        span = slice(i * CHUNK, (i + 1) * CHUNK)
        _, top, total, out = softmax_of(scores_of(chunk(q, i), k, row_bias, i), v)
        o_ref[0, 0, :, span] = out
        lse_ref[0, 0, :, span] = top + jnp.log2(total)
        grad_t = chunk(g, i).astype(F32).T
        dot_ref[0, 0, :, span] = jnp.sum(grad_t * out, axis=0, keepdims=True)


def row_forward(q, k, v, g):
    rows, length, width = q.shape
    heads = width // HEAD_DIM
    block = pl.BlockSpec((1, length, HEAD_DIM), lambda r, h: (r, 0, h))
    stat = pl.BlockSpec((1, 1, 1, length), lambda r, h: (r, h, 0, 0))
    stat_shape = jax.ShapeDtypeStruct((rows, heads, 1, length), F32)
    return pl.pallas_call(
        row_forward_kernel,
        grid=(rows, heads),
        in_specs=[block] * 4,
        out_specs=[
            pl.BlockSpec((1, 1, HEAD_DIM, length), lambda r, h: (r, h, 0, 0)),
            stat,
            stat,
        ],
        out_shape=[
            jax.ShapeDtypeStruct((rows, heads, HEAD_DIM, length), F32),
            stat_shape,
            stat_shape,
        ],
        cost_estimate=pl.CostEstimate(
            flops=rows * heads * length * length * HEAD_DIM * 8,
            bytes_accessed=rows * length * width * 12,
            transcendentals=rows * heads * length * length,
        ),
        name="row_forward",
    )(q, k, v, g)


def col_kernel(x_ref, stat_ref, y_ref, lse_ref):
    devices, _, _, per, width = x_ref.shape
    tokens = devices * per
    chunks = tokens // CHUNK
    q, k, v, g = [x_ref[:, a, 0].reshape(tokens, width) for a in range(4)]
    gk, gv = [None] * chunks, [None] * chunks
    slab = CHUNK // per
    for i in range(chunks):
        span = slice(i * CHUNK, (i + 1) * CHUNK)
        here = slice(i * slab, (i + 1) * slab)
        weights, top, total, out = softmax_of(scores_of(chunk(q, i), k, col_bias, i), v)
        lse_col = top + jnp.log2(total)
        lse_ref[0, 0, :, span] = lse_col
        out_low = out.T.astype(BF16)
        y_ref[here, 0, 0] = out_low.reshape(slab, per, width)
        lse, w_row, w_col = merge(stat_ref[0, 0, 0, :, span], lse_col)
        dot_col = jnp.sum(
            (chunk(g, i).astype(F32) * out_low.astype(F32)).T, axis=0, keepdims=True
        )
        delta = w_row * stat_ref[1, 0, 0, :, span] + w_col * dot_col
        factor = jnp.exp2(top - lse)
        probs = [w * factor for w in weights]
        gq = backward_of(i, probs, delta, q, k, v, g, gk, gv)
        y_ref[here, 1, 0] = gq.astype(BF16).reshape(slab, per, width)
    for j in range(chunks):
        here = slice(j * slab, (j + 1) * slab)
        y_ref[here, 2, 0] = (gk[j] * SCALE).astype(BF16).reshape(slab, per, width)
        y_ref[here, 3, 0] = gv[j].astype(BF16).reshape(slab, per, width)


def col_both(x, stats, first_head):
    devices, kinds, groups, per, width = x.shape
    heads = width // HEAD_DIM
    tokens = devices * per
    block = pl.BlockSpec(
        (devices, kinds, 1, per, HEAD_DIM), lambda c, h: (0, 0, c, 0, h)
    )
    return pl.pallas_call(
        col_kernel,
        grid=(groups, heads),
        in_specs=[
            block,
            pl.BlockSpec((2, 1, 1, 1, tokens), lambda c, h: (0, first_head + h, c, 0, 0)),
        ],
        out_specs=[block, pl.BlockSpec((1, 1, 1, tokens), lambda c, h: (h, c, 0, 0))],
        out_shape=[
            jax.ShapeDtypeStruct(x.shape, BF16),
            jax.ShapeDtypeStruct((heads, groups, 1, tokens), F32),
        ],
        cost_estimate=pl.CostEstimate(
            flops=groups * heads * tokens * tokens * HEAD_DIM * 20,
            bytes_accessed=x.size * 4,
            transcendentals=groups * heads * tokens * tokens,
        ),
        name="col_both",
    )(x, stats)


def row_backward_kernel(
    q_ref, k_ref, v_ref, g_ref, o_ref, lse_ref, back_ref, lse_col_ref, *rest
):
    att_ref, gq_ref, gk_ref, gv_ref = rest[-4:]
    q, k, v, g = q_ref[0], k_ref[0], v_ref[0], g_ref[0]
    length = q.shape[0]
    chunks = length // CHUNK
    devices = back_ref.shape[0]
    slab = devices // chunks

    def came_back(kind, i):
        part = back_ref[i * slab : (i + 1) * slab, kind, :, 0].astype(F32)
        return part.reshape(CHUNK, HEAD_DIM)

    gk, gv = [None] * chunks, [None] * chunks
    for i in range(chunks):
        span = slice(i * CHUNK, (i + 1) * CHUNK)
        lse, w_row, w_col = merge(lse_ref[0, 0, :, span], lse_col_ref[0, 0, :, span])
        col_t = came_back(0, i).T
        att_t = o_ref[0, 0, :, span] * w_row + col_t * w_col
        low = att_t.T.astype(BF16)
        att_ref[0, span, :] = low
        delta = jnp.sum(
            (chunk(g, i).astype(F32) * low.astype(F32)).T, axis=0, keepdims=True
        )
        scores = scores_of(chunk(q, i), k, row_bias, i)
        probs = [jnp.exp2(s - lse) for s in scores]
        gq = backward_of(i, probs, delta, q, k, v, g, gk, gv)
        gq_ref[0, span, :] = (gq + came_back(1, i)).astype(BF16)
    for j in range(chunks):
        span = slice(j * CHUNK, (j + 1) * CHUNK)
        gk_ref[0, span, :] = (gk[j] * SCALE + came_back(2, j)).astype(BF16)
        gv_ref[0, span, :] = (gv[j] + came_back(3, j)).astype(BF16)


def row_backward(q, k, v, g, o, lse, back, lse_col, first_head, earlier):
    rows, length, width = q.shape
    devices, kinds, groups, _, size, piece = back.shape
    heads = piece // HEAD_DIM
    block = pl.BlockSpec((1, length, HEAD_DIM), lambda r, h: (r, 0, first_head + h))
    stat = pl.BlockSpec((1, 1, 1, length), lambda r, h: (r, first_head + h, 0, 0))
    in_specs = [block] * 4 + [
        pl.BlockSpec((1, 1, HEAD_DIM, length), lambda r, h: (r, first_head + h, 0, 0)),
        stat,
        pl.BlockSpec(
            (devices, kinds, groups, 1, size, HEAD_DIM), lambda r, h: (0, 0, 0, r, 0, h)
        ),
        stat,
    ]
    aliases = {}
    if earlier:
        aliases = {len(in_specs) + n: n for n in range(4)}
        in_specs = in_specs + [pl.BlockSpec(memory_space=pl.ANY)] * 4
    return pl.pallas_call(
        row_backward_kernel,
        grid=(rows, heads),
        in_specs=in_specs,
        out_specs=[block] * 4,
        out_shape=[jax.ShapeDtypeStruct(q.shape, BF16)] * 4,
        input_output_aliases=aliases,
        cost_estimate=pl.CostEstimate(
            flops=rows * heads * length * length * HEAD_DIM * 14,
            bytes_accessed=rows * length * piece * 28,
            transcendentals=rows * heads * length * length,
        ),
        name="row_backward",
    )(q, k, v, g, o, lse, back, lse_col, *earlier)


def exchange(array):
    return lax.all_to_all(array, "seq", split_axis=0, concat_axis=0, tiled=True)


def by_all_to_all(queries, key_vectors, value_vectors, grad_output):
    devices = lax.axis_size("seq")
    rows = queries.shape[0] // ROW_LEN
    width = queries.shape[1]
    heads = width // HEAD_DIM
    groups = ROW_LEN // devices // GROUP
    per = rows * GROUP
    tokens = devices * per
    piece = width // PIECES
    piece_heads = piece // HEAD_DIM
    arrays = (queries, key_vectors, value_vectors, grad_output)
    by_row = [a.reshape(rows, ROW_LEN, width) for a in arrays]

    packs = []
    for n in range(PIECES):
        parts = [
            jnp.transpose(
                a[:, n * piece : (n + 1) * piece].reshape(rows, devices, groups, GROUP, piece),
                (1, 2, 0, 3, 4),
            )
            for a in arrays
        ]
        packed = jnp.stack(parts, axis=1).reshape(devices, 4, groups, per, piece)
        packs.append(packed)
    arrived = [exchange(packs[0])]

    o, lse, dots = row_forward(*by_row)
    stats = jnp.stack([lse, dots]).reshape(2, rows, heads, devices, groups, GROUP)
    stats = jnp.transpose(stats, (3, 0, 2, 4, 1, 5)).reshape(devices, -1)
    arrived[0], stats = lax.optimization_barrier((arrived[0], stats))
    stats = exchange(stats)
    for n in range(1, PIECES):
        packs[n], stats = lax.optimization_barrier((packs[n], stats))
        arrived.append(exchange(packs[n]))
    stats = stats.reshape(devices, 2, heads, groups, per)
    stats = jnp.transpose(stats, (1, 2, 3, 0, 4)).reshape(2, heads, groups, 1, tokens)

    columns = [col_both(arrived[n], stats, n * piece_heads) for n in range(PIECES)]
    lse_col = jnp.concatenate([lse_col for _, lse_col in columns], axis=0)
    lse_col = jnp.transpose(
        lse_col.reshape(heads, groups, devices, per), (2, 0, 1, 3)
    ).reshape(devices, -1)
    lse_col = exchange(lse_col)
    sent = [y for y, _ in columns]
    sent[-1], lse_col = lax.optimization_barrier((sent[-1], lse_col))
    lse_col = lse_col.reshape(devices, heads, groups, rows, GROUP)
    lse_col = jnp.transpose(lse_col, (3, 1, 0, 2, 4)).reshape(rows, heads, 1, ROW_LEN)
    backs = [exchange(y).reshape(devices, 4, groups, rows, GROUP, piece) for y in sent]

    outs = ()
    for n in range(PIECES):
        outs = row_backward(*by_row, o, lse, backs[n], lse_col, n * piece_heads, tuple(outs))
    return tuple(a.reshape(queries.shape) for a in outs)


PLANES = 4
SPLITS = 16
LANES = 128


def drain(ref, sem):
    pltpu.make_async_copy(ref, ref, sem).wait()


def fold_lanes(x):
    for shift in (8, 16, 32, 64):
        x = x + pltpu.roll(x, shift, 1)
    return x


def lane_masks():
    group = lax.broadcasted_iota(jnp.int32, (LANES // GROUP, LANES), 1) // GROUP
    row = lax.broadcasted_iota(jnp.int32, (LANES // GROUP, LANES), 0)
    return group, group == row


def to_tile(stat, block):
    group, diagonal = lane_masks()
    spread = fold_lanes(jnp.where(group == block, stat, 0.0))
    return jnp.sum(jnp.where(diagonal, spread, 0.0), axis=0, keepdims=True)


def from_tile(line, block):
    group, diagonal = lane_masks()
    spread = fold_lanes(jnp.where(diagonal, line, 0.0))
    return jnp.where(group == block, spread, 0.0)


def column_unit(q, g, keys, values, query_chunk, lse_row, dot_row):
    count = len(keys)
    scores = []
    for j in range(count):
        bias = col_bias(None, j, count - 1)
        scores.append(dot_t(keys[j], q) * (SCALE * LOG2E) + bias)
    top = functools.reduce(
        jnp.maximum, [jnp.max(s, axis=0, keepdims=True) for s in scores]
    )
    top = jnp.maximum(top, FLOOR)
    weights = [jnp.exp2(s - top) for s in scores]
    total = sum(jnp.sum(w, axis=0, keepdims=True) for w in weights)
    acc = sum(dot_f(v, w.astype(BF16)) for v, w in zip(values, weights))
    total = jnp.maximum(total, 1.0)
    out_low = (acc / total).T.astype(BF16)
    lse_col = top + jnp.log2(total)
    lse, w_row, w_col = merge(lse_row, lse_col)
    dot_col = jnp.sum(
        (g.astype(F32) * out_low.astype(F32)).T, axis=0, keepdims=True
    )
    delta = w_row * dot_row + w_col * dot_col
    factor = jnp.exp2(top - lse)
    gq, gk, gv = None, [], []
    for j in range(count):
        p = weights[j] * factor
        gv.append(dot(p.astype(BF16), g))
        dp = dot_t(values[j], g)
        ds = (p * (dp - delta)).astype(BF16)
        gk.append(dot(ds, q) * SCALE)
        dq = dot_f(keys[j], ds)
        gq = dq if gq is None else gq + dq
    return out_low, (gq * SCALE).T.astype(BF16), gk, gv, lse_col


def stat_line(ref, r, i):
    base = i * (CHUNK // LANES)
    return jnp.concatenate(
        [ref[base + n, pl.ds(r, 1), :] for n in range(CHUNK // LANES)], axis=1
    )


def row_gradients(q, k, v, g, o_row, lse_row, lse_col, came_back, give):
    count = q.shape[0] // CHUNK
    gk, gv = [None] * count, [None] * count
    for i in range(count):
        span = slice(i * CHUNK, (i + 1) * CHUNK)
        lse, w_row, w_col = merge(lse_row(i), lse_col(i))
        att_t = o_row(span) * w_row + came_back(0, i).T * w_col
        att = att_t.T.astype(BF16)
        give(0, i, att)
        delta = jnp.sum(
            (chunk(g, i).astype(F32) * att.astype(F32)).T, axis=0, keepdims=True
        )
        scores = scores_of(chunk(q, i), k, row_bias, i)
        probs = [jnp.exp2(s - lse) for s in scores]
        gq = backward_of(i, probs, delta, q, k, v, g, gk, gv)
        give(1, i, gq + came_back(1, i))
    return gk, gv


def copy_kernel(*refs):
    ins, outs = refs[0:4], refs[4:8]
    held, in_sem, out_sem = refs[8:]
    rows = held.shape[1]
    fetches = [
        pltpu.make_async_copy(ins[n].at[r], held.at[n, r], in_sem.at[n, r])
        for r in range(rows) for n in range(4)
    ]
    stores = [
        pltpu.make_async_copy(held.at[n, r], outs[n].at[r], out_sem.at[n, r])
        for r in range(rows) for n in range(4)
    ]
    for fetch in fetches:
        fetch.start()
    for fetch, store in zip(fetches, stores):
        fetch.wait()
        store.start()
    for store in stores:
        store.wait()


def copy_out(arrays):
    shape = arrays[0].shape
    sems = pltpu.SemaphoreType.DMA((4, shape[0]))
    return pl.pallas_call(
        copy_kernel,
        in_specs=[pl.BlockSpec(memory_space=pl.ANY)] * 4,
        out_specs=[pl.BlockSpec(memory_space=pl.ANY)] * 4,
        out_shape=[jax.ShapeDtypeStruct(shape, BF16)] * 4,
        scratch_shapes=[pltpu.VMEM((4, *shape), BF16), sems, sems],
        name="copy_out",
    )(*arrays)


def fused_kernel(*refs):
    xs, flat, outs = refs[0:4], refs[4:8], refs[8:12]
    (xin, own, far, low, back, orow, ring, row_sum, st_row, st_own, st_far,
     lse_own, lse_far, lse_back, in_sem, a_loc, a_send, a_recv, b_send, bkv_recv,
     bqg_recv, k1_send, k1_recv, k0_send, k0_recv, d2_send, d2_recv, d1_send,
     d1_recv, f1_send, f1_recv, e_send, e_recv, g_send, g_recv, s_send, s_recv, sf_send, sf_recv, l1_send, l1_recv,
     le_send, le_recv, out_sem) = refs[12:]
    heads, _, rows = xin.shape[:3]
    chunks = own.shape[0]
    plane_rows, per = own.shape[2], own.shape[3]
    splits = chunks // heads
    devices = lax.axis_size("seq")
    m = devices // PLANES
    blocks = per * splits
    seq, head_index = lax.axis_index("seq"), lax.axis_index("head")
    z, p = seq // m, seq % m
    first = z * m

    def send(src, dst, send_sem, recv_sem, to):
        pltpu.make_async_remote_copy(
            src_ref=src, dst_ref=dst, send_sem=send_sem, recv_sem=recv_sem,
            device_id=(to, head_index), device_id_type=pl.DeviceIdType.MESH,
        ).start()

    outer = (z == 0) | (z == PLANES - 1)
    inner_peer = jnp.where(z == 0, seq + m, seq - m)
    outer_peer = jnp.where(z == 1, seq - m, seq + m)

    barrier = pltpu.get_barrier_semaphore()
    for d in range(1, m):
        pl.semaphore_signal(barrier, inc=1, device_id=(first + (p + d) % m, head_index),
                            device_id_type=pl.DeviceIdType.MESH)
    for d in range(1, PLANES):
        pl.semaphore_signal(barrier, inc=1,
                            device_id=((z + d) % PLANES * m + p, head_index),
                            device_id_type=pl.DeviceIdType.MESH)

    def lanes_of(h):
        return pl.ds(pl.multiple_of(h * HEAD_DIM, HEAD_DIM), HEAD_DIM)

    def load_rows(h, carry):
        for kind in range(4):
            pltpu.make_async_copy(
                flat[kind].at[:, :, lanes_of(h)], xin.at[h, kind], in_sem.at[h]
            ).start()
        return carry

    load_rows(0, 0)
    pl.semaphore_wait(barrier, m - 1 + PLANES - 1)

    def spread_chunk(c, carry):
        h, part = c // splits, c % splits
        for d in range(1, m):
            peer = (p + d) % m
            for kind in range(4):
                send(
                    xs[kind].at[:, pl.ds(peer * blocks + part * per, per), :, lanes_of(h)],
                    own.at[c, kind, pl.ds(p * rows, rows)],
                    a_send, a_recv.at[c], first + peer,
                )
        for kind in range(4):
            pltpu.make_async_copy(
                xs[kind].at[:, pl.ds(p * blocks + part * per, per), :, lanes_of(h)],
                own.at[c, kind, pl.ds(p * rows, rows)],
                a_loc.at[c],
            ).start()
        return carry

    lax.fori_loop(0, AHEAD, spread_chunk, 0)
    lax.fori_loop(1, heads, load_rows, 0)

    def forward_row(h, r):
        q, g, k, v = [xin[h, kind, r] for kind in range(4)]
        for i in range(q.shape[0] // CHUNK):
            span = slice(i * CHUNK, (i + 1) * CHUNK)
            _, top, total, out = softmax_of(scores_of(chunk(q, i), k, row_bias, i), v)
            orow[h, r, :, span] = out
            lse = top + jnp.log2(total)
            grad_t = chunk(g, i).astype(F32).T
            dots = jnp.sum(grad_t * out, axis=0, keepdims=True)
            for part in range(CHUNK // LANES):
                lanes = slice(part * LANES, (part + 1) * LANES)
                at = i * (CHUNK // LANES) + part
                st_row[2 * h, at, pl.ds(r, 1), :] = lse[:, lanes]
                st_row[2 * h + 1, at, pl.ds(r, 1), :] = dots[:, lanes]

    def send_stats(h):
        pair = pl.ds(2 * h, 2)
        for d in range(1, m):
            peer = (p + d) % m
            send(st_row.at[pair, peer], st_own.at[pair, p], s_send, s_recv.at[h], first + peer)
        st_own[pair, p] = st_row[pair, p]

    def wait_stats(h):
        drain(st_own.at[pl.ds(2 * h, 2), pl.ds(0, m - 1)], s_recv.at[h])

    def pass_stats(h):
        wait_stats(h)
        pair = pl.ds(2 * h, 2)
        send(st_own.at[pair], st_far.at[pair], sf_send, sf_recv.at[h], inner_peer)

    def tile(ref, *at):
        return ref[at].reshape(plane_rows * GROUP, HEAD_DIM)

    def put(ref, at, value):
        ref[at] = value.astype(BF16).reshape(plane_rows, GROUP, HEAD_DIM)

    def stat_of(ref, which, block):
        return to_tile(ref[which].reshape(plane_rows, LANES), block)

    def add_lse(ref, h, line, block):
        ref[h] = ref[h] + from_tile(line, block).reshape(m, rows, LANES)

    half = plane_rows * GROUP

    def solve(c, lower):
        h, part = c // splits, c % splits
        pair = (far, own) if lower else (own, far)
        lses = (lse_far, lse_own) if lower else (lse_own, lse_far)
        stats = (st_far, st_own) if lower else (st_own, st_far)

        @pl.when(part == 0)
        def _():
            wait_stats(h)
            drain(st_far.at[pl.ds(2 * h, 2)], sf_recv.at[h])
            lse_own[h] = jnp.zeros(lse_own.shape[1:], F32)
            lse_far[h] = jnp.zeros(lse_far.shape[1:], F32)

        def body(b, carry):
            block = part * per + b
            every = slice(None)

            def both(kind):
                return jnp.concatenate([tile(ref, c, kind, every, b) for ref in pair], axis=0)

            q, g, k, v = [both(kind) for kind in range(4)]
            keys, values = [k], [v]
            if not lower:
                keys = [jnp.concatenate([tile(low, c, 0, every, b), tile(low, c, 2, every, b)], axis=0), k]
                values = [jnp.concatenate([tile(low, c, 1, every, b), tile(low, c, 3, every, b)], axis=0), v]
            lse_row = jnp.concatenate([stat_of(s, 2 * h, block) for s in stats], axis=1)
            dot_row = jnp.concatenate([stat_of(s, 2 * h + 1, block) for s in stats], axis=1)
            o, gq, gk, gv, lse_col = column_unit(q, g, keys, values, None, lse_row, dot_row)
            if lower:
                ring[c % ring.shape[0], b, 0] = gk[-1]
                ring[c % ring.shape[0], b, 1] = gv[-1]
                values = (o, gq)
            else:
                put(low, (c, 0, every, b), gk[0][:half])
                put(low, (c, 1, every, b), gv[0][:half])
                put(low, (c, 2, every, b), gk[0][half:])
                put(low, (c, 3, every, b), gv[0][half:])
                values = (o, gq, gk[-1], gv[-1])
            for n, ref in enumerate(pair):
                span = slice(n * half, (n + 1) * half)
                for kind, value in enumerate(values):
                    put(ref, (c, kind, every, b), value[span])
                add_lse(lses[n], h, lse_col[:, span], block)
            return carry

        lax.fori_loop(0, per, body, 0)

    def add_upper(c):
        def body(b, carry):
            for kind in range(2):
                total = ring[c % ring.shape[0], b, kind]
                for n, ref in enumerate((far, own)):
                    share = tile(low, c, 2 * n + kind, slice(None), b).astype(F32)
                    put(ref, (c, 2 + kind, slice(None), b), total[n * half:(n + 1) * half] + share)
            return carry

        lax.fori_loop(0, per, body, 0)

    early, late = pl.ds(0, 2), pl.ds(2, 2)

    def return_rows(c, ref, kinds, send_sem, recv_sem):
        h, part = c // splits, c % splits
        at = pl.ds(p * blocks + part * per, per)
        for d in range(1, m):
            peer = (p + d) % m
            send(
                ref.at[c, kinds, pl.ds(peer * rows, rows)], back.at[h, kinds, :, at],
                send_sem, recv_sem.at[h], first + peer,
            )
        back[h, kinds, :, at] = ref[c, kinds, pl.ds(p * rows, rows)]

    def return_first(c, ref):
        h, part = c // splits, c % splits
        return_rows(c, ref, early, e_send, e_recv)

        @pl.when(part == splits - 1)
        def _():
            for d in range(1, m):
                peer = (p + d) % m
                send(lse_own.at[h, peer], lse_back.at[h, p], le_send, le_recv.at[h], first + peer)
            lse_back[h, p] = lse_own[h, p]

    def return_second(c, ref):
        return_rows(c, ref, late, g_send, g_recv)

    def far_first(c):
        h, part = c // splits, c % splits
        send(far.at[c, early], far.at[c, early], d1_send, d1_recv.at[c], outer_peer)

        @pl.when(part == splits - 1)
        def _():
            send(lse_far.at[h], lse_own.at[h], l1_send, l1_recv.at[h], outer_peer)

    def far_second(c):
        send(far.at[c, late], far.at[c, late], f1_send, f1_recv.at[c], outer_peer)

    def pass_on(c):
        drain(own.at[c, :, pl.ds(0, rows * (m - 1))], a_recv.at[c])
        drain(own.at[c, :, pl.ds(0, rows)], a_loc.at[c])

        @pl.when(outer)
        def _():
            send(own.at[c, late], far.at[c, late], b_send, bkv_recv.at[c], inner_peer)
            send(own.at[c, early], far.at[c, early], b_send, bqg_recv.at[c], inner_peer)

        @pl.when(z == 1)
        def _():
            send(own.at[c, late], low.at[c, pl.ds(2, 2)], k1_send.at[c], k1_recv.at[c], seq + m)

    def pass_far(c):
        drain(far.at[c, late], bkv_recv.at[c])
        send(far.at[c, late], low.at[c, pl.ds(0, 2)], k0_send.at[c], k0_recv.at[c], seq + m)

    def upper(c):
        drain(far.at[c, late], bkv_recv.at[c])
        drain(far.at[c, early], bqg_recv.at[c])
        drain(low.at[c, pl.ds(2, 2)], k1_recv.at[c])
        drain(low.at[c, pl.ds(0, 2)], k0_recv.at[c])
        solve(c, False)
        send(low.at[c], low.at[c], d2_send, d2_recv.at[c], seq - m)
        far_first(c)
        return_first(c, own)
        far_second(c)
        return_second(c, own)

    def lower_first(c):
        drain(far.at[c, early], bqg_recv.at[c])
        solve(c, True)
        far_first(c)
        return_first(c, own)

    def lower_second(c):
        drain(low.at[c], d2_recv.at[c])
        drain(own.at[c, late], k1_send.at[c])
        drain(far.at[c, late], k0_send.at[c])
        add_upper(c)
        far_second(c)
        return_second(c, own)

    def edge_first(c):
        h, part = c // splits, c % splits
        drain(far.at[c, early], d1_recv.at[c])

        @pl.when(part == splits - 1)
        def _():
            drain(lse_own.at[h], l1_recv.at[h])

        return_first(c, far)

    def edge_second(c):
        drain(far.at[c, late], f1_recv.at[c])
        return_second(c, far)

    def backward_row(h, r):
        slab = CHUNK // GROUP

        def came_back(kind, i):
            return back[h, kind, r, i * slab:(i + 1) * slab].reshape(CHUNK, HEAD_DIM).astype(F32)

        def give(kind, i, value):
            back[h, kind, r, i * slab:(i + 1) * slab] = value.astype(BF16).reshape(slab, GROUP, HEAD_DIM)

        q, g, k, v = [xin[h, kind, r] for kind in range(4)]
        gk, gv = row_gradients(
            q, k, v, g,
            lambda span: orow[h, r, :, span],
            lambda i: stat_line(st_row.at[2 * h], r, i),
            lambda i: stat_line(lse_back.at[h], r, i),
            came_back, give,
        )
        for j in range(len(gk)):
            span = slice(j * CHUNK, (j + 1) * CHUNK)
            row_sum[r, 0, span] = gk[j] * SCALE
            row_sum[r, 1, span] = gv[j]

    ready = pl.ds(0, blocks * (m - 1))

    def backward_ready(h):
        drain(back.at[h, early, :, ready], e_recv.at[h])
        drain(lse_back.at[h, pl.ds(0, m - 1)], le_recv.at[h])

    def give_out(h, kind):
        pltpu.make_async_copy(
            back.at[h, kind], outs[kind].at[:, :, :, lanes_of(h)], out_sem
        ).start()

    def backward_done(h):
        drain(back.at[h, late, :, ready], g_recv.at[h])

        def body(r, carry):
            for n in range(2):
                share = back[h, 2 + n, r].reshape(ROW_LEN, HEAD_DIM).astype(F32)
                total = (row_sum[r, n] + share).astype(BF16)
                back[h, 2 + n, r] = total.reshape(back.shape[3:])
            return carry

        lax.fori_loop(0, rows, body, 0)
        give_out(h, 2)
        give_out(h, 3)

    lag_upper, lag_low1, lag_low2, lag_edge1, lag_edge2, lag_rows = LAGS
    pace = splits // rows

    def rows_forward(s):
        h = s // splits + 1

        @pl.when((h < heads) & (s % splits == 0))
        def _():
            drain(xin.at[h], in_sem.at[h])

        @pl.when((h < heads) & (s % pace == 0))
        def _():
            forward_row(h, s % splits // pace)

        @pl.when((h < heads) & (s % splits == (rows - 1) * pace))
        def _():
            send_stats(h)

        @pl.when((h < heads) & (s % splits == splits - 1) & outer)
        def _():
            pass_stats(h)

    def rows_backward(t):
        h = t // splits
        last = h == heads - 1

        @pl.when((t >= 0) & (t % splits == 0))
        def _():
            backward_ready(h)

        @pl.when((t >= 0) & ((t % pace == 0) & ~last | (t == chunks - splits)))
        def _():
            def body(r, carry):
                backward_row(h, r)
                return carry

            start = jnp.where(last, 0, t % splits // pace)
            lax.fori_loop(start, jnp.where(last, rows, start + 1), body, 0)

        @pl.when((t >= 0) & ((t % splits == splits - 1) & ~last | (t == chunks - splits)))
        def _():
            give_out(h, 0)
            give_out(h, 1)

        @pl.when((t >= 0) & (t % splits == splits - 1) & ~last)
        def _():
            backward_done(h)

    def step(s, carry):
        def at(lag, role=None):
            ready = (s >= lag) & (s < chunks + lag)
            return ready if role is None else ready & role

        @pl.when(at(0))
        def _():
            pass_on(s)

        @pl.when(s + AHEAD < chunks)
        def _():
            spread_chunk(s + AHEAD, 0)

        @pl.when(at(1, z == 1))
        def _():
            pass_far(s - 1)

        @pl.when((s == 0) & outer)
        def _():
            pass_stats(0)

        @pl.when(at(lag_upper, z == 2))
        def _():
            upper(s - lag_upper)

        @pl.when(at(lag_low1, z == 1))
        def _():
            lower_first(s - lag_low1)

        @pl.when(at(lag_low2, z == 1))
        def _():
            lower_second(s - lag_low2)

        @pl.when(at(lag_edge1, outer))
        def _():
            edge_first(s - lag_edge1)

        @pl.when(at(lag_edge2, outer))
        def _():
            edge_second(s - lag_edge2)

        rows_forward(s)
        rows_backward(s - lag_rows - (splits - 1))
        return carry

    drain(xin.at[0], in_sem.at[0])

    def first_head(r, carry):
        forward_row(0, r)
        return carry

    lax.fori_loop(0, rows, first_head, 0)
    send_stats(0)
    lax.fori_loop(0, chunks + max(LAGS), step, 0)
    backward_done(heads - 1)

    drain(own.at[:, :, pl.ds(0, rows * (m - 1))], a_send)
    drain(own.at[:, early, pl.ds(0, rows * (m - 1))], e_send)
    drain(own.at[:, late, pl.ds(0, rows * (m - 1))], g_send)
    drain(st_own.at[:, pl.ds(0, m - 1)], s_send)
    drain(lse_own.at[:, pl.ds(0, m - 1)], le_send)

    @pl.when(outer)
    def _():
        drain(own, b_send)
        drain(st_far, sf_send)

    @pl.when((z == 1) | (z == 2))
    def _():
        drain(far.at[:, early], d1_send)
        drain(far.at[:, late], f1_send)
        drain(lse_far, l1_send)

    @pl.when(z == 2)
    def _():
        drain(low, d2_send)

    drain(back, out_sem)


AHEAD = 2
RING = 8
LAGS = (2, 2, 5, 4, 7, 6)


def fits(tokens, width, devices):
    rows = tokens // ROW_LEN
    if tokens % ROW_LEN or devices % PLANES or width % HEAD_DIM:
        return False
    m = devices // PLANES
    blocks = ROW_LEN // GROUP
    return (
        m > 1
        and ROW_LEN // m == LANES
        and rows * m * GROUP == LANES
        and (blocks // m) % SPLITS == 0
        and SPLITS % rows == 0
    )


def by_planes(queries, key_vectors, value_vectors, grad_output):
    devices = lax.axis_size("seq")
    m = devices // PLANES
    tokens, width = queries.shape
    rows, heads, blocks = tokens // ROW_LEN, width // HEAD_DIM, ROW_LEN // GROUP
    per = blocks // m // SPLITS
    chunks = heads * SPLITS
    arrays = (queries, grad_output, key_vectors, value_vectors)
    views = [a.reshape(rows, blocks, GROUP, width) for a in arrays]
    flat = [a.reshape(rows, ROW_LEN, width) for a in arrays]
    buffer = pltpu.VMEM((chunks, 4, rows * m, per, GROUP, HEAD_DIM), BF16)
    dma = pltpu.SemaphoreType.DMA
    stat = pltpu.VMEM((2 * heads, m, rows, LANES), F32)
    lse = pltpu.VMEM((heads, m, rows, LANES), F32)
    each, by_head, single = dma((chunks,)), dma((heads,)), dma(())
    outs = pl.pallas_call(
        fused_kernel,
        in_specs=[pl.BlockSpec(memory_space=pl.ANY)] * 8,
        out_specs=[pl.BlockSpec(memory_space=pl.ANY)] * 4,
        out_shape=[jax.ShapeDtypeStruct(views[0].shape, BF16)] * 4,
        scratch_shapes=[
            pltpu.VMEM((heads, 4, rows, ROW_LEN, HEAD_DIM), BF16),
            buffer, buffer, buffer,
            pltpu.VMEM((heads, 4, rows, blocks, GROUP, HEAD_DIM), BF16),
            pltpu.VMEM((heads, rows, HEAD_DIM, ROW_LEN), F32),
            pltpu.VMEM((RING, per, 2, 2 * LANES, HEAD_DIM), F32),
            pltpu.VMEM((rows, 2, ROW_LEN, HEAD_DIM), F32),
            stat, stat, stat, lse, lse, lse,
            by_head, each, single, each, single, each, each,
            each, each, each, each, single, each, single,
            each, single, each, single, by_head, single, by_head,
            single, by_head, single, by_head, single, by_head, single, by_head,
            single,
        ],
        compiler_params=pltpu.CompilerParams(
            collective_id=0, has_side_effects=True, vmem_limit_bytes=63 * 1024 * 1024
        ),
        cost_estimate=pl.CostEstimate(
            flops=tokens * width * 512 * 24,
            bytes_accessed=tokens * width * 16,
            transcendentals=tokens * width,
        ),
        name="by_planes",
    )(*views, *flat)
    outs = copy_out(outs)
    return tuple(a.reshape(queries.shape) for a in outs)


def on_device(queries, key_vectors, value_vectors, grad_output):
    arrays = (queries, key_vectors, value_vectors, grad_output)
    if fits(*queries.shape, lax.axis_size("seq")):
        return by_planes(*arrays)
    return by_all_to_all(*arrays)


def solution(mesh):
    spec = P("seq", "head")
    return jax.shard_map(
        on_device,
        mesh=mesh,
        in_specs=(spec,) * 4,
        out_specs=(spec,) * 4,
        check_vma=False,
    )
```

```python
import functools
import math

import jax
import jax.numpy as jnp
from jax import lax
from jax.experimental import pallas as pl
from jax.experimental.pallas import tpu as pltpu
from jax.sharding import PartitionSpec as P

ROW_LEN = 512
HEAD_DIM = 128
GROUP = 8
CHUNK = 256
PIECES = 2
MASKED = -1e30
FLOOR = -1e20
LOG2E = 1.0 / math.log(2.0)
SCALE = 1.0 / math.sqrt(HEAD_DIM)
F32 = jnp.float32
BF16 = jnp.bfloat16


def dot_t(left, right):
    return lax.dot_general(left, right, (((1,), (1,)), ((), ())), preferred_element_type=F32)


def dot_f(left, right):
    return lax.dot_general(left, right, (((0,), (0,)), ((), ())), preferred_element_type=F32)


def dot(left, right):
    return jnp.dot(left, right, preferred_element_type=F32)


def row_bias(first, key_chunk, query_chunk):
    if key_chunk < query_chunk:
        return None
    keys = lax.broadcasted_iota(jnp.int32, (CHUNK, CHUNK), 0)
    queries = lax.broadcasted_iota(jnp.int32, (CHUNK, CHUNK), 1)
    return jnp.where(keys <= queries, 0.0, MASKED)


def col_bias(first, key_chunk, query_chunk):
    keys = lax.broadcasted_iota(jnp.int32, (CHUNK, CHUNK), 0)
    queries = lax.broadcasted_iota(jnp.int32, (CHUNK, CHUNK), 1)
    gap = queries - keys
    same = (gap & (GROUP - 1)) == 0
    if key_chunk == query_chunk:
        same = same & (gap > 0)
    return jnp.where(same, 0.0, MASKED)


def chunk(array, index):
    return array[index * CHUNK : (index + 1) * CHUNK]


def scores_of(query, keys, bias, query_chunk):
    out = []
    for j in range(query_chunk + 1):
        s = dot_t(chunk(keys, j), query) * (SCALE * LOG2E)
        b = bias(None, j, query_chunk)
        out.append(s if b is None else s + b)
    return out


def softmax_of(scores, values):
    top = functools.reduce(
        jnp.maximum, [jnp.max(s, axis=0, keepdims=True) for s in scores]
    )
    top = jnp.maximum(top, FLOOR)
    weights = [jnp.exp2(s - top) for s in scores]
    total = sum(jnp.sum(w, axis=0, keepdims=True) for w in weights)
    acc = sum(dot_f(chunk(values, j), w.astype(BF16)) for j, w in enumerate(weights))
    total = jnp.maximum(total, 1.0)
    return weights, top, total, acc / total


def merge(left, right):
    top = jnp.maximum(left, right)
    w_left, w_right = jnp.exp2(left - top), jnp.exp2(right - top)
    den = w_left + w_right
    return top + jnp.log2(den), w_left / den, w_right / den


def backward_of(i, probs, delta, q, k, v, g, gk, gv):
    query, grad = chunk(q, i), chunk(g, i)
    gq = None
    for j, p in enumerate(probs):
        dv = dot(p.astype(BF16), grad)
        dp = dot_t(chunk(v, j), grad)
        ds = (p * (dp - delta)).astype(BF16)
        dk = dot(ds, query)
        dq = dot_f(chunk(k, j), ds)
        gv[j] = dv if gv[j] is None else gv[j] + dv
        gk[j] = dk if gk[j] is None else gk[j] + dk
        gq = dq if gq is None else gq + dq
    return (gq * SCALE).T


def row_forward_kernel(q_ref, k_ref, v_ref, g_ref, o_ref, lse_ref, dot_ref):
    q, k, v, g = q_ref[0], k_ref[0], v_ref[0], g_ref[0]
    for i in range(q.shape[0] // CHUNK):
        span = slice(i * CHUNK, (i + 1) * CHUNK)
        _, top, total, out = softmax_of(scores_of(chunk(q, i), k, row_bias, i), v)
        o_ref[0, 0, :, span] = out
        lse_ref[0, 0, :, span] = top + jnp.log2(total)
        grad_t = chunk(g, i).astype(F32).T
        dot_ref[0, 0, :, span] = jnp.sum(grad_t * out, axis=0, keepdims=True)


def row_forward(q, k, v, g):
    rows, length, width = q.shape
    heads = width // HEAD_DIM
    block = pl.BlockSpec((1, length, HEAD_DIM), lambda r, h: (r, 0, h))
    stat = pl.BlockSpec((1, 1, 1, length), lambda r, h: (r, h, 0, 0))
    stat_shape = jax.ShapeDtypeStruct((rows, heads, 1, length), F32)
    return pl.pallas_call(
        row_forward_kernel,
        grid=(rows, heads),
        in_specs=[block] * 4,
        out_specs=[
            pl.BlockSpec((1, 1, HEAD_DIM, length), lambda r, h: (r, h, 0, 0)),
            stat,
            stat,
        ],
        out_shape=[
            jax.ShapeDtypeStruct((rows, heads, HEAD_DIM, length), F32),
            stat_shape,
            stat_shape,
        ],
        cost_estimate=pl.CostEstimate(
            flops=rows * heads * length * length * HEAD_DIM * 8,
            bytes_accessed=rows * length * width * 12,
            transcendentals=rows * heads * length * length,
        ),
        name="row_forward",
    )(q, k, v, g)


def col_kernel(x_ref, stat_ref, y_ref, lse_ref):
    devices, _, _, per, width = x_ref.shape
    tokens = devices * per
    chunks = tokens // CHUNK
    q, k, v, g = [x_ref[:, a, 0].reshape(tokens, width) for a in range(4)]
    gk, gv = [None] * chunks, [None] * chunks
    slab = CHUNK // per
    for i in range(chunks):
        span = slice(i * CHUNK, (i + 1) * CHUNK)
        here = slice(i * slab, (i + 1) * slab)
        weights, top, total, out = softmax_of(scores_of(chunk(q, i), k, col_bias, i), v)
        lse_col = top + jnp.log2(total)
        lse_ref[0, 0, :, span] = lse_col
        out_low = out.T.astype(BF16)
        y_ref[here, 0, 0] = out_low.reshape(slab, per, width)
        lse, w_row, w_col = merge(stat_ref[0, 0, 0, :, span], lse_col)
        dot_col = jnp.sum(
            (chunk(g, i).astype(F32) * out_low.astype(F32)).T, axis=0, keepdims=True
        )
        delta = w_row * stat_ref[1, 0, 0, :, span] + w_col * dot_col
        factor = jnp.exp2(top - lse)
        probs = [w * factor for w in weights]
        gq = backward_of(i, probs, delta, q, k, v, g, gk, gv)
        y_ref[here, 1, 0] = gq.astype(BF16).reshape(slab, per, width)
    for j in range(chunks):
        here = slice(j * slab, (j + 1) * slab)
        y_ref[here, 2, 0] = (gk[j] * SCALE).astype(BF16).reshape(slab, per, width)
        y_ref[here, 3, 0] = gv[j].astype(BF16).reshape(slab, per, width)


def col_both(x, stats, first_head):
    devices, kinds, groups, per, width = x.shape
    heads = width // HEAD_DIM
    tokens = devices * per
    block = pl.BlockSpec(
        (devices, kinds, 1, per, HEAD_DIM), lambda c, h: (0, 0, c, 0, h)
    )
    return pl.pallas_call(
        col_kernel,
        grid=(groups, heads),
        in_specs=[
            block,
            pl.BlockSpec((2, 1, 1, 1, tokens), lambda c, h: (0, first_head + h, c, 0, 0)),
        ],
        out_specs=[block, pl.BlockSpec((1, 1, 1, tokens), lambda c, h: (h, c, 0, 0))],
        out_shape=[
            jax.ShapeDtypeStruct(x.shape, BF16),
            jax.ShapeDtypeStruct((heads, groups, 1, tokens), F32),
        ],
        cost_estimate=pl.CostEstimate(
            flops=groups * heads * tokens * tokens * HEAD_DIM * 20,
            bytes_accessed=x.size * 4,
            transcendentals=groups * heads * tokens * tokens,
        ),
        name="col_both",
    )(x, stats)


def row_backward_kernel(
    q_ref, k_ref, v_ref, g_ref, o_ref, lse_ref, back_ref, lse_col_ref, *rest
):
    att_ref, gq_ref, gk_ref, gv_ref = rest[-4:]
    q, k, v, g = q_ref[0], k_ref[0], v_ref[0], g_ref[0]
    length = q.shape[0]
    chunks = length // CHUNK
    devices = back_ref.shape[0]
    slab = devices // chunks

    def came_back(kind, i):
        part = back_ref[i * slab : (i + 1) * slab, kind, :, 0].astype(F32)
        return part.reshape(CHUNK, HEAD_DIM)

    gk, gv = [None] * chunks, [None] * chunks
    for i in range(chunks):
        span = slice(i * CHUNK, (i + 1) * CHUNK)
        lse, w_row, w_col = merge(lse_ref[0, 0, :, span], lse_col_ref[0, 0, :, span])
        col_t = came_back(0, i).T
        att_t = o_ref[0, 0, :, span] * w_row + col_t * w_col
        low = att_t.T.astype(BF16)
        att_ref[0, span, :] = low
        delta = jnp.sum(
            (chunk(g, i).astype(F32) * low.astype(F32)).T, axis=0, keepdims=True
        )
        scores = scores_of(chunk(q, i), k, row_bias, i)
        probs = [jnp.exp2(s - lse) for s in scores]
        gq = backward_of(i, probs, delta, q, k, v, g, gk, gv)
        gq_ref[0, span, :] = (gq + came_back(1, i)).astype(BF16)
    for j in range(chunks):
        span = slice(j * CHUNK, (j + 1) * CHUNK)
        gk_ref[0, span, :] = (gk[j] * SCALE + came_back(2, j)).astype(BF16)
        gv_ref[0, span, :] = (gv[j] + came_back(3, j)).astype(BF16)


def row_backward(q, k, v, g, o, lse, back, lse_col, first_head, earlier):
    rows, length, width = q.shape
    devices, kinds, groups, _, size, piece = back.shape
    heads = piece // HEAD_DIM
    block = pl.BlockSpec((1, length, HEAD_DIM), lambda r, h: (r, 0, first_head + h))
    stat = pl.BlockSpec((1, 1, 1, length), lambda r, h: (r, first_head + h, 0, 0))
    in_specs = [block] * 4 + [
        pl.BlockSpec((1, 1, HEAD_DIM, length), lambda r, h: (r, first_head + h, 0, 0)),
        stat,
        pl.BlockSpec(
            (devices, kinds, groups, 1, size, HEAD_DIM), lambda r, h: (0, 0, 0, r, 0, h)
        ),
        stat,
    ]
    aliases = {}
    if earlier:
        aliases = {len(in_specs) + n: n for n in range(4)}
        in_specs = in_specs + [pl.BlockSpec(memory_space=pl.ANY)] * 4
    return pl.pallas_call(
        row_backward_kernel,
        grid=(rows, heads),
        in_specs=in_specs,
        out_specs=[block] * 4,
        out_shape=[jax.ShapeDtypeStruct(q.shape, BF16)] * 4,
        input_output_aliases=aliases,
        cost_estimate=pl.CostEstimate(
            flops=rows * heads * length * length * HEAD_DIM * 14,
            bytes_accessed=rows * length * piece * 28,
            transcendentals=rows * heads * length * length,
        ),
        name="row_backward",
    )(q, k, v, g, o, lse, back, lse_col, *earlier)


def exchange(array):
    return lax.all_to_all(array, "seq", split_axis=0, concat_axis=0, tiled=True)


def by_all_to_all(queries, key_vectors, value_vectors, grad_output):
    devices = lax.axis_size("seq")
    rows = queries.shape[0] // ROW_LEN
    width = queries.shape[1]
    heads = width // HEAD_DIM
    groups = ROW_LEN // devices // GROUP
    per = rows * GROUP
    tokens = devices * per
    piece = width // PIECES
    piece_heads = piece // HEAD_DIM
    arrays = (queries, key_vectors, value_vectors, grad_output)
    by_row = [a.reshape(rows, ROW_LEN, width) for a in arrays]

    packs = []
    for n in range(PIECES):
        parts = [
            jnp.transpose(
                a[:, n * piece : (n + 1) * piece].reshape(rows, devices, groups, GROUP, piece),
                (1, 2, 0, 3, 4),
            )
            for a in arrays
        ]
        packed = jnp.stack(parts, axis=1).reshape(devices, 4, groups, per, piece)
        packs.append(packed)
    arrived = [exchange(packs[0])]

    o, lse, dots = row_forward(*by_row)
    stats = jnp.stack([lse, dots]).reshape(2, rows, heads, devices, groups, GROUP)
    stats = jnp.transpose(stats, (3, 0, 2, 4, 1, 5)).reshape(devices, -1)
    arrived[0], stats = lax.optimization_barrier((arrived[0], stats))
    stats = exchange(stats)
    for n in range(1, PIECES):
        packs[n], stats = lax.optimization_barrier((packs[n], stats))
        arrived.append(exchange(packs[n]))
    stats = stats.reshape(devices, 2, heads, groups, per)
    stats = jnp.transpose(stats, (1, 2, 3, 0, 4)).reshape(2, heads, groups, 1, tokens)

    columns = [col_both(arrived[n], stats, n * piece_heads) for n in range(PIECES)]
    lse_col = jnp.concatenate([lse_col for _, lse_col in columns], axis=0)
    lse_col = jnp.transpose(
        lse_col.reshape(heads, groups, devices, per), (2, 0, 1, 3)
    ).reshape(devices, -1)
    lse_col = exchange(lse_col)
    sent = [y for y, _ in columns]
    sent[-1], lse_col = lax.optimization_barrier((sent[-1], lse_col))
    lse_col = lse_col.reshape(devices, heads, groups, rows, GROUP)
    lse_col = jnp.transpose(lse_col, (3, 1, 0, 2, 4)).reshape(rows, heads, 1, ROW_LEN)
    backs = [exchange(y).reshape(devices, 4, groups, rows, GROUP, piece) for y in sent]

    outs = ()
    for n in range(PIECES):
        outs = row_backward(*by_row, o, lse, backs[n], lse_col, n * piece_heads, tuple(outs))
    return tuple(a.reshape(queries.shape) for a in outs)


PLANES = 4
SPLITS = 16
LANES = 128


def drain(ref, sem):
    pltpu.make_async_copy(ref, ref, sem).wait()


def fold_lanes(x):
    for shift in (8, 16, 32, 64):
        x = x + pltpu.roll(x, shift, 1)
    return x


def lane_masks():
    group = lax.broadcasted_iota(jnp.int32, (LANES // GROUP, LANES), 1) // GROUP
    row = lax.broadcasted_iota(jnp.int32, (LANES // GROUP, LANES), 0)
    return group, group == row


def to_tile(stat, block):
    group, diagonal = lane_masks()
    spread = fold_lanes(jnp.where(group == block, stat, 0.0))
    return jnp.sum(jnp.where(diagonal, spread, 0.0), axis=0, keepdims=True)


def from_tile(line, block):
    group, diagonal = lane_masks()
    spread = fold_lanes(jnp.where(diagonal, line, 0.0))
    return jnp.where(group == block, spread, 0.0)


def column_unit(q, g, keys, values, query_chunk, lse_row, dot_row):
    count = len(keys)
    scores = []
    for j in range(count):
        bias = col_bias(None, j, count - 1)
        scores.append(dot_t(keys[j], q) * (SCALE * LOG2E) + bias)
    top = functools.reduce(
        jnp.maximum, [jnp.max(s, axis=0, keepdims=True) for s in scores]
    )
    top = jnp.maximum(top, FLOOR)
    weights = [jnp.exp2(s - top) for s in scores]
    total = sum(jnp.sum(w, axis=0, keepdims=True) for w in weights)
    acc = sum(dot_f(v, w.astype(BF16)) for v, w in zip(values, weights))
    total = jnp.maximum(total, 1.0)
    out_low = (acc / total).T.astype(BF16)
    lse_col = top + jnp.log2(total)
    lse, w_row, w_col = merge(lse_row, lse_col)
    dot_col = jnp.sum(
        (g.astype(F32) * out_low.astype(F32)).T, axis=0, keepdims=True
    )
    delta = w_row * dot_row + w_col * dot_col
    factor = jnp.exp2(top - lse)
    gq, gk, gv = None, [], []
    for j in range(count):
        p = weights[j] * factor
        gv.append(dot(p.astype(BF16), g))
        dp = dot_t(values[j], g)
        ds = (p * (dp - delta)).astype(BF16)
        gk.append(dot(ds, q) * SCALE)
        dq = dot_f(keys[j], ds)
        gq = dq if gq is None else gq + dq
    return out_low, (gq * SCALE).T.astype(BF16), gk, gv, lse_col


def stat_line(ref, r, i):
    base = i * (CHUNK // LANES)
    return jnp.concatenate(
        [ref[base + n, pl.ds(r, 1), :] for n in range(CHUNK // LANES)], axis=1
    )


def row_gradients(q, k, v, g, o_row, lse_row, lse_col, came_back, give):
    count = q.shape[0] // CHUNK
    gk, gv = [None] * count, [None] * count
    for i in range(count):
        span = slice(i * CHUNK, (i + 1) * CHUNK)
        lse, w_row, w_col = merge(lse_row(i), lse_col(i))
        att_t = o_row(span) * w_row + came_back(0, i).T * w_col
        att = att_t.T.astype(BF16)
        give(0, i, att)
        delta = jnp.sum(
            (chunk(g, i).astype(F32) * att.astype(F32)).T, axis=0, keepdims=True
        )
        scores = scores_of(chunk(q, i), k, row_bias, i)
        probs = [jnp.exp2(s - lse) for s in scores]
        gq = backward_of(i, probs, delta, q, k, v, g, gk, gv)
        give(1, i, gq + came_back(1, i))
    return gk, gv


def copy_kernel(*refs):
    back, outs, sem = refs[0], refs[1:5], refs[5]
    copies = [
        pltpu.make_async_copy(
            back.at[h, n], outs[n].at[:, :, :, h * HEAD_DIM:(h + 1) * HEAD_DIM], sem.at[h, n]
        )
        for h in range(back.shape[0]) for n in range(4)
    ]
    for copy in copies:
        copy.start()
    for copy in copies:
        copy.wait()


def copy_out(back, shape):
    return pl.pallas_call(
        copy_kernel,
        in_specs=[pl.BlockSpec(memory_space=pltpu.VMEM)],
        out_specs=[pl.BlockSpec(memory_space=pl.ANY)] * 4,
        out_shape=[jax.ShapeDtypeStruct(shape, BF16)] * 4,
        scratch_shapes=[pltpu.SemaphoreType.DMA(back.shape[:2])],
        compiler_params=pltpu.CompilerParams(vmem_limit_bytes=2 * 1024 * 1024),
        name="copy_out",
    )(back)


def fused_kernel(*refs):
    xs, flat, back = refs[0:4], refs[4:8], refs[8]
    (xin, own, far, low, orow, ring, row_sum, st_row, st_own, st_far,
     lse_own, lse_far, lse_back, in_sem, a_loc, a_send, a_recv, b_send, bkv_recv,
     bqg_recv, k1_send, k1_recv, k0_send, k0_recv, d2_send, d2_recv, d1_send,
     d1_recv, f1_send, f1_recv, e_send, e_recv, g_send, g_recv, s_send, s_recv, sf_send, sf_recv, l1_send, l1_recv,
     le_send, le_recv) = refs[9:]
    heads, _, rows = xin.shape[:3]
    chunks = own.shape[0]
    plane_rows, per = own.shape[2], own.shape[3]
    splits = chunks // heads
    devices = lax.axis_size("seq")
    m = devices // PLANES
    blocks = per * splits
    seq, head_index = lax.axis_index("seq"), lax.axis_index("head")
    z, p = seq // m, seq % m
    first = z * m

    def send(src, dst, send_sem, recv_sem, to):
        pltpu.make_async_remote_copy(
            src_ref=src, dst_ref=dst, send_sem=send_sem, recv_sem=recv_sem,
            device_id=(to, head_index), device_id_type=pl.DeviceIdType.MESH,
        ).start()

    outer = (z == 0) | (z == PLANES - 1)
    inner_peer = jnp.where(z == 0, seq + m, seq - m)
    outer_peer = jnp.where(z == 1, seq - m, seq + m)

    barrier = pltpu.get_barrier_semaphore()
    for d in range(1, m):
        pl.semaphore_signal(barrier, inc=1, device_id=(first + (p + d) % m, head_index),
                            device_id_type=pl.DeviceIdType.MESH)
    for d in range(1, PLANES):
        pl.semaphore_signal(barrier, inc=1,
                            device_id=((z + d) % PLANES * m + p, head_index),
                            device_id_type=pl.DeviceIdType.MESH)

    def lanes_of(h):
        return pl.ds(pl.multiple_of(h * HEAD_DIM, HEAD_DIM), HEAD_DIM)

    def load_rows(h, carry):
        for kind in range(4):
            pltpu.make_async_copy(
                flat[kind].at[:, :, lanes_of(h)], xin.at[h, kind], in_sem.at[h]
            ).start()
        return carry

    load_rows(0, 0)
    pl.semaphore_wait(barrier, m - 1 + PLANES - 1)

    def spread_chunk(c, carry):
        h, part = c // splits, c % splits
        for d in range(1, m):
            peer = (p + d) % m
            for kind in range(4):
                send(
                    xs[kind].at[:, pl.ds(peer * blocks + part * per, per), :, lanes_of(h)],
                    own.at[c, kind, pl.ds(p * rows, rows)],
                    a_send, a_recv.at[c], first + peer,
                )
        for kind in range(4):
            pltpu.make_async_copy(
                xs[kind].at[:, pl.ds(p * blocks + part * per, per), :, lanes_of(h)],
                own.at[c, kind, pl.ds(p * rows, rows)],
                a_loc.at[c],
            ).start()
        return carry

    lax.fori_loop(0, AHEAD, spread_chunk, 0)
    lax.fori_loop(1, heads, load_rows, 0)

    def forward_row(h, r):
        q, g, k, v = [xin[h, kind, r] for kind in range(4)]
        for i in range(q.shape[0] // CHUNK):
            span = slice(i * CHUNK, (i + 1) * CHUNK)
            _, top, total, out = softmax_of(scores_of(chunk(q, i), k, row_bias, i), v)
            orow[h, r, :, span] = out
            lse = top + jnp.log2(total)
            grad_t = chunk(g, i).astype(F32).T
            dots = jnp.sum(grad_t * out, axis=0, keepdims=True)
            for part in range(CHUNK // LANES):
                lanes = slice(part * LANES, (part + 1) * LANES)
                at = i * (CHUNK // LANES) + part
                st_row[2 * h, at, pl.ds(r, 1), :] = lse[:, lanes]
                st_row[2 * h + 1, at, pl.ds(r, 1), :] = dots[:, lanes]

    def send_stats(h):
        pair = pl.ds(2 * h, 2)
        for d in range(1, m):
            peer = (p + d) % m
            send(st_row.at[pair, peer], st_own.at[pair, p], s_send, s_recv.at[h], first + peer)
        st_own[pair, p] = st_row[pair, p]

    def wait_stats(h):
        drain(st_own.at[pl.ds(2 * h, 2), pl.ds(0, m - 1)], s_recv.at[h])

    def pass_stats(h):
        wait_stats(h)
        pair = pl.ds(2 * h, 2)
        send(st_own.at[pair], st_far.at[pair], sf_send, sf_recv.at[h], inner_peer)

    def tile(ref, *at):
        return ref[at].reshape(plane_rows * GROUP, HEAD_DIM)

    def put(ref, at, value):
        ref[at] = value.astype(BF16).reshape(plane_rows, GROUP, HEAD_DIM)

    def stat_of(ref, which, block):
        return to_tile(ref[which].reshape(plane_rows, LANES), block)

    def add_lse(ref, h, line, block):
        ref[h] = ref[h] + from_tile(line, block).reshape(m, rows, LANES)

    half = plane_rows * GROUP

    def solve(c, lower):
        h, part = c // splits, c % splits
        pair = (far, own) if lower else (own, far)
        lses = (lse_far, lse_own) if lower else (lse_own, lse_far)
        stats = (st_far, st_own) if lower else (st_own, st_far)

        @pl.when(part == 0)
        def _():
            wait_stats(h)
            drain(st_far.at[pl.ds(2 * h, 2)], sf_recv.at[h])
            lse_own[h] = jnp.zeros(lse_own.shape[1:], F32)
            lse_far[h] = jnp.zeros(lse_far.shape[1:], F32)

        def body(b, carry):
            block = part * per + b
            every = slice(None)

            def both(kind):
                return jnp.concatenate([tile(ref, c, kind, every, b) for ref in pair], axis=0)

            q, g, k, v = [both(kind) for kind in range(4)]
            keys, values = [k], [v]
            if not lower:
                keys = [jnp.concatenate([tile(low, c, 0, every, b), tile(low, c, 2, every, b)], axis=0), k]
                values = [jnp.concatenate([tile(low, c, 1, every, b), tile(low, c, 3, every, b)], axis=0), v]
            lse_row = jnp.concatenate([stat_of(s, 2 * h, block) for s in stats], axis=1)
            dot_row = jnp.concatenate([stat_of(s, 2 * h + 1, block) for s in stats], axis=1)
            o, gq, gk, gv, lse_col = column_unit(q, g, keys, values, None, lse_row, dot_row)
            if lower:
                ring[c % ring.shape[0], b, 0] = gk[-1]
                ring[c % ring.shape[0], b, 1] = gv[-1]
                values = (o, gq)
            else:
                put(low, (c, 0, every, b), gk[0][:half])
                put(low, (c, 1, every, b), gv[0][:half])
                put(low, (c, 2, every, b), gk[0][half:])
                put(low, (c, 3, every, b), gv[0][half:])
                values = (o, gq, gk[-1], gv[-1])
            for n, ref in enumerate(pair):
                span = slice(n * half, (n + 1) * half)
                for kind, value in enumerate(values):
                    put(ref, (c, kind, every, b), value[span])
                add_lse(lses[n], h, lse_col[:, span], block)
            return carry

        lax.fori_loop(0, per, body, 0)

    def add_upper(c):
        def body(b, carry):
            for kind in range(2):
                total = ring[c % ring.shape[0], b, kind]
                for n, ref in enumerate((far, own)):
                    share = tile(low, c, 2 * n + kind, slice(None), b).astype(F32)
                    put(ref, (c, 2 + kind, slice(None), b), total[n * half:(n + 1) * half] + share)
            return carry

        lax.fori_loop(0, per, body, 0)

    early, late = pl.ds(0, 2), pl.ds(2, 2)

    def return_rows(c, ref, kinds, send_sem, recv_sem):
        h, part = c // splits, c % splits
        at = pl.ds(p * blocks + part * per, per)
        for d in range(1, m):
            peer = (p + d) % m
            send(
                ref.at[c, kinds, pl.ds(peer * rows, rows)], back.at[h, kinds, :, at],
                send_sem, recv_sem.at[h], first + peer,
            )
        back[h, kinds, :, at] = ref[c, kinds, pl.ds(p * rows, rows)]

    def return_first(c, ref):
        h, part = c // splits, c % splits
        return_rows(c, ref, early, e_send, e_recv)

        @pl.when(part == splits - 1)
        def _():
            for d in range(1, m):
                peer = (p + d) % m
                send(lse_own.at[h, peer], lse_back.at[h, p], le_send, le_recv.at[h], first + peer)
            lse_back[h, p] = lse_own[h, p]

    def return_second(c, ref):
        return_rows(c, ref, late, g_send, g_recv)

    def far_first(c):
        h, part = c // splits, c % splits
        send(far.at[c, early], far.at[c, early], d1_send, d1_recv.at[c], outer_peer)

        @pl.when(part == splits - 1)
        def _():
            send(lse_far.at[h], lse_own.at[h], l1_send, l1_recv.at[h], outer_peer)

    def far_second(c):
        send(far.at[c, late], far.at[c, late], f1_send, f1_recv.at[c], outer_peer)

    def pass_on(c):
        drain(own.at[c, :, pl.ds(0, rows * (m - 1))], a_recv.at[c])
        drain(own.at[c, :, pl.ds(0, rows)], a_loc.at[c])

        @pl.when(outer)
        def _():
            send(own.at[c, late], far.at[c, late], b_send, bkv_recv.at[c], inner_peer)
            send(own.at[c, early], far.at[c, early], b_send, bqg_recv.at[c], inner_peer)

        @pl.when(z == 1)
        def _():
            send(own.at[c, late], low.at[c, pl.ds(2, 2)], k1_send.at[c], k1_recv.at[c], seq + m)

    def pass_far(c):
        drain(far.at[c, late], bkv_recv.at[c])
        send(far.at[c, late], low.at[c, pl.ds(0, 2)], k0_send.at[c], k0_recv.at[c], seq + m)

    def upper(c):
        drain(far.at[c, late], bkv_recv.at[c])
        drain(far.at[c, early], bqg_recv.at[c])
        drain(low.at[c, pl.ds(2, 2)], k1_recv.at[c])
        drain(low.at[c, pl.ds(0, 2)], k0_recv.at[c])
        solve(c, False)
        send(low.at[c], low.at[c], d2_send, d2_recv.at[c], seq - m)
        far_first(c)
        return_first(c, own)
        far_second(c)
        return_second(c, own)

    def lower_first(c):
        drain(far.at[c, early], bqg_recv.at[c])
        solve(c, True)
        far_first(c)
        return_first(c, own)

    def lower_second(c):
        drain(low.at[c], d2_recv.at[c])
        drain(own.at[c, late], k1_send.at[c])
        drain(far.at[c, late], k0_send.at[c])
        add_upper(c)
        far_second(c)
        return_second(c, own)

    def edge_first(c):
        h, part = c // splits, c % splits
        drain(far.at[c, early], d1_recv.at[c])

        @pl.when(part == splits - 1)
        def _():
            drain(lse_own.at[h], l1_recv.at[h])

        return_first(c, far)

    def edge_second(c):
        drain(far.at[c, late], f1_recv.at[c])
        return_second(c, far)

    def backward_row(h, r):
        slab = CHUNK // GROUP

        def came_back(kind, i):
            return back[h, kind, r, i * slab:(i + 1) * slab].reshape(CHUNK, HEAD_DIM).astype(F32)

        def give(kind, i, value):
            back[h, kind, r, i * slab:(i + 1) * slab] = value.astype(BF16).reshape(slab, GROUP, HEAD_DIM)

        q, g, k, v = [xin[h, kind, r] for kind in range(4)]
        gk, gv = row_gradients(
            q, k, v, g,
            lambda span: orow[h, r, :, span],
            lambda i: stat_line(st_row.at[2 * h], r, i),
            lambda i: stat_line(lse_back.at[h], r, i),
            came_back, give,
        )
        for j in range(len(gk)):
            span = slice(j * CHUNK, (j + 1) * CHUNK)
            row_sum[r, 0, span] = gk[j] * SCALE
            row_sum[r, 1, span] = gv[j]

    ready = pl.ds(0, blocks * (m - 1))

    def backward_ready(h):
        drain(back.at[h, early, :, ready], e_recv.at[h])
        drain(lse_back.at[h, pl.ds(0, m - 1)], le_recv.at[h])

    def backward_done(h):
        drain(back.at[h, late, :, ready], g_recv.at[h])

        def body(r, carry):
            for n in range(2):
                share = back[h, 2 + n, r].reshape(ROW_LEN, HEAD_DIM).astype(F32)
                total = (row_sum[r, n] + share).astype(BF16)
                back[h, 2 + n, r] = total.reshape(back.shape[3:])
            return carry

        lax.fori_loop(0, rows, body, 0)

    lag_upper, lag_low1, lag_low2, lag_edge1, lag_edge2, lag_rows = LAGS
    pace = splits // rows

    def rows_forward(s):
        h = s // splits + 1

        @pl.when((h < heads) & (s % splits == 0))
        def _():
            drain(xin.at[h], in_sem.at[h])

        @pl.when((h < heads) & (s % pace == 0))
        def _():
            forward_row(h, s % splits // pace)

        @pl.when((h < heads) & (s % splits == (rows - 1) * pace))
        def _():
            send_stats(h)

        @pl.when((h < heads) & (s % splits == splits - 1) & outer)
        def _():
            pass_stats(h)

    def rows_backward(t):
        h = t // splits
        last = h == heads - 1

        @pl.when((t >= 0) & (t % splits == 0))
        def _():
            backward_ready(h)

        @pl.when((t >= 0) & ((t % pace == 0) & ~last | (t == chunks - splits)))
        def _():
            def body(r, carry):
                backward_row(h, r)
                return carry

            start = jnp.where(last, 0, t % splits // pace)
            lax.fori_loop(start, jnp.where(last, rows, start + 1), body, 0)

        @pl.when((t >= 0) & (t % splits == splits - 1) & ~last)
        def _():
            backward_done(h)

    def step(s, carry):
        def at(lag, role=None):
            ready = (s >= lag) & (s < chunks + lag)
            return ready if role is None else ready & role

        @pl.when(at(0))
        def _():
            pass_on(s)

        @pl.when(s + AHEAD < chunks)
        def _():
            spread_chunk(s + AHEAD, 0)

        @pl.when(at(1, z == 1))
        def _():
            pass_far(s - 1)

        @pl.when((s == 0) & outer)
        def _():
            pass_stats(0)

        @pl.when(at(lag_upper, z == 2))
        def _():
            upper(s - lag_upper)

        @pl.when(at(lag_low1, z == 1))
        def _():
            lower_first(s - lag_low1)

        @pl.when(at(lag_low2, z == 1))
        def _():
            lower_second(s - lag_low2)

        @pl.when(at(lag_edge1, outer))
        def _():
            edge_first(s - lag_edge1)

        @pl.when(at(lag_edge2, outer))
        def _():
            edge_second(s - lag_edge2)

        rows_forward(s)
        rows_backward(s - lag_rows - (splits - 1))
        return carry

    drain(xin.at[0], in_sem.at[0])

    def first_head(r, carry):
        forward_row(0, r)
        return carry

    lax.fori_loop(0, rows, first_head, 0)
    send_stats(0)
    lax.fori_loop(0, chunks + max(LAGS), step, 0)
    backward_done(heads - 1)

    drain(own.at[:, :, pl.ds(0, rows * (m - 1))], a_send)
    drain(own.at[:, early, pl.ds(0, rows * (m - 1))], e_send)
    drain(own.at[:, late, pl.ds(0, rows * (m - 1))], g_send)
    drain(st_own.at[:, pl.ds(0, m - 1)], s_send)
    drain(lse_own.at[:, pl.ds(0, m - 1)], le_send)

    @pl.when(outer)
    def _():
        drain(own, b_send)
        drain(st_far, sf_send)

    @pl.when((z == 1) | (z == 2))
    def _():
        drain(far.at[:, early], d1_send)
        drain(far.at[:, late], f1_send)
        drain(lse_far, l1_send)

    @pl.when(z == 2)
    def _():
        drain(low, d2_send)


AHEAD = 2
RING = 8
LAGS = (2, 2, 5, 4, 7, 6)


def fits(tokens, width, devices):
    rows = tokens // ROW_LEN
    if tokens % ROW_LEN or devices % PLANES or width % HEAD_DIM:
        return False
    m = devices // PLANES
    blocks = ROW_LEN // GROUP
    return (
        m > 1
        and ROW_LEN // m == LANES
        and rows * m * GROUP == LANES
        and (blocks // m) % SPLITS == 0
        and SPLITS % rows == 0
    )


def by_planes(queries, key_vectors, value_vectors, grad_output):
    devices = lax.axis_size("seq")
    m = devices // PLANES
    tokens, width = queries.shape
    rows, heads, blocks = tokens // ROW_LEN, width // HEAD_DIM, ROW_LEN // GROUP
    per = blocks // m // SPLITS
    chunks = heads * SPLITS
    arrays = (queries, grad_output, key_vectors, value_vectors)
    views = [a.reshape(rows, blocks, GROUP, width) for a in arrays]
    flat = [a.reshape(rows, ROW_LEN, width) for a in arrays]
    buffer = pltpu.VMEM((chunks, 4, rows * m, per, GROUP, HEAD_DIM), BF16)
    dma = pltpu.SemaphoreType.DMA
    stat = pltpu.VMEM((2 * heads, m, rows, LANES), F32)
    lse = pltpu.VMEM((heads, m, rows, LANES), F32)
    each, by_head, single = dma((chunks,)), dma((heads,)), dma(())
    back = pl.pallas_call(
        fused_kernel,
        in_specs=[pl.BlockSpec(memory_space=pl.ANY)] * 8,
        out_specs=pl.BlockSpec(memory_space=pltpu.VMEM),
        out_shape=pltpu.VMEM((heads, 4, rows, blocks, GROUP, HEAD_DIM), BF16),
        scratch_shapes=[
            pltpu.VMEM((heads, 4, rows, ROW_LEN, HEAD_DIM), BF16),
            buffer, buffer, buffer,
            pltpu.VMEM((heads, rows, HEAD_DIM, ROW_LEN), F32),
            pltpu.VMEM((RING, per, 2, 2 * LANES, HEAD_DIM), F32),
            pltpu.VMEM((rows, 2, ROW_LEN, HEAD_DIM), F32),
            stat, stat, stat, lse, lse, lse,
            by_head, each, single, each, single, each, each,
            each, each, each, each, single, each, single,
            each, single, each, single, by_head, single, by_head,
            single, by_head, single, by_head, single, by_head, single, by_head,
        ],
        compiler_params=pltpu.CompilerParams(
            collective_id=0, has_side_effects=True, vmem_limit_bytes=50 * 1024 * 1024
        ),
        cost_estimate=pl.CostEstimate(
            flops=tokens * width * 512 * 24,
            bytes_accessed=tokens * width * 16,
            transcendentals=tokens * width,
        ),
        name="by_planes",
    )(*views, *flat)
    outs = copy_out(back, views[0].shape)
    return tuple(a.reshape(queries.shape) for a in outs)


def on_device(queries, key_vectors, value_vectors, grad_output):
    arrays = (queries, key_vectors, value_vectors, grad_output)
    if fits(*queries.shape, lax.axis_size("seq")):
        return by_planes(*arrays)
    return by_all_to_all(*arrays)


def solution(mesh):
    spec = P("seq", "head")
    return jax.shard_map(
        on_device,
        mesh=mesh,
        in_specs=(spec,) * 4,
        out_specs=(spec,) * 4,
        check_vma=False,
    )
```

```python
import functools
import math

import jax
import jax.numpy as jnp
from jax import lax
from jax.experimental import pallas as pl
from jax.experimental.pallas import tpu as pltpu
from jax.sharding import PartitionSpec as P

ROW_LEN = 512
HEAD_DIM = 128
GROUP = 8
CHUNK = 256
PIECES = 2
MASKED = -1e30
FLOOR = -1e20
LOG2E = 1.0 / math.log(2.0)
SCALE = 1.0 / math.sqrt(HEAD_DIM)
F32 = jnp.float32
BF16 = jnp.bfloat16


def dot_t(left, right):
    return lax.dot_general(left, right, (((1,), (1,)), ((), ())), preferred_element_type=F32)


def dot_f(left, right):
    return lax.dot_general(left, right, (((0,), (0,)), ((), ())), preferred_element_type=F32)


def dot(left, right):
    return jnp.dot(left, right, preferred_element_type=F32)


def row_bias(first, key_chunk, query_chunk):
    if key_chunk < query_chunk:
        return None
    keys = lax.broadcasted_iota(jnp.int32, (CHUNK, CHUNK), 0)
    queries = lax.broadcasted_iota(jnp.int32, (CHUNK, CHUNK), 1)
    return jnp.where(keys <= queries, 0.0, MASKED)


def col_bias(first, key_chunk, query_chunk):
    keys = lax.broadcasted_iota(jnp.int32, (CHUNK, CHUNK), 0)
    queries = lax.broadcasted_iota(jnp.int32, (CHUNK, CHUNK), 1)
    gap = queries - keys
    same = (gap & (GROUP - 1)) == 0
    if key_chunk == query_chunk:
        same = same & (gap > 0)
    return jnp.where(same, 0.0, MASKED)


def chunk(array, index):
    return array[index * CHUNK : (index + 1) * CHUNK]


def scores_of(query, keys, bias, query_chunk):
    out = []
    for j in range(query_chunk + 1):
        s = dot_t(chunk(keys, j), query) * (SCALE * LOG2E)
        b = bias(None, j, query_chunk)
        out.append(s if b is None else s + b)
    return out


def softmax_of(scores, values):
    top = functools.reduce(
        jnp.maximum, [jnp.max(s, axis=0, keepdims=True) for s in scores]
    )
    top = jnp.maximum(top, FLOOR)
    weights = [jnp.exp2(s - top) for s in scores]
    total = sum(jnp.sum(w, axis=0, keepdims=True) for w in weights)
    acc = sum(dot_f(chunk(values, j), w.astype(BF16)) for j, w in enumerate(weights))
    total = jnp.maximum(total, 1.0)
    return weights, top, total, acc / total


def merge(left, right):
    top = jnp.maximum(left, right)
    w_left, w_right = jnp.exp2(left - top), jnp.exp2(right - top)
    den = w_left + w_right
    return top + jnp.log2(den), w_left / den, w_right / den


def backward_of(i, probs, delta, q, k, v, g, gk, gv):
    query, grad = chunk(q, i), chunk(g, i)
    gq = None
    for j, p in enumerate(probs):
        dv = dot(p.astype(BF16), grad)
        dp = dot_t(chunk(v, j), grad)
        ds = (p * (dp - delta)).astype(BF16)
        dk = dot(ds, query)
        dq = dot_f(chunk(k, j), ds)
        gv[j] = dv if gv[j] is None else gv[j] + dv
        gk[j] = dk if gk[j] is None else gk[j] + dk
        gq = dq if gq is None else gq + dq
    return (gq * SCALE).T


def row_forward_kernel(q_ref, k_ref, v_ref, g_ref, o_ref, lse_ref, dot_ref):
    q, k, v, g = q_ref[0], k_ref[0], v_ref[0], g_ref[0]
    for i in range(q.shape[0] // CHUNK):
        span = slice(i * CHUNK, (i + 1) * CHUNK)
        _, top, total, out = softmax_of(scores_of(chunk(q, i), k, row_bias, i), v)
        o_ref[0, 0, :, span] = out
        lse_ref[0, 0, :, span] = top + jnp.log2(total)
        grad_t = chunk(g, i).astype(F32).T
        dot_ref[0, 0, :, span] = jnp.sum(grad_t * out, axis=0, keepdims=True)


def row_forward(q, k, v, g):
    rows, length, width = q.shape
    heads = width // HEAD_DIM
    block = pl.BlockSpec((1, length, HEAD_DIM), lambda r, h: (r, 0, h))
    stat = pl.BlockSpec((1, 1, 1, length), lambda r, h: (r, h, 0, 0))
    stat_shape = jax.ShapeDtypeStruct((rows, heads, 1, length), F32)
    return pl.pallas_call(
        row_forward_kernel,
        grid=(rows, heads),
        in_specs=[block] * 4,
        out_specs=[
            pl.BlockSpec((1, 1, HEAD_DIM, length), lambda r, h: (r, h, 0, 0)),
            stat,
            stat,
        ],
        out_shape=[
            jax.ShapeDtypeStruct((rows, heads, HEAD_DIM, length), F32),
            stat_shape,
            stat_shape,
        ],
        cost_estimate=pl.CostEstimate(
            flops=rows * heads * length * length * HEAD_DIM * 8,
            bytes_accessed=rows * length * width * 12,
            transcendentals=rows * heads * length * length,
        ),
        name="row_forward",
    )(q, k, v, g)


def col_kernel(x_ref, stat_ref, y_ref, lse_ref):
    devices, _, _, per, width = x_ref.shape
    tokens = devices * per
    chunks = tokens // CHUNK
    q, k, v, g = [x_ref[:, a, 0].reshape(tokens, width) for a in range(4)]
    gk, gv = [None] * chunks, [None] * chunks
    slab = CHUNK // per
    for i in range(chunks):
        span = slice(i * CHUNK, (i + 1) * CHUNK)
        here = slice(i * slab, (i + 1) * slab)
        weights, top, total, out = softmax_of(scores_of(chunk(q, i), k, col_bias, i), v)
        lse_col = top + jnp.log2(total)
        lse_ref[0, 0, :, span] = lse_col
        out_low = out.T.astype(BF16)
        y_ref[here, 0, 0] = out_low.reshape(slab, per, width)
        lse, w_row, w_col = merge(stat_ref[0, 0, 0, :, span], lse_col)
        dot_col = jnp.sum(
            (chunk(g, i).astype(F32) * out_low.astype(F32)).T, axis=0, keepdims=True
        )
        delta = w_row * stat_ref[1, 0, 0, :, span] + w_col * dot_col
        factor = jnp.exp2(top - lse)
        probs = [w * factor for w in weights]
        gq = backward_of(i, probs, delta, q, k, v, g, gk, gv)
        y_ref[here, 1, 0] = gq.astype(BF16).reshape(slab, per, width)
    for j in range(chunks):
        here = slice(j * slab, (j + 1) * slab)
        y_ref[here, 2, 0] = (gk[j] * SCALE).astype(BF16).reshape(slab, per, width)
        y_ref[here, 3, 0] = gv[j].astype(BF16).reshape(slab, per, width)


def col_both(x, stats, first_head):
    devices, kinds, groups, per, width = x.shape
    heads = width // HEAD_DIM
    tokens = devices * per
    block = pl.BlockSpec(
        (devices, kinds, 1, per, HEAD_DIM), lambda c, h: (0, 0, c, 0, h)
    )
    return pl.pallas_call(
        col_kernel,
        grid=(groups, heads),
        in_specs=[
            block,
            pl.BlockSpec((2, 1, 1, 1, tokens), lambda c, h: (0, first_head + h, c, 0, 0)),
        ],
        out_specs=[block, pl.BlockSpec((1, 1, 1, tokens), lambda c, h: (h, c, 0, 0))],
        out_shape=[
            jax.ShapeDtypeStruct(x.shape, BF16),
            jax.ShapeDtypeStruct((heads, groups, 1, tokens), F32),
        ],
        cost_estimate=pl.CostEstimate(
            flops=groups * heads * tokens * tokens * HEAD_DIM * 20,
            bytes_accessed=x.size * 4,
            transcendentals=groups * heads * tokens * tokens,
        ),
        name="col_both",
    )(x, stats)


def row_backward_kernel(
    q_ref, k_ref, v_ref, g_ref, o_ref, lse_ref, back_ref, lse_col_ref, *rest
):
    att_ref, gq_ref, gk_ref, gv_ref = rest[-4:]
    q, k, v, g = q_ref[0], k_ref[0], v_ref[0], g_ref[0]
    length = q.shape[0]
    chunks = length // CHUNK
    devices = back_ref.shape[0]
    slab = devices // chunks

    def came_back(kind, i):
        part = back_ref[i * slab : (i + 1) * slab, kind, :, 0].astype(F32)
        return part.reshape(CHUNK, HEAD_DIM)

    gk, gv = [None] * chunks, [None] * chunks
    for i in range(chunks):
        span = slice(i * CHUNK, (i + 1) * CHUNK)
        lse, w_row, w_col = merge(lse_ref[0, 0, :, span], lse_col_ref[0, 0, :, span])
        col_t = came_back(0, i).T
        att_t = o_ref[0, 0, :, span] * w_row + col_t * w_col
        low = att_t.T.astype(BF16)
        att_ref[0, span, :] = low
        delta = jnp.sum(
            (chunk(g, i).astype(F32) * low.astype(F32)).T, axis=0, keepdims=True
        )
        scores = scores_of(chunk(q, i), k, row_bias, i)
        probs = [jnp.exp2(s - lse) for s in scores]
        gq = backward_of(i, probs, delta, q, k, v, g, gk, gv)
        gq_ref[0, span, :] = (gq + came_back(1, i)).astype(BF16)
    for j in range(chunks):
        span = slice(j * CHUNK, (j + 1) * CHUNK)
        gk_ref[0, span, :] = (gk[j] * SCALE + came_back(2, j)).astype(BF16)
        gv_ref[0, span, :] = (gv[j] + came_back(3, j)).astype(BF16)


def row_backward(q, k, v, g, o, lse, back, lse_col, first_head, earlier):
    rows, length, width = q.shape
    devices, kinds, groups, _, size, piece = back.shape
    heads = piece // HEAD_DIM
    block = pl.BlockSpec((1, length, HEAD_DIM), lambda r, h: (r, 0, first_head + h))
    stat = pl.BlockSpec((1, 1, 1, length), lambda r, h: (r, first_head + h, 0, 0))
    in_specs = [block] * 4 + [
        pl.BlockSpec((1, 1, HEAD_DIM, length), lambda r, h: (r, first_head + h, 0, 0)),
        stat,
        pl.BlockSpec(
            (devices, kinds, groups, 1, size, HEAD_DIM), lambda r, h: (0, 0, 0, r, 0, h)
        ),
        stat,
    ]
    aliases = {}
    if earlier:
        aliases = {len(in_specs) + n: n for n in range(4)}
        in_specs = in_specs + [pl.BlockSpec(memory_space=pl.ANY)] * 4
    return pl.pallas_call(
        row_backward_kernel,
        grid=(rows, heads),
        in_specs=in_specs,
        out_specs=[block] * 4,
        out_shape=[jax.ShapeDtypeStruct(q.shape, BF16)] * 4,
        input_output_aliases=aliases,
        cost_estimate=pl.CostEstimate(
            flops=rows * heads * length * length * HEAD_DIM * 14,
            bytes_accessed=rows * length * piece * 28,
            transcendentals=rows * heads * length * length,
        ),
        name="row_backward",
    )(q, k, v, g, o, lse, back, lse_col, *earlier)


def exchange(array):
    return lax.all_to_all(array, "seq", split_axis=0, concat_axis=0, tiled=True)


def by_all_to_all(queries, key_vectors, value_vectors, grad_output):
    devices = lax.axis_size("seq")
    rows = queries.shape[0] // ROW_LEN
    width = queries.shape[1]
    heads = width // HEAD_DIM
    groups = ROW_LEN // devices // GROUP
    per = rows * GROUP
    tokens = devices * per
    piece = width // PIECES
    piece_heads = piece // HEAD_DIM
    arrays = (queries, key_vectors, value_vectors, grad_output)
    by_row = [a.reshape(rows, ROW_LEN, width) for a in arrays]

    packs = []
    for n in range(PIECES):
        parts = [
            jnp.transpose(
                a[:, n * piece : (n + 1) * piece].reshape(rows, devices, groups, GROUP, piece),
                (1, 2, 0, 3, 4),
            )
            for a in arrays
        ]
        packed = jnp.stack(parts, axis=1).reshape(devices, 4, groups, per, piece)
        packs.append(packed)
    arrived = [exchange(packs[0])]

    o, lse, dots = row_forward(*by_row)
    stats = jnp.stack([lse, dots]).reshape(2, rows, heads, devices, groups, GROUP)
    stats = jnp.transpose(stats, (3, 0, 2, 4, 1, 5)).reshape(devices, -1)
    arrived[0], stats = lax.optimization_barrier((arrived[0], stats))
    stats = exchange(stats)
    for n in range(1, PIECES):
        packs[n], stats = lax.optimization_barrier((packs[n], stats))
        arrived.append(exchange(packs[n]))
    stats = stats.reshape(devices, 2, heads, groups, per)
    stats = jnp.transpose(stats, (1, 2, 3, 0, 4)).reshape(2, heads, groups, 1, tokens)

    columns = [col_both(arrived[n], stats, n * piece_heads) for n in range(PIECES)]
    lse_col = jnp.concatenate([lse_col for _, lse_col in columns], axis=0)
    lse_col = jnp.transpose(
        lse_col.reshape(heads, groups, devices, per), (2, 0, 1, 3)
    ).reshape(devices, -1)
    lse_col = exchange(lse_col)
    sent = [y for y, _ in columns]
    sent[-1], lse_col = lax.optimization_barrier((sent[-1], lse_col))
    lse_col = lse_col.reshape(devices, heads, groups, rows, GROUP)
    lse_col = jnp.transpose(lse_col, (3, 1, 0, 2, 4)).reshape(rows, heads, 1, ROW_LEN)
    backs = [exchange(y).reshape(devices, 4, groups, rows, GROUP, piece) for y in sent]

    outs = ()
    for n in range(PIECES):
        outs = row_backward(*by_row, o, lse, backs[n], lse_col, n * piece_heads, tuple(outs))
    return tuple(a.reshape(queries.shape) for a in outs)


PLANES = 4
SPLITS = 16
LANES = 128


def drain(ref, sem):
    pltpu.make_async_copy(ref, ref, sem).wait()


def fold_lanes(x):
    for shift in (8, 16, 32, 64):
        x = x + pltpu.roll(x, shift, 1)
    return x


def lane_masks():
    group = lax.broadcasted_iota(jnp.int32, (LANES // GROUP, LANES), 1) // GROUP
    row = lax.broadcasted_iota(jnp.int32, (LANES // GROUP, LANES), 0)
    return group, group == row


def to_tile(stat, block):
    group, diagonal = lane_masks()
    spread = fold_lanes(jnp.where(group == block, stat, 0.0))
    return jnp.sum(jnp.where(diagonal, spread, 0.0), axis=0, keepdims=True)


def from_tile(line, block):
    group, diagonal = lane_masks()
    spread = fold_lanes(jnp.where(diagonal, line, 0.0))
    return jnp.where(group == block, spread, 0.0)


def column_unit(q, g, keys, values, query_chunk, lse_row, dot_row):
    count = len(keys)
    scores = []
    for j in range(count):
        bias = col_bias(None, j, count - 1)
        scores.append(dot_t(keys[j], q) * (SCALE * LOG2E) + bias)
    top = functools.reduce(
        jnp.maximum, [jnp.max(s, axis=0, keepdims=True) for s in scores]
    )
    top = jnp.maximum(top, FLOOR)
    weights = [jnp.exp2(s - top) for s in scores]
    total = sum(jnp.sum(w, axis=0, keepdims=True) for w in weights)
    acc = sum(dot_f(v, w.astype(BF16)) for v, w in zip(values, weights))
    total = jnp.maximum(total, 1.0)
    out_low = (acc / total).T.astype(BF16)
    lse_col = top + jnp.log2(total)
    lse, w_row, w_col = merge(lse_row, lse_col)
    dot_col = jnp.sum(
        (g.astype(F32) * out_low.astype(F32)).T, axis=0, keepdims=True
    )
    delta = w_row * dot_row + w_col * dot_col
    factor = jnp.exp2(top - lse)
    gq, gk, gv = None, [], []
    for j in range(count):
        p = weights[j] * factor
        gv.append(dot(p.astype(BF16), g))
        dp = dot_t(values[j], g)
        ds = (p * (dp - delta)).astype(BF16)
        gk.append(dot(ds, q) * SCALE)
        dq = dot_f(keys[j], ds)
        gq = dq if gq is None else gq + dq
    return out_low, (gq * SCALE).T.astype(BF16), gk, gv, lse_col


def stat_line(ref, r, i):
    base = i * (CHUNK // LANES)
    return jnp.concatenate(
        [ref[base + n, pl.ds(r, 1), :] for n in range(CHUNK // LANES)], axis=1
    )


def row_gradients(q, k, v, g, o_row, lse_row, lse_col, came_back, give):
    count = q.shape[0] // CHUNK
    gk, gv = [None] * count, [None] * count
    for i in range(count):
        span = slice(i * CHUNK, (i + 1) * CHUNK)
        lse, w_row, w_col = merge(lse_row(i), lse_col(i))
        att_t = o_row(span) * w_row + came_back(0, i).T * w_col
        att = att_t.T.astype(BF16)
        give(0, i, att)
        delta = jnp.sum(
            (chunk(g, i).astype(F32) * att.astype(F32)).T, axis=0, keepdims=True
        )
        scores = scores_of(chunk(q, i), k, row_bias, i)
        probs = [jnp.exp2(s - lse) for s in scores]
        gq = backward_of(i, probs, delta, q, k, v, g, gk, gv)
        give(1, i, gq + came_back(1, i))
    return gk, gv


def copy_kernel(*refs):
    back, outs, sem = refs[0], refs[1:5], refs[5]
    copies = [
        pltpu.make_async_copy(
            back.at[h, n], outs[n].at[:, :, :, h * HEAD_DIM:(h + 1) * HEAD_DIM], sem.at[h, n]
        )
        for h in range(back.shape[0]) for n in range(4)
    ]
    for copy in copies:
        copy.start()
    for copy in copies:
        copy.wait()


def copy_out(back, shape):
    return pl.pallas_call(
        copy_kernel,
        in_specs=[pl.BlockSpec(memory_space=pltpu.VMEM)],
        out_specs=[pl.BlockSpec(memory_space=pl.ANY)] * 4,
        out_shape=[jax.ShapeDtypeStruct(shape, BF16)] * 4,
        scratch_shapes=[pltpu.SemaphoreType.DMA(back.shape[:2])],
        compiler_params=pltpu.CompilerParams(vmem_limit_bytes=2 * 1024 * 1024),
        name="copy_out",
    )(back)


def fused_kernel(*refs):
    xs, flat, back = refs[0:4], refs[4:8], refs[8]
    (xin, own, far, low, orow, ring, row_sum, st_row, st_own, st_far,
     lse_own, lse_far, lse_back, in_sem, a_loc, a_send, a_recv, b_send, bkv_recv,
     bqg_recv, k1_send, k1_recv, k0_send, k0_recv, d2_send, d2_recv, d1_send,
     d1_recv, f1_send, f1_recv, e_send, e_recv, g_send, g_recv, s_send, s_recv, sf_send, sf_recv, l1_send, l1_recv,
     le_send, le_recv) = refs[9:]
    heads, _, rows = xin.shape[:3]
    chunks = own.shape[0]
    plane_rows, per = own.shape[2], own.shape[3]
    splits = chunks // heads
    devices = lax.axis_size("seq")
    m = devices // PLANES
    blocks = per * splits
    seq, head_index = lax.axis_index("seq"), lax.axis_index("head")
    z, p = seq // m, seq % m
    first = z * m

    def send(src, dst, send_sem, recv_sem, to):
        pltpu.make_async_remote_copy(
            src_ref=src, dst_ref=dst, send_sem=send_sem, recv_sem=recv_sem,
            device_id=(to, head_index), device_id_type=pl.DeviceIdType.MESH,
        ).start()

    outer = (z == 0) | (z == PLANES - 1)
    inner_peer = jnp.where(z == 0, seq + m, seq - m)
    outer_peer = jnp.where(z == 1, seq - m, seq + m)

    barrier = pltpu.get_barrier_semaphore()
    for d in range(1, m):
        pl.semaphore_signal(barrier, inc=1, device_id=(first + (p + d) % m, head_index),
                            device_id_type=pl.DeviceIdType.MESH)
    for d in range(1, PLANES):
        pl.semaphore_signal(barrier, inc=1,
                            device_id=((z + d) % PLANES * m + p, head_index),
                            device_id_type=pl.DeviceIdType.MESH)

    def lanes_of(h):
        return pl.ds(pl.multiple_of(h * HEAD_DIM, HEAD_DIM), HEAD_DIM)

    def load_rows(h, carry):
        for kind in range(4):
            pltpu.make_async_copy(
                flat[kind].at[:, :, lanes_of(h)], xin.at[h, kind], in_sem.at[h]
            ).start()
        return carry

    load_rows(0, 0)
    pl.semaphore_wait(barrier, m - 1 + PLANES - 1)

    def spread_chunk(c, carry):
        h, part = c // splits, c % splits
        for d in range(1, m):
            peer = (p + d) % m
            for kind in range(4):
                send(
                    xs[kind].at[:, pl.ds(peer * blocks + part * per, per), :, lanes_of(h)],
                    own.at[c, kind, pl.ds(p * rows, rows)],
                    a_send, a_recv.at[c], first + peer,
                )
        for kind in range(4):
            pltpu.make_async_copy(
                xs[kind].at[:, pl.ds(p * blocks + part * per, per), :, lanes_of(h)],
                own.at[c, kind, pl.ds(p * rows, rows)],
                a_loc.at[c],
            ).start()
        return carry

    lax.fori_loop(0, AHEAD, spread_chunk, 0)
    lax.fori_loop(1, heads, load_rows, 0)

    def forward_row(h, r):
        q, g, k, v = [xin[h, kind, r] for kind in range(4)]
        for i in range(q.shape[0] // CHUNK):
            span = slice(i * CHUNK, (i + 1) * CHUNK)
            _, top, total, out = softmax_of(scores_of(chunk(q, i), k, row_bias, i), v)
            orow[h, r, :, span] = out
            lse = top + jnp.log2(total)
            grad_t = chunk(g, i).astype(F32).T
            dots = jnp.sum(grad_t * out, axis=0, keepdims=True)
            for part in range(CHUNK // LANES):
                lanes = slice(part * LANES, (part + 1) * LANES)
                at = i * (CHUNK // LANES) + part
                st_row[2 * h, at, pl.ds(r, 1), :] = lse[:, lanes]
                st_row[2 * h + 1, at, pl.ds(r, 1), :] = dots[:, lanes]

    def send_stats(h):
        pair = pl.ds(2 * h, 2)
        for d in range(1, m):
            peer = (p + d) % m
            send(st_row.at[pair, peer], st_own.at[pair, p], s_send, s_recv.at[h], first + peer)
        st_own[pair, p] = st_row[pair, p]

    def wait_stats(h):
        drain(st_own.at[pl.ds(2 * h, 2), pl.ds(0, m - 1)], s_recv.at[h])

    def pass_stats(h):
        wait_stats(h)
        pair = pl.ds(2 * h, 2)
        send(st_own.at[pair], st_far.at[pair], sf_send, sf_recv.at[h], inner_peer)

    def tile(ref, *at):
        return ref[at].reshape(plane_rows * GROUP, HEAD_DIM)

    def put(ref, at, value):
        ref[at] = value.astype(BF16).reshape(plane_rows, GROUP, HEAD_DIM)

    def stat_of(ref, which, block):
        return to_tile(ref[which].reshape(plane_rows, LANES), block)

    def add_lse(ref, h, line, block):
        ref[h] = ref[h] + from_tile(line, block).reshape(m, rows, LANES)

    half = plane_rows * GROUP

    def solve(c, lower):
        h, part = c // splits, c % splits
        pair = (far, own) if lower else (own, far)
        lses = (lse_far, lse_own) if lower else (lse_own, lse_far)
        stats = (st_far, st_own) if lower else (st_own, st_far)

        @pl.when(part == 0)
        def _():
            wait_stats(h)
            drain(st_far.at[pl.ds(2 * h, 2)], sf_recv.at[h])
            lse_own[h] = jnp.zeros(lse_own.shape[1:], F32)
            lse_far[h] = jnp.zeros(lse_far.shape[1:], F32)

        def body(b, carry):
            block = part * per + b
            every = slice(None)

            def both(kind):
                return jnp.concatenate([tile(ref, c, kind, every, b) for ref in pair], axis=0)

            q, g, k, v = [both(kind) for kind in range(4)]
            keys, values = [k], [v]
            if not lower:
                keys = [jnp.concatenate([tile(low, c, 0, every, b), tile(low, c, 2, every, b)], axis=0), k]
                values = [jnp.concatenate([tile(low, c, 1, every, b), tile(low, c, 3, every, b)], axis=0), v]
            lse_row = jnp.concatenate([stat_of(s, 2 * h, block) for s in stats], axis=1)
            dot_row = jnp.concatenate([stat_of(s, 2 * h + 1, block) for s in stats], axis=1)
            o, gq, gk, gv, lse_col = column_unit(q, g, keys, values, None, lse_row, dot_row)
            if lower:
                ring[c % ring.shape[0], b, 0] = gk[-1]
                ring[c % ring.shape[0], b, 1] = gv[-1]
                values = (o, gq)
            else:
                put(low, (c, 0, every, b), gk[0][:half])
                put(low, (c, 1, every, b), gv[0][:half])
                put(low, (c, 2, every, b), gk[0][half:])
                put(low, (c, 3, every, b), gv[0][half:])
                values = (o, gq, gk[-1], gv[-1])
            for n, ref in enumerate(pair):
                span = slice(n * half, (n + 1) * half)
                for kind, value in enumerate(values):
                    put(ref, (c, kind, every, b), value[span])
                add_lse(lses[n], h, lse_col[:, span], block)
            return carry

        lax.fori_loop(0, per, body, 0)

    def add_upper(c):
        def body(b, carry):
            for kind in range(2):
                total = ring[c % ring.shape[0], b, kind]
                for n, ref in enumerate((far, own)):
                    share = tile(low, c, 2 * n + kind, slice(None), b).astype(F32)
                    put(ref, (c, 2 + kind, slice(None), b), total[n * half:(n + 1) * half] + share)
            return carry

        lax.fori_loop(0, per, body, 0)

    early, late = pl.ds(0, 2), pl.ds(2, 2)

    def return_rows(c, ref, kinds, send_sem, recv_sem):
        h, part = c // splits, c % splits
        at = pl.ds(p * blocks + part * per, per)
        for d in range(1, m):
            peer = (p + d) % m
            send(
                ref.at[c, kinds, pl.ds(peer * rows, rows)], back.at[h, kinds, :, at],
                send_sem, recv_sem.at[h], first + peer,
            )
        back[h, kinds, :, at] = ref[c, kinds, pl.ds(p * rows, rows)]

    def return_first(c, ref):
        h, part = c // splits, c % splits
        return_rows(c, ref, early, e_send, e_recv)

        @pl.when(part == splits - 1)
        def _():
            for d in range(1, m):
                peer = (p + d) % m
                send(lse_own.at[h, peer], lse_back.at[h, p], le_send, le_recv.at[h], first + peer)
            lse_back[h, p] = lse_own[h, p]

    def return_second(c, ref):
        return_rows(c, ref, late, g_send, g_recv)

    def far_first(c):
        h, part = c // splits, c % splits
        send(far.at[c, early], far.at[c, early], d1_send, d1_recv.at[c], outer_peer)

        @pl.when(part == splits - 1)
        def _():
            send(lse_far.at[h], lse_own.at[h], l1_send, l1_recv.at[h], outer_peer)

    def far_second(c):
        send(far.at[c, late], far.at[c, late], f1_send, f1_recv.at[c], outer_peer)

    def pass_on(c):
        drain(own.at[c, :, pl.ds(0, rows * (m - 1))], a_recv.at[c])
        drain(own.at[c, :, pl.ds(0, rows)], a_loc.at[c])

        @pl.when(outer)
        def _():
            send(own.at[c, late], far.at[c, late], b_send, bkv_recv.at[c], inner_peer)
            send(own.at[c, early], far.at[c, early], b_send, bqg_recv.at[c], inner_peer)

        @pl.when(z == 1)
        def _():
            send(own.at[c, late], low.at[c, pl.ds(2, 2)], k1_send.at[c], k1_recv.at[c], seq + m)

    def pass_far(c):
        drain(far.at[c, late], bkv_recv.at[c])
        send(far.at[c, late], low.at[c, pl.ds(0, 2)], k0_send.at[c], k0_recv.at[c], seq + m)

    def upper(c):
        drain(far.at[c, late], bkv_recv.at[c])
        drain(far.at[c, early], bqg_recv.at[c])
        drain(low.at[c, pl.ds(2, 2)], k1_recv.at[c])
        drain(low.at[c, pl.ds(0, 2)], k0_recv.at[c])
        solve(c, False)
        send(low.at[c], low.at[c], d2_send, d2_recv.at[c], seq - m)
        far_first(c)
        return_first(c, own)
        far_second(c)
        return_second(c, own)

    def lower_first(c):
        drain(far.at[c, early], bqg_recv.at[c])
        solve(c, True)
        far_first(c)
        return_first(c, own)

    def lower_second(c):
        drain(low.at[c], d2_recv.at[c])
        drain(own.at[c, late], k1_send.at[c])
        drain(far.at[c, late], k0_send.at[c])
        add_upper(c)
        far_second(c)
        return_second(c, own)

    def edge_first(c):
        h, part = c // splits, c % splits
        drain(far.at[c, early], d1_recv.at[c])

        @pl.when(part == splits - 1)
        def _():
            drain(lse_own.at[h], l1_recv.at[h])

        return_first(c, far)

    def edge_second(c):
        drain(far.at[c, late], f1_recv.at[c])
        return_second(c, far)

    def backward_row(h, r):
        slab = CHUNK // GROUP

        def came_back(kind, i):
            return back[h, kind, r, i * slab:(i + 1) * slab].reshape(CHUNK, HEAD_DIM).astype(F32)

        def give(kind, i, value):
            back[h, kind, r, i * slab:(i + 1) * slab] = value.astype(BF16).reshape(slab, GROUP, HEAD_DIM)

        q, g, k, v = [xin[h, kind, r] for kind in range(4)]
        gk, gv = row_gradients(
            q, k, v, g,
            lambda span: orow[h, r, :, span],
            lambda i: stat_line(st_row.at[2 * h], r, i),
            lambda i: stat_line(lse_back.at[h], r, i),
            came_back, give,
        )
        for j in range(len(gk)):
            span = slice(j * CHUNK, (j + 1) * CHUNK)
            row_sum[r, 0, span] = gk[j] * SCALE
            row_sum[r, 1, span] = gv[j]

    ready = pl.ds(0, blocks * (m - 1))

    def backward_ready(h):
        drain(back.at[h, early, :, ready], e_recv.at[h])
        drain(lse_back.at[h, pl.ds(0, m - 1)], le_recv.at[h])

    def backward_done(h):
        drain(back.at[h, late, :, ready], g_recv.at[h])

        def body(r, carry):
            for n in range(2):
                share = back[h, 2 + n, r].reshape(ROW_LEN, HEAD_DIM).astype(F32)
                total = (row_sum[r, n] + share).astype(BF16)
                back[h, 2 + n, r] = total.reshape(back.shape[3:])
            return carry

        lax.fori_loop(0, rows, body, 0)

    lag_upper, lag_low1, lag_low2, lag_edge1, lag_edge2, lag_rows = LAGS
    pace = splits // rows

    def rows_forward(s):
        h = s // splits + 1

        @pl.when((h < heads) & (s % splits == 0))
        def _():
            drain(xin.at[h], in_sem.at[h])

        @pl.when((h < heads) & (s % pace == 0))
        def _():
            forward_row(h, s % splits // pace)

        @pl.when((h < heads) & (s % splits == (rows - 1) * pace))
        def _():
            send_stats(h)

        @pl.when((h < heads) & (s % splits == splits - 1) & outer)
        def _():
            pass_stats(h)

    def rows_backward(t):
        h = t // splits
        last = h == heads - 1

        @pl.when((t >= 0) & (t % splits == 0))
        def _():
            backward_ready(h)

        @pl.when((t >= 0) & ((t % pace == 0) & ~last | (t == chunks - splits)))
        def _():
            def body(r, carry):
                backward_row(h, r)
                return carry

            start = jnp.where(last, 0, t % splits // pace)
            lax.fori_loop(start, jnp.where(last, rows, start + 1), body, 0)

        @pl.when((t >= 0) & (t % splits == splits - 1) & ~last)
        def _():
            backward_done(h)

    def step(s, carry):
        def at(lag, role=None):
            ready = (s >= lag) & (s < chunks + lag)
            return ready if role is None else ready & role

        @pl.when(at(0))
        def _():
            pass_on(s)

        @pl.when(s + AHEAD < chunks)
        def _():
            spread_chunk(s + AHEAD, 0)

        @pl.when(at(1, z == 1))
        def _():
            pass_far(s - 1)

        @pl.when(s < rows - rows // 2)
        def _():
            forward_row(0, rows // 2 + s)

        @pl.when(s == rows - rows // 2 - 1)
        def _():
            send_stats(0)

        @pl.when((s == rows - rows // 2 - 1) & outer)
        def _():
            pass_stats(0)

        @pl.when(at(lag_upper, z == 2))
        def _():
            upper(s - lag_upper)

        @pl.when(at(lag_low1, z == 1))
        def _():
            lower_first(s - lag_low1)

        @pl.when(at(lag_low2, z == 1))
        def _():
            lower_second(s - lag_low2)

        @pl.when(at(lag_edge1, outer))
        def _():
            edge_first(s - lag_edge1)

        @pl.when(at(lag_edge2, outer))
        def _():
            edge_second(s - lag_edge2)

        rows_forward(s)
        rows_backward(s - lag_rows - (splits - 1))
        return carry

    drain(xin.at[0], in_sem.at[0])

    def first_head(r, carry):
        forward_row(0, r)
        return carry

    lax.fori_loop(0, rows // 2, first_head, 0)
    lax.fori_loop(0, chunks + max(LAGS), step, 0)
    backward_done(heads - 1)

    drain(own.at[:, :, pl.ds(0, rows * (m - 1))], a_send)
    drain(own.at[:, early, pl.ds(0, rows * (m - 1))], e_send)
    drain(own.at[:, late, pl.ds(0, rows * (m - 1))], g_send)
    drain(st_own.at[:, pl.ds(0, m - 1)], s_send)
    drain(lse_own.at[:, pl.ds(0, m - 1)], le_send)

    @pl.when(outer)
    def _():
        drain(own, b_send)
        drain(st_far, sf_send)

    @pl.when((z == 1) | (z == 2))
    def _():
        drain(far.at[:, early], d1_send)
        drain(far.at[:, late], f1_send)
        drain(lse_far, l1_send)

    @pl.when(z == 2)
    def _():
        drain(low, d2_send)


AHEAD = 2
RING = 8
LAGS = (2, 2, 5, 4, 7, 6)


def fits(tokens, width, devices):
    rows = tokens // ROW_LEN
    if tokens % ROW_LEN or devices % PLANES or width % HEAD_DIM:
        return False
    m = devices // PLANES
    blocks = ROW_LEN // GROUP
    return (
        m > 1
        and ROW_LEN // m == LANES
        and rows * m * GROUP == LANES
        and (blocks // m) % SPLITS == 0
        and SPLITS % rows == 0
    )


def by_planes(queries, key_vectors, value_vectors, grad_output):
    devices = lax.axis_size("seq")
    m = devices // PLANES
    tokens, width = queries.shape
    rows, heads, blocks = tokens // ROW_LEN, width // HEAD_DIM, ROW_LEN // GROUP
    per = blocks // m // SPLITS
    chunks = heads * SPLITS
    arrays = (queries, grad_output, key_vectors, value_vectors)
    views = [a.reshape(rows, blocks, GROUP, width) for a in arrays]
    flat = [a.reshape(rows, ROW_LEN, width) for a in arrays]
    buffer = pltpu.VMEM((chunks, 4, rows * m, per, GROUP, HEAD_DIM), BF16)
    dma = pltpu.SemaphoreType.DMA
    stat = pltpu.VMEM((2 * heads, m, rows, LANES), F32)
    lse = pltpu.VMEM((heads, m, rows, LANES), F32)
    each, by_head, single = dma((chunks,)), dma((heads,)), dma(())
    back = pl.pallas_call(
        fused_kernel,
        in_specs=[pl.BlockSpec(memory_space=pl.ANY)] * 8,
        out_specs=pl.BlockSpec(memory_space=pltpu.VMEM),
        out_shape=pltpu.VMEM((heads, 4, rows, blocks, GROUP, HEAD_DIM), BF16),
        scratch_shapes=[
            pltpu.VMEM((heads, 4, rows, ROW_LEN, HEAD_DIM), BF16),
            buffer, buffer, buffer,
            pltpu.VMEM((heads, rows, HEAD_DIM, ROW_LEN), F32),
            pltpu.VMEM((RING, per, 2, 2 * LANES, HEAD_DIM), F32),
            pltpu.VMEM((rows, 2, ROW_LEN, HEAD_DIM), F32),
            stat, stat, stat, lse, lse, lse,
            by_head, each, single, each, single, each, each,
            each, each, each, each, single, each, single,
            each, single, each, single, by_head, single, by_head,
            single, by_head, single, by_head, single, by_head, single, by_head,
        ],
        compiler_params=pltpu.CompilerParams(
            collective_id=0, has_side_effects=True, vmem_limit_bytes=50 * 1024 * 1024
        ),
        cost_estimate=pl.CostEstimate(
            flops=tokens * width * 512 * 24,
            bytes_accessed=tokens * width * 16,
            transcendentals=tokens * width,
        ),
        name="by_planes",
    )(*views, *flat)
    outs = copy_out(back, views[0].shape)
    return tuple(a.reshape(queries.shape) for a in outs)


def on_device(queries, key_vectors, value_vectors, grad_output):
    arrays = (queries, key_vectors, value_vectors, grad_output)
    if fits(*queries.shape, lax.axis_size("seq")):
        return by_planes(*arrays)
    return by_all_to_all(*arrays)


def solution(mesh):
    spec = P("seq", "head")
    return jax.shard_map(
        on_device,
        mesh=mesh,
        in_specs=(spec,) * 4,
        out_specs=(spec,) * 4,
        check_vma=False,
    )
```
